32 devices in a mesh: dp: 4 (over x, core), ctx: 8 (over z, y).
Axes of the slice: x: 2, y: 2, z: 4, core: 2. Of those that a mesh axis runs over, the one named last changes fastest.
Arguments:
- tokens: bfloat16 [4, 1024, 1024], P('dp', 'ctx'), may hold values from -6 to 6
- doc_lengths: int32 [4, 8], P('dp'), may hold values from 1 to 512, 1024 in all within a row
- first_gain: float32 [1024], P(('dp', 'ctx')), may hold values from 0.5 to 1.5
- factor_weights: float32 [1024, 800], P(('dp', 'ctx')), may hold values from -0.25 to 0.25
- output_weights: float32 [1024, 1024], P(('dp', 'ctx')), may hold values from -1.5 to 1.5
- second_gain: float32 [1024], P(('dp', 'ctx')), may hold values from 0.5 to 1.5
- gate_weights: float32 [1024, 2816], P(('dp', 'ctx')), may hold values from -0.1875 to 0.1875
- up_weights: float32 [1024, 2816], P(('dp', 'ctx')), may hold values from -0.1875 to 0.1875
- down_weights: float32 [2816, 1024], P(('dp', 'ctx')), may hold values from -0.109375 to 0.109375
- cotangent: bfloat16 [4, 1024, 1024], P('dp', 'ctx'), may hold values from -6 to 6
Outputs:
- layer_output: bfloat16 [4, 1024, 1024], P('dp', 'ctx')
- input_grad: bfloat16 [4, 1024, 1024], P('dp', 'ctx')
- first_grads: float32 [1024], P(('dp', 'ctx'))
- factor_grads: float32 [1024, 800], P(('dp', 'ctx'))
- output_grads: float32 [1024, 1024], P(('dp', 'ctx'))
- second_grads: float32 [1024], P(('dp', 'ctx'))
- gate_grads: float32 [1024, 2816], P(('dp', 'ctx'))
- up_grads: float32 [1024, 2816], P(('dp', 'ctx'))
- down_grads: float32 [2816, 1024], P(('dp', 'ctx'))
The draws below stay inside these ranges and needn't reach their ends.
Inputs may be any that keep to these rules, and one draw needn't show every extreme that they name: `doc_lengths`: each stream's 8 document lengths sum to 1024; the documents lie end to end from position 0.
All inputs are finite; a program needn't handle non-finite values.
Results may differ from the reference program's by a relative error of at most 0.018.
The reference program's roundings to bfloat16 on the way count: a program that leaves them out, or rounds other values in their place, can miss the bound.
Values may be sent and summed in bfloat16 or wider, within the bound.
A program may use at most 256 MiB of HBM per device.

```python
import math
import jax
import jax.numpy as jnp
import numpy as np
from jax import lax

D = 1024
H = 16
DH = 64
RQ = 6
RKV = 2
FF = 2816
HD = 1024
FDIM = 800
LENGTH = 1024
STREAMS = 4
MAXDOC = 512
NDOC = 8


def with_spikes(values, key, source, target, parts, factor):
    owner, partner = [(jnp.arange(values.shape[axis_at]) // (values.shape[axis_at] // parts)).reshape([-1 if axis == axis_at else 1 for axis in range(values.ndim)]) for axis_at in (source, target)]
    chosen = jax.random.permutation(key, parts)[partner]
    strong = (owner == chosen) | (owner == (partner + parts // 2) % parts)
    return jnp.where(strong, factor * values, values)


def block_scale(own_key, dims, pieces, smallest, high):
    def one(axis_at, parts):
        steps = jax.random.uniform(jax.random.fold_in(jax.random.fold_in(own_key, 6), axis_at), (parts,), jnp.float32, smallest / len(pieces), high / len(pieces))
        return jnp.repeat(jnp.exp(steps), dims[axis_at] // parts).reshape((-1,) + (1,) * (len(dims) - axis_at - 1))

    level = one(*pieces[0])
    for cut in pieces[1:]:
        level = level * one(*cut)
    return level


def length_profile(amount, total, most, slope):
    portions = [(1 << 20) // math.isqrt(grade ** slope) + 1 for grade in range(2, amount + 1)]
    rest, holding = total - most - (amount - 1), [1] * (amount - 1)
    while rest > 0:
        free = [i for i in range(amount - 1) if holding[i] < most]
        whole, budget = sum([portions[i] for i in free]), rest
        for i in free:
            extra = min(most - holding[i], max(1, budget * portions[i] // whole), rest)
            holding[i] = holding[i] + extra
            rest = rest - extra
    return np.array([most] + holding)


def uneven(key, number_of, total, most, lean):
    if number_of == 2:
        one = jax.random.randint(key, (), max(1, total - most), min(most, total - 1) + 1)
        return jnp.stack([one, total - one])
    tallies = jnp.asarray(length_profile(number_of, total, most, lean), jnp.int32)
    twos = (number_of - 1) // 2
    giver, taker = tallies[1:1 + 2 * twos:2], tallies[2:2 + 2 * twos:2]
    room = jnp.minimum(giver - 1, most - taker)
    shifted = jax.random.randint(jax.random.fold_in(key, 1), (twos,), 0, 1 << 20) % (room + 1)
    tallies = tallies.at[1:1 + 2 * twos:2].set(giver - shifted).at[2:2 + 2 * twos:2].set(taker + shifted)
    return tallies[jax.random.permutation(jax.random.fold_in(key, 2), number_of)]


def scatter_about(key, extent, width, most, split=(), kind=jnp.bfloat16):
    values = width * jax.random.normal(key, extent, jnp.float32)
    if split:
        values = values * block_scale(key, extent, split, -0.22, 0.18)
    return jnp.clip(values, -most, most).astype(kind)


def noise_with(stream_key, extent, width, most, pieces, heavy, held_as=jnp.bfloat16):
    values = width * jax.random.normal(stream_key, extent, jnp.float32)
    if pieces:
        values = values * block_scale(stream_key, extent, pieces, -0.22, 0.18)
    return jnp.clip(with_spikes(values, jax.random.fold_in(stream_key, 3), *heavy), -most, most).astype(held_as)


def setup_inputs(seed: int = 0) -> dict:
    key_of = jax.random.split(jax.random.key(seed), 11)
    tokens = scatter_about(key_of[0], (STREAMS, LENGTH, D), 1.0, 6.0, ((0, 4), (1, 8)))
    doc_lengths = jax.vmap(lambda own: uneven(own, NDOC, LENGTH, MAXDOC, 2))(jax.random.split(key_of[1], STREAMS)).reshape((STREAMS, NDOC)).astype(jnp.int32)
    first_gain = jnp.clip(1.0 + 0.1 * jax.random.normal(key_of[2], (D,), jnp.float32), 0.5, 1.5)
    factor_weights = scatter_about(key_of[3], (D, FDIM), (D // 2) ** -0.5, 0.25, ((0, 32),), jnp.float32)
    output_weights = scatter_about(key_of[4], (HD, D), 16 ** -0.5, 1.5, ((0, 32),), jnp.float32)
    second_gain = jnp.clip(1.0 + 0.1 * jax.random.normal(key_of[5], (D,), jnp.float32), 0.5, 1.5)
    gate_weights = scatter_about(key_of[6], (D, FF), D ** -0.5, 0.1875, ((0, 32),), jnp.float32)
    up_weights = scatter_about(key_of[7], (D, FF), D ** -0.5, 0.1875, ((0, 32),), jnp.float32)
    down_weights = scatter_about(key_of[8], (FF, D), FF ** -0.5, 0.109375, ((0, 32),), jnp.float32)
    cotangent = noise_with(key_of[9], (STREAMS, LENGTH, D), 1.0, 6.0, ((0, 4), (1, 8)), (1, 2, 8, 2.0))
    return dict(tokens=tokens, doc_lengths=doc_lengths, first_gain=first_gain, factor_weights=factor_weights, output_weights=output_weights, second_gain=second_gain, gate_weights=gate_weights, up_weights=up_weights, down_weights=down_weights, cotangent=cotangent)


@jax.custom_vjp
def low(v):
    return lax.optimization_barrier(v.astype(jnp.bfloat16)).astype(jnp.float32)

@jax.custom_vjp
def low_back(v):
    return v

def low_keep(v):
    return (low(v), None)

def low_pass(kept, grad):
    return (grad,)

def back_keep(v):
    return (v, None)

def back_low(kept, grad):
    return (low(grad),)
low.defvjp(low_keep, low_pass)
low_back.defvjp(back_keep, back_low)
EPS = 1e-05
HIGH = lax.Precision.HIGHEST

def matmul(left, right):
    return jnp.dot(left, right, precision=HIGH, preferred_element_type=jnp.float32)

def rms_scale(values_in, gain):
    return values_in * lax.rsqrt(lax.optimization_barrier(jnp.mean(values_in * values_in, axis=-1, keepdims=True)) + EPS) * gain

def rope_tables(positions):
    inverse = 10000.0 ** (-(jnp.arange(DH // 2, dtype=jnp.float32) * 2.0 / DH))
    angles = positions[:, None] * inverse[None, :]
    return (jnp.cos(angles), jnp.sin(angles))

def rotate(vector, cosine, sine):
    half_width = vector.shape[-1] // 2
    lower_half = vector[..., :half_width]
    upper_half = vector[..., half_width:]
    return jnp.concatenate([lower_half * cosine - upper_half * sine, upper_half * cosine + lower_half * sine], axis=-1)

def stream_forward(inputs, lengths, gain_first, weight_fac, weight_out, gain_second, weight_gate, weight_up, weight_down):
    score_scale = DH ** (-0.5)
    normed_in = low(rms_scale(inputs, gain_first))
    factors = low_back(matmul(normed_in, weight_fac))
    edge_one = RQ * H
    edge_two = edge_one + RQ * DH
    edge_three = edge_two + RKV * H
    edge_four = edge_three + RKV * DH
    edge_five = edge_four + RKV * H
    cosine_table, sine_table = rope_tables(jnp.arange(LENGTH, dtype=jnp.float32))
    cos_rank = cosine_table[:, None, :]
    sin_rank = sine_table[:, None, :]
    a_query = factors[:, :edge_one].reshape(LENGTH, RQ, H)
    b_query = rotate(factors[:, edge_one:edge_two].reshape(LENGTH, RQ, DH), cos_rank, sin_rank)
    a_key = low(factors[:, edge_two:edge_three].reshape(LENGTH, RKV, H))
    b_key = low(rotate(factors[:, edge_three:edge_four].reshape(LENGTH, RKV, DH), cos_rank, sin_rank))
    a_value = low(factors[:, edge_four:edge_five].reshape(LENGTH, RKV, H))
    b_value = low(factors[:, edge_five:].reshape(LENGTH, RKV, DH))
    query = low(jnp.einsum('trh,tre->the', a_query, b_query, precision=HIGH) / RQ)
    keys = low(jnp.einsum('trh,tre->the', a_key, b_key, precision=HIGH) / RKV)
    values = low(jnp.einsum('trh,tre->the', a_value, b_value, precision=HIGH) / RKV)
    doc_ends = jnp.cumsum(lengths, dtype=jnp.int32)
    doc_starts = doc_ends - lengths
    places = jnp.arange(LENGTH, dtype=jnp.int32)
    docs = lax.optimization_barrier(jnp.sum((places[:, None] >= doc_starts[None, :]).astype(jnp.int32), axis=1, dtype=jnp.int32)) - 1
    span = min(512, LENGTH)
    reach = min(LENGTH, MAXDOC + span)

    def attend(block_index):
        first_query = block_index * span
        first_key = jnp.clip(first_query + span - reach, 0, LENGTH - reach).astype(jnp.int32)
        query_part = lax.dynamic_slice_in_dim(query, first_query, span, 0)
        key_part = lax.dynamic_slice_in_dim(keys, first_key, reach, 0)
        value_part = lax.dynamic_slice_in_dim(values, first_key, reach, 0)
        query_doc = lax.dynamic_slice_in_dim(docs, first_query, span, 0)
        key_doc = lax.dynamic_slice_in_dim(docs, first_key, reach, 0)
        query_pos = first_query + jnp.arange(span, dtype=jnp.int32)
        key_pos = first_key + jnp.arange(reach, dtype=jnp.int32)
        allowed = (query_doc[:, None] == key_doc[None, :]) & (key_pos[None, :] <= query_pos[:, None])
        score = low_back(jnp.einsum('qhe,khe->hqk', query_part, key_part, precision=HIGH) * score_scale)
        expo = jnp.where(allowed[None], jnp.exp(score), 0.0)
        total = lax.optimization_barrier(jnp.sum(expo, axis=-1))
        numer = low_back(jnp.einsum('hqk,khe->qhe', low(expo), value_part, precision=HIGH))
        return numer / total.T[:, :, None]
    blocks_out = lax.map(jax.checkpoint(attend), jnp.arange(LENGTH // span, dtype=jnp.int32))
    attn = low(blocks_out.reshape(LENGTH, H * DH))
    branch = low_back(matmul(attn, weight_out))
    middle = inputs + branch
    normed_mid = low(rms_scale(middle, gain_second))
    gate = low_back(matmul(normed_mid, weight_gate))
    upward = low_back(matmul(normed_mid, weight_up))
    hidden = low(jax.nn.silu(gate) * upward)
    return middle + low_back(matmul(hidden, weight_down))

def reference(tokens, doc_lengths, first_gain, factor_weights, output_weights, second_gain, gate_weights, up_weights, down_weights, cotangent):

    def forward(inputs, gain_a, weight_fac, weight_out, gain_b, weight_gate, weight_up, weight_down):
        low_gain_a = low(gain_a)
        low_fac = low(weight_fac)
        low_out = low(weight_out)
        low_gain_b = low(gain_b)
        low_gate = low(weight_gate)
        low_up = low(weight_up)
        low_down = low(weight_down)
        stream_fn = jax.checkpoint(stream_forward)

        def one_stream(carry, item):
            return (carry, stream_fn(item[0], item[1], low_gain_a, low_fac, low_out, low_gain_b, low_gate, low_up, low_down))
        unused, outputs = lax.scan(one_stream, jnp.zeros((), jnp.float32), (inputs, doc_lengths))
        return outputs
    result, pull = jax.vjp(forward, tokens.astype(jnp.float32), first_gain, factor_weights, output_weights, second_gain, gate_weights, up_weights, down_weights)
    grads = pull(cotangent.astype(jnp.float32))
    return (result.astype(jnp.bfloat16), grads[0].astype(jnp.bfloat16), grads[1], grads[2], grads[3], grads[4], grads[5], grads[6], grads[7])
```

```python
import functools

import jax
import jax.numpy as jnp
import numpy as np
from jax import lax
from jax.experimental import pallas as pl
from jax.experimental.pallas import tpu as pltpu
from jax.sharding import PartitionSpec as P

H = 16
DH = 64
RQ = 6
RKV = 2
EPS = 1e-05
BF = jnp.bfloat16
F32 = jnp.float32
AQ = RQ * H
BQ = RQ * DH
AK = RKV * H
BK = RKV * DH
PACK = 2 * (AK + BK)
KEY_ROWS = AK + BK
FDIM = AQ + BQ + PACK
FPAD = 896
LOG2E = 1.4426950408889634
NEG = -1e30


def nt(a, b):
    return lax.dot_general(a, b, (((1,), (1,)), ((), ())), preferred_element_type=F32)


def nn(a, b):
    return jnp.dot(a, b, preferred_element_type=F32)


def blocks(count, step, state):
    if count <= 8:
        for j in range(count):
            state = step(j, state)
        return state
    return lax.fori_loop(0, count, step, state)


def lane_block(j, size):
    if isinstance(j, int):
        return pl.ds(j * size, size)
    return pl.ds(pl.multiple_of(j * size, size), size)


def rope(b, cosine, sine, ranks):
    parts = []
    half = DH // 2
    for r in range(ranks):
        u1 = b[r * DH : r * DH + half]
        u2 = b[r * DH + half : (r + 1) * DH]
        parts += [u1 * cosine - u2 * sine, u2 * cosine + u1 * sine]
    return jnp.concatenate(parts, axis=0)


def rope_back(v, cosine, sine, ranks):
    return rope(v, cosine, -sine, ranks)


def pre_kernel(x_ref, g_ref, w_ref, cos_ref, sin_ref, nt_ref, q_ref, p_ref, a_ref, b_ref):
    x = x_ref[...].astype(F32)
    r1 = lax.rsqrt(jnp.mean(x * x, axis=-1, keepdims=True) + EPS)
    n = (x * r1 * g_ref[...]).astype(BF)
    nt_ref[...] = n.T
    ft = nn(n, w_ref[...]).T
    cosine, sine = cos_ref[...], sin_ref[...]
    a = ft[:AQ]
    b = rope(ft[AQ : AQ + BQ], cosine, sine, RQ)
    for i in range(AQ):
        a_ref[i] = a[i : i + 1]
    b_ref[...] = b
    k0 = AQ + BQ
    bk = rope(ft[k0 + AK : k0 + AK + BK], cosine, sine, RKV)
    p_ref[...] = jnp.concatenate(
        [ft[k0 : k0 + AK], bk, ft[k0 + KEY_ROWS : k0 + PACK]], axis=0
    ).astype(BF)
    for h in range(H):
        acc = a[h : h + 1] * b[:DH]
        for r in range(1, RQ):
            acc = acc + a[r * H + h : r * H + h + 1] * b[r * DH : (r + 1) * DH]
        q_ref[h * DH : (h + 1) * DH, :] = (acc * (1.0 / RQ)).astype(BF)


def expand_pair(ka, kb, side, p, lanes):
    rows = []
    for hh in range(2):
        acc = 0.0
        for r in range(RKV):
            a = ka[side * AK + r * H + 2 * p + hh, :, lanes]
            b = kb[side * BK + r * DH : side * BK + (r + 1) * DH, lanes]
            acc = acc + a * b
        rows.append(acc * (1.0 / RKV))
    return jnp.concatenate(rows, axis=0)


def unpack(kv_ref, ka, kb):
    for side in range(2):
        first = side * KEY_ROWS
        a = kv_ref[first : first + AK, :].astype(F32)
        for i in range(AK):
            ka[side * AK + i] = a[i : i + 1]
        kb[side * BK : (side + 1) * BK, :] = kv_ref[first + AK : first + KEY_ROWS, :].astype(F32)


def diagonal(pair):
    zero = jnp.zeros((DH, pair.shape[1]), pair.dtype)
    left = jnp.concatenate([pair[:DH], zero], axis=0)
    right = jnp.concatenate([zero, pair[DH:]], axis=0)
    return jnp.concatenate([left, right], axis=1)


def undiagonal(wide):
    t = wide.shape[1] // 2
    return jnp.concatenate([wide[:DH, :t], wide[DH:, t:]], axis=0)


def attend_kernel(nblk, base_ref, len_ref, q_ref, kv_ref, at_ref, af_ref, inv_ref, p_ref, ka, kb, bias):
    t = q_ref.shape[1]
    c = lax.axis_index("ctx")
    tpos = c * t + lax.broadcasted_iota(jnp.int32, (1, t), 1)
    start = jnp.zeros((1, t), jnp.int32)
    run = jnp.int32(0)
    for j in range(len_ref.shape[1]):
        start = jnp.where(tpos >= run, run, start)
        run = run + len_ref[0, j]
    unpack(kv_ref, ka, kb)

    def bias_block(j, _):
        spos = base_ref[0] + j * t + lax.broadcasted_iota(jnp.int32, (t, t), 0)
        ok = (spos >= start) & (spos <= tpos)
        bias[lane_block(j, t), :] = jnp.where(ok, 0.0, NEG)
        return _

    blocks(nblk, bias_block, 0)

    def pair(p, _):
        rows = pl.ds(pl.multiple_of(p * 2 * DH, 2 * DH), 2 * DH)
        qd = diagonal(q_ref[rows, :])

        def step(j, state):
            num, tot = state
            lanes = lane_block(j, t)
            k = expand_pair(ka, kb, 0, p, lanes).T.astype(BF)
            v = expand_pair(ka, kb, 1, p, lanes).astype(BF)
            b = bias[lanes, :]
            s = nn(k, qd) * (LOG2E * DH**-0.5) + jnp.concatenate([b, b], axis=1)
            e = jnp.exp2(s)
            tot = tot + jnp.sum(e, axis=0, keepdims=True)
            pb = e.astype(BF)
            p_ref[p, lanes, :] = pb
            return (num + nn(v, pb), tot)

        num, tot = blocks(
            nblk, step, (jnp.zeros((2 * DH, 2 * t), F32), jnp.zeros((1, 2 * t), F32))
        )
        inv = 1.0 / tot
        af = undiagonal(num * inv)
        af_ref[rows, :] = af
        at_ref[rows, :] = af.astype(BF)
        inv_ref[p] = jnp.broadcast_to(inv, (8, 2 * t))
        return _

    lax.fori_loop(0, H // 2, pair, 0)


def attend_back_kernel(
    nblk, da_ref, af_ref, inv_ref, p_ref, q_ref, kv_ref, a_ref, b_ref, cos_ref, sin_ref,
    dq_ref, dkv_ref, ka, kb, dka, dqa, db,
):
    t = q_ref.shape[1]
    unpack(kv_ref, ka, kb)
    db[...] = jnp.zeros_like(db)
    for side in range(2):
        first = side * KEY_ROWS + AK
        dkv_ref[first : first + BK, :] = jnp.zeros((BK, nblk * t), F32)

    def factor_back(dwide, side, p, lanes):
        for hh in range(2):
            d = dwide[hh * DH : (hh + 1) * DH] * (1.0 / RKV)
            for r in range(RKV):
                row = side * AK + r * H + 2 * p + hh
                first = side * KEY_ROWS + AK + r * DH
                b = kb[side * BK + r * DH : side * BK + (r + 1) * DH, lanes]
                dka[row, :, lanes] = jnp.sum(d * b, axis=0, keepdims=True)
                dkv_ref[first : first + DH, lanes] += d * ka[row, :, lanes]

    def pair(p, _):
        rows = pl.ds(pl.multiple_of(p * 2 * DH, 2 * DH), 2 * DH)
        da = da_ref[rows, :]
        inv = inv_ref[p][:1]
        dd = diagonal(da)
        dn = (dd * inv).astype(BF)
        dtot = -jnp.sum(dd * diagonal(af_ref[rows, :]), axis=0, keepdims=True) * inv
        qd = diagonal(q_ref[rows, :])

        def step(j, dq):
            lanes = lane_block(j, t)
            k = expand_pair(ka, kb, 0, p, lanes).astype(BF)
            v = expand_pair(ka, kb, 1, p, lanes).T.astype(BF)
            pb = p_ref[p, lanes, :]
            ds = (pb.astype(F32) * (nn(v, dn) + dtot)).astype(BF)
            dq = dq + nn(k, ds)
            factor_back(nt(qd, ds) * (DH**-0.5), 0, p, lanes)
            factor_back(nt(dn, pb), 1, p, lanes)
            return dq

        dq = undiagonal(blocks(nblk, step, jnp.zeros((2 * DH, 2 * t), F32)))
        dq = dq * (DH**-0.5 / RQ)
        for hh in range(2):
            d = dq[hh * DH : (hh + 1) * DH]
            for r in range(RQ):
                row = r * H + 2 * p + hh
                dqa[row] = jnp.sum(d * b_ref[r * DH : (r + 1) * DH, :], axis=0, keepdims=True)
                db[r * DH : (r + 1) * DH, :] += d * a_ref[row]
        return _

    lax.fori_loop(0, H // 2, pair, 0)
    for i in range(AQ):
        dq_ref[i : i + 1, :] = dqa[i]
    for side in range(2):
        for i in range(AK):
            dkv_ref[side * KEY_ROWS + i : side * KEY_ROWS + i + 1, :] = dka[side * AK + i]
    dq_ref[AQ : AQ + BQ, :] = rope_back(db[...], cos_ref[...], sin_ref[...], RQ)


def vmem(n):
    return [pl.BlockSpec(memory_space=pltpu.VMEM)] * n


SMEM = pl.BlockSpec(memory_space=pltpu.SMEM)


def silu_parts(gate):
    s = jax.nn.sigmoid(gate)
    return s, gate * s


def body(
    tokens,
    doc_lengths,
    first_gain,
    factor_weights,
    output_weights,
    second_gain,
    gate_weights,
    up_weights,
    down_weights,
    cotangent,
):
    _, t, width = tokens.shape
    n_ctx, n_dp = lax.axis_size("ctx"), lax.axis_size("dp")
    n_all = n_ctx * n_dp
    both = ("dp", "ctx")
    length = t * n_ctx
    nblk = min(n_ctx, -(-(length // 2 - 1) // t) + 1)
    ff = gate_weights.shape[1]
    ffq = ff // n_dp
    rows = width // n_all
    c = lax.axis_index("ctx")

    pack = jnp.concatenate(
        [factor_weights, first_gain[:, None], second_gain[:, None],
         jnp.zeros((rows, FPAD - FDIM - 2), F32)], axis=1).astype(BF)
    fac = lax.all_gather(pack, both, axis=0, tiled=True)
    wo = lax.all_gather(output_weights.astype(BF), both, axis=0, tiled=True)
    gu = jnp.stack([gate_weights, up_weights]).astype(BF).reshape(2, rows, n_dp, ffq)
    gu = lax.all_to_all(gu.transpose(2, 0, 1, 3), "dp", 0, 0, tiled=False)
    gu = lax.all_gather(gu, "ctx", axis=2, tiled=False)
    gu = gu.transpose(1, 0, 2, 3, 4).reshape(2, width, ffq)
    wg, wu = gu[0], gu[1]
    wd = lax.all_gather(down_weights.astype(BF), "ctx", axis=0, tiled=True)
    g1 = fac[:, FDIM].reshape(1, width).astype(F32)
    g2 = fac[:, FDIM + 1].reshape(1, width).astype(F32)

    half = DH // 2
    freq = 10000.0 ** (-(np.arange(half) * 2.0 / DH))
    pos = (c * t + jnp.arange(t, dtype=jnp.int32)).astype(F32)
    angles = jnp.asarray(freq, F32)[:, None] * pos[None, :]
    cosine, sine = jnp.cos(angles), jnp.sin(angles)

    x16 = tokens.reshape(t, width)
    normed_t, q_t, packet, a_t, b_t = pl.pallas_call(
        pre_kernel,
        out_shape=(
            jax.ShapeDtypeStruct((width, t), BF),
            jax.ShapeDtypeStruct((H * DH, t), BF),
            jax.ShapeDtypeStruct((PACK, t), BF),
            jax.ShapeDtypeStruct((AQ, 1, t), F32),
            jax.ShapeDtypeStruct((BQ, t), F32),
        ),
        in_specs=vmem(5),
        out_specs=tuple(vmem(5)),
        name="pre",
    )(x16, g1, fac, cosine, sine)

    whole = lax.all_gather(packet, "ctx", axis=1, tiled=True)
    base = jnp.maximum(c - nblk + 1, 0) * t
    kv = lax.dynamic_slice_in_dim(whole, base, nblk * t, 1)
    attn_t, attn_f, inv, probs = pl.pallas_call(
        functools.partial(attend_kernel, nblk),
        out_shape=(
            jax.ShapeDtypeStruct((H * DH, t), BF),
            jax.ShapeDtypeStruct((H * DH, t), F32),
            jax.ShapeDtypeStruct((H // 2, 8, 2 * t), F32),
            jax.ShapeDtypeStruct((H // 2, nblk * t, 2 * t), BF),
        ),
        in_specs=[SMEM, SMEM] + vmem(2),
        out_specs=tuple(vmem(4)),
        scratch_shapes=[
            pltpu.VMEM((2 * AK, 1, nblk * t), F32),
            pltpu.VMEM((2 * BK, nblk * t), F32),
            pltpu.VMEM((nblk * t, t), F32),
        ],
        name="attend",
    )(base[None], doc_lengths, q_t, kv)

    x = x16.astype(F32)
    middle = x + nn(attn_t.T, wo)
    r2 = lax.rsqrt(jnp.mean(middle * middle, axis=-1, keepdims=True) + EPS)
    nm = (middle * r2 * g2).astype(BF)
    cot_own = cotangent.reshape(t, width)
    cot = lax.all_gather(cot_own, "dp", axis=0, tiled=True)
    nm_all = lax.all_gather(nm, "dp", axis=0, tiled=True)
    gate = nn(nm_all, wg)
    upward = nn(nm_all, wu)
    sig, act = silu_parts(gate)
    hidden = (act * upward).astype(BF)
    d_hidden = nt(cot, wd)
    d_gate = (d_hidden * upward * sig * (1.0 + gate * (1.0 - sig))).astype(BF)
    d_up = (d_hidden * act).astype(BF)
    dn_part = nt(d_gate, wg) + nt(d_up, wu)
    d_norm_mid = lax.psum_scatter(dn_part.astype(BF), "dp", scatter_dimension=0, tiled=True).astype(F32)
    out_part = nn(hidden, wd)
    out_sum = lax.psum_scatter(out_part.astype(BF), "dp", scatter_dimension=0, tiled=True)
    layer_output = (middle + out_sum.astype(F32)).astype(BF)

    def tn(a, b):
        return lax.dot_general(a, b, (((0,), (0,)), ((), ())), preferred_element_type=F32)

    gu_part = jnp.stack([tn(nm_all, d_gate), tn(nm_all, d_up)]).astype(BF)
    gu_part = gu_part.reshape(2, n_dp, n_ctx, rows, ffq).transpose(2, 1, 0, 3, 4)
    gu_part = gu_part.reshape(n_ctx * n_dp * 2 * rows, ffq)
    gu_own = lax.psum_scatter(gu_part, "ctx", scatter_dimension=0, tiled=True)
    gu_own = gu_own.reshape(n_dp, 2, rows, ffq)
    gu_own = lax.all_to_all(gu_own, "dp", 0, 0, tiled=False)
    gu_own = gu_own.astype(F32).transpose(1, 2, 0, 3).reshape(2, rows, ff)
    down_sum = lax.psum_scatter(
        tn(hidden, cot).astype(BF), "ctx", scatter_dimension=0, tiled=True
    ).astype(F32)

    second_part = jnp.sum(d_norm_mid * middle * r2, axis=0)
    u2 = d_norm_mid * g2
    d_middle = (
        cot_own.astype(F32)
        + r2 * u2
        - middle * (r2**3 * jnp.mean(u2 * middle, axis=-1, keepdims=True))
    )
    d_branch = d_middle.astype(BF)
    d_attn_t = nt(wo, d_branch)
    out_grad_part = nn(attn_t, d_branch)

    dq_rows, dkv = pl.pallas_call(
        functools.partial(attend_back_kernel, nblk),
        out_shape=(
            jax.ShapeDtypeStruct((AQ + BQ, t), F32),
            jax.ShapeDtypeStruct((PACK, nblk * t), F32),
        ),
        in_specs=vmem(10),
        out_specs=tuple(vmem(2)),
        scratch_shapes=[
            pltpu.VMEM((2 * AK, 1, nblk * t), F32),
            pltpu.VMEM((2 * BK, nblk * t), F32),
            pltpu.VMEM((2 * AK, 1, nblk * t), F32),
            pltpu.VMEM((AQ, 1, t), F32),
            pltpu.VMEM((BQ, t), F32),
        ],
        name="attend_back",
    )(d_attn_t, attn_f, inv, probs, q_t, kv, a_t, b_t, cosine, sine)

    spread = lax.dynamic_update_slice_in_dim(
        jnp.zeros((PACK, length), BF), dkv.astype(BF), base, 1
    )
    d_packet = lax.psum_scatter(spread, "ctx", scatter_dimension=1, tiled=True).astype(F32)
    d_bk = rope_back(d_packet[AK : AK + BK], cosine, sine, RKV)
    d_fac_t = jnp.concatenate([dq_rows, d_packet[:AK], d_bk, d_packet[KEY_ROWS:]], axis=0).astype(BF)
    d_fac = d_fac_t.T
    d_norm_in = nt(d_fac, fac[:, :FDIM])
    r1 = lax.rsqrt(jnp.mean(x * x, axis=-1, keepdims=True) + EPS)
    first_part = jnp.sum(d_norm_in * x * r1, axis=0)
    u1 = d_norm_in * g1
    input_grad = (
        d_middle + r1 * u1 - x * (r1**3 * jnp.mean(u1 * x, axis=-1, keepdims=True))
    ).astype(BF)
    fac_part = nt(normed_t, d_fac_t)
    out_own = lax.psum_scatter(out_grad_part.astype(BF), both, scatter_dimension=0, tiled=True)
    last = jnp.concatenate(
        [fac_part, first_part[:, None], second_part[:, None],
         jnp.zeros((width, FPAD - FDIM - 2), F32)], axis=1).astype(BF)
    last_own = lax.psum_scatter(last, both, scatter_dimension=0, tiled=True).astype(F32)
    return (
        layer_output.reshape(1, t, width),
        input_grad.reshape(1, t, width),
        last_own[:, FDIM],
        last_own[:, :FDIM],
        out_own.astype(F32),
        last_own[:, FDIM + 1],
        gu_own[0],
        gu_own[1],
        down_sum,
    )


def solution(mesh):
    return jax.shard_map(
        body,
        mesh=mesh,
        in_specs=(
            P("dp", "ctx", None),
            P("dp", None),
            P(("dp", "ctx")),
            P(("dp", "ctx"), None),
            P(("dp", "ctx"), None),
            P(("dp", "ctx")),
            P(("dp", "ctx"), None),
            P(("dp", "ctx"), None),
            P(("dp", "ctx"), None),
            P("dp", "ctx", None),
        ),
        out_specs=(
            P("dp", "ctx", None),
            P("dp", "ctx", None),
            P(("dp", "ctx")),
            P(("dp", "ctx"), None),
            P(("dp", "ctx"), None),
            P(("dp", "ctx")),
            P(("dp", "ctx"), None),
            P(("dp", "ctx"), None),
            P(("dp", "ctx"), None),
        ),
        check_vma=False,
    )
```

```python
import functools

import jax
import jax.numpy as jnp
import numpy as np
from jax import lax
from jax.experimental import pallas as pl
from jax.experimental.pallas import tpu as pltpu
from jax.sharding import PartitionSpec as P

H = 16
DH = 64
RQ = 6
RKV = 2
EPS = 1e-05
BF = jnp.bfloat16
F32 = jnp.float32
AQ = RQ * H
BQ = RQ * DH
AK = RKV * H
BK = RKV * DH
PACK = 2 * (AK + BK)
KEY_ROWS = AK + BK
FDIM = AQ + BQ + PACK
FPAD = 896
LOG2E = 1.4426950408889634
NEG = -1e30


def nt(a, b):
    return lax.dot_general(a, b, (((1,), (1,)), ((), ())), preferred_element_type=F32)


def nn(a, b):
    return jnp.dot(a, b, preferred_element_type=F32)

MESH = pl.DeviceIdType.MESH


def ring_place(c, n):
    z = c // 2
    return z + (c % 2) * (n - 1 - 2 * z)


def ring_index(p, n):
    p = (p + 2 * n) % n
    q = p // (n // 2)
    return (1 - q) * (2 * p) + q * (2 * (n - 1 - p) + 1)


def remote(src, dst, send, recv, dev):
    return pltpu.make_async_remote_copy(
        src_ref=src, dst_ref=dst, send_sem=send, recv_sem=recv, device_id=dev, device_id_type=MESH
    )


def places():
    d, c = lax.axis_index("dp"), lax.axis_index("ctx")
    core = d % 2
    return d, c, core, d + 1 - 2 * core, (d + 2) % 4


def meet(n, near):
    d, c, _, _, _ = places()
    barrier = pltpu.get_barrier_semaphore()
    count = 0
    n_dp = lax.axis_size("dp")
    for k in range(1, n_dp):
        pl.semaphore_signal(barrier, inc=1, device_id=((d + k) % n_dp, c), device_id_type=MESH)
        count += 1
    if near:
        r = ring_place(c, n)
        for way in (1, -1):
            pl.semaphore_signal(
                barrier, inc=1, device_id=(d, ring_index(r + way, n)), device_id_type=MESH
            )
            count += 1
    else:
        for k in range(1, n):
            pl.semaphore_signal(barrier, inc=1, device_id=(d, (c + k) % n), device_id_type=MESH)
            count += 1
    pl.semaphore_wait(barrier, count)


def steps(lo, hi, step):
    if isinstance(lo, int) and isinstance(hi, int) and hi - lo <= 4:
        for s in range(lo, hi):
            step(s)
    elif not (isinstance(lo, int) and isinstance(hi, int) and hi <= lo):
        lax.fori_loop(lo, hi, lambda s, _: (step(s), _)[1], 0)


class GatherRing:
    def __init__(self, n, slot, half, send, recv):
        self.n, self.h, self.slot, self.half, self.send, self.recv = n, n // 2, slot, half, send, recv
        self.d, c, _, _, _ = places()
        self.r = ring_place(c, n)

    def copy(self, s, i, arriving=False):
        way = 1 - 2 * i
        last = isinstance(s, int) and s == self.h - 1
        owner = ring_index(self.r - way * (s + (1 if arriving else 0)), self.n)
        ref = self.half(owner, i) if last else self.slot(owner)
        to = (self.d, ring_index(self.r + way, self.n))
        return remote(ref, ref, self.send.at[i, s], self.recv.at[i, s], to)

    def start(self, s):
        for i in range(2):
            self.copy(s, i).start()

    def arrive(self, s):
        for i in range(2):
            self.copy(s, i, True).wait_recv()

    def step(self, s):
        for i in range(2):
            self.copy(s - 1, i, True).wait_recv()
            self.copy(s, i).start()

    def last(self):
        self.step(self.h - 1)

    def drain(self):
        steps(0, self.h - 1, lambda s: [self.copy(s, i).wait_send() for i in range(2)])
        for i in range(2):
            self.copy(self.h - 1, i).wait_send()


class ScatterRing:
    def __init__(self, n, part, half, land, whole_of, half_of, send, recv):
        self.n, self.h, self.part, self.half = n, n // 2, part, half
        self.land, self.whole_of, self.half_of = land, whole_of, half_of
        self.send, self.recv = send, recv
        self.d, c, _, _, _ = places()
        self.c, self.r = c, ring_place(c, n)

    def copy(self, s, i):
        way = 1 - 2 * i
        to = (self.d, ring_index(self.r + way, self.n))
        first = isinstance(s, int) and s == 0
        if first:
            owner = ring_index(self.r + way * self.h, self.n)
            src, dst = self.half(owner, i), self.half_of(self.land.at[i, 0], i)
        else:
            src, dst = self.land.at[i, s - 1], self.land.at[i, s]
        return remote(src, dst, self.send.at[i, s], self.recv.at[i, s], to)

    def start(self):
        for i in range(2):
            self.copy(0, i).start()

    def step(self, s):
        first = isinstance(s, int) and s == 1
        for i in range(2):
            way = 1 - 2 * i
            self.copy(s - 1, i).wait_recv()
            owner = ring_index(self.r + way * (self.h - s), self.n)
            held = self.land.at[i, s - 1]
            if first:
                mine = self.half_of(held, i)
                mine[...] = (mine[...].astype(F32) + self.half(owner, i)[...].astype(F32)).astype(BF)
                self.half_of(held, 1 - i)[...] = self.half(owner, 1 - i)[...]
            else:
                held[...] = (held[...].astype(F32) + self.part(owner)[...].astype(F32)).astype(BF)
            self.copy(s, i).start()

    def rest(self, lo, hi):
        if lo == 1 and hi > 1:
            self.step(1)
            lo = 2
        steps(lo, hi, self.step)

    def result(self):
        for i in range(2):
            self.copy(self.h - 1, i).wait_recv()
        out = self.part(self.c)[...].astype(F32)
        for i in range(2):
            out = out + self.land[i, self.h - 1].astype(F32)
        return out

    def drain(self):
        for i in range(2):
            self.copy(0, i).wait_send()
        steps(1, self.h, lambda s: [self.copy(s, i).wait_send() for i in range(2)])


class Spread:
    def __init__(self, ref, send, recv):
        d, c, _, cd, xd = places()
        self.copies = [
            remote(ref.at[d], ref.at[d], send.at[0], recv.at[0], (cd, c)),
            remote(ref.at[d], ref.at[d], send.at[1], recv.at[1], (xd, c)),
            remote(ref.at[xd], ref.at[xd], send.at[2], recv.at[2], (cd, c)),
        ]

    def start(self):
        self.copies[1].start()
        self.copies[0].start()

    def forward(self):
        self.copies[1].wait_recv()
        self.copies[2].start()

    def finish(self):
        self.copies[0].wait_recv()
        self.copies[2].wait_recv()
        for copy in self.copies:
            copy.wait_send()


def blocks(count, step, state):
    if count <= 8:
        for j in range(count):
            state = step(j, state)
        return state
    return lax.fori_loop(0, count, step, state)


def lane_block(j, size):
    if isinstance(j, int):
        return pl.ds(j * size, size)
    return pl.ds(pl.multiple_of(j * size, size), size)


def rope(b, cosine, sine, ranks):
    parts = []
    half = DH // 2
    for r in range(ranks):
        u1 = b[r * DH : r * DH + half]
        u2 = b[r * DH + half : (r + 1) * DH]
        parts += [u1 * cosine - u2 * sine, u2 * cosine + u1 * sine]
    return jnp.concatenate(parts, axis=0)


def rope_back(v, cosine, sine, ranks):
    return rope(v, cosine, -sine, ranks)


def pre_part(x, g1, w, cosine, sine, nt_ref, q_ref, p_ref, a_ref, b_ref):
    r1 = lax.rsqrt(jnp.mean(x * x, axis=-1, keepdims=True) + EPS)
    n = (x * r1 * g1).astype(BF)
    nt_ref[...] = n.T
    ft = nn(n, w).T
    a = ft[:AQ]
    b = rope(ft[AQ : AQ + BQ], cosine, sine, RQ)
    for i in range(AQ):
        a_ref[i] = a[i : i + 1]
    b_ref[...] = b
    k0 = AQ + BQ
    bk = rope(ft[k0 + AK : k0 + AK + BK], cosine, sine, RKV)
    p_ref[...] = jnp.concatenate(
        [ft[k0 : k0 + AK], bk, ft[k0 + KEY_ROWS : k0 + PACK]], axis=0
    ).astype(BF)
    for h in range(H):
        acc = a[h : h + 1] * b[:DH]
        for r in range(1, RQ):
            acc = acc + a[r * H + h : r * H + h + 1] * b[r * DH : (r + 1) * DH]
        q_ref[h * DH : (h + 1) * DH, :] = (acc * (1.0 / RQ)).astype(BF)


def expand_pair(ka, kb, side, p, lanes):
    rows = []
    for hh in range(2):
        acc = 0.0
        for r in range(RKV):
            a = ka[side * AK + r * H + 2 * p + hh, :, lanes]
            b = kb[side * BK + r * DH : side * BK + (r + 1) * DH, lanes]
            acc = acc + a * b
        rows.append(acc * (1.0 / RKV))
    return jnp.concatenate(rows, axis=0)


def unpack(kv_ref, ka, kb):
    for side in range(2):
        first = side * KEY_ROWS
        a = kv_ref[first : first + AK, :].astype(F32)
        for i in range(AK):
            ka[side * AK + i] = a[i : i + 1]
        kb[side * BK : (side + 1) * BK, :] = kv_ref[first + AK : first + KEY_ROWS, :].astype(F32)


def diagonal(pair):
    zero = jnp.zeros((DH, pair.shape[1]), pair.dtype)
    left = jnp.concatenate([pair[:DH], zero], axis=0)
    right = jnp.concatenate([zero, pair[DH:]], axis=0)
    return jnp.concatenate([left, right], axis=1)


def undiagonal(wide):
    t = wide.shape[1] // 2
    return jnp.concatenate([wide[:DH, :t], wide[DH:, t:]], axis=0)


def attend_part(nblk, len_ref, q_ref, kv_ref, at_ref, af_ref, inv_ref, p_ref, ka, kb, bias):
    t = q_ref.shape[1]
    c = lax.axis_index("ctx")
    tpos = c * t + lax.broadcasted_iota(jnp.int32, (1, t), 1)
    start = jnp.zeros((1, t), jnp.int32)
    run = jnp.int32(0)
    for j in range(len_ref.shape[1]):
        start = jnp.where(tpos >= run, run, start)
        run = run + len_ref[0, j]
    unpack(kv_ref, ka, kb)

    def bias_block(j, _):
        spos = (c - nblk + 1 + j) * t + lax.broadcasted_iota(jnp.int32, (t, t), 0)
        ok = (spos >= start) & (spos <= tpos)
        bias[lane_block(j, t), :] = jnp.where(ok, 0.0, NEG)
        return _

    blocks(nblk, bias_block, 0)

    def pair(p, _):
        rows = pl.ds(pl.multiple_of(p * 2 * DH, 2 * DH), 2 * DH)
        qd = diagonal(q_ref[rows, :])

        def step(j, state):
            num, tot = state
            lanes = lane_block(j, t)
            k = expand_pair(ka, kb, 0, p, lanes).T.astype(BF)
            v = expand_pair(ka, kb, 1, p, lanes).astype(BF)
            b = bias[lanes, :]
            s = nn(k, qd) * (LOG2E * DH**-0.5) + jnp.concatenate([b, b], axis=1)
            e = jnp.exp2(s)
            tot = tot + jnp.sum(e, axis=0, keepdims=True)
            pb = e.astype(BF)
            p_ref[p, lanes, :] = pb
            return (num + nn(v, pb), tot)

        num, tot = blocks(
            nblk, step, (jnp.zeros((2 * DH, 2 * t), F32), jnp.zeros((1, 2 * t), F32))
        )
        inv = 1.0 / tot
        af = undiagonal(num * inv)
        af_ref[rows, :] = af
        at_ref[rows, :] = af.astype(BF)
        inv_ref[p] = jnp.broadcast_to(inv, (8, 2 * t))
        return _

    lax.fori_loop(0, H // 2, pair, 0)


def attend_back_part(
    nblk, serve, da_ref, af_ref, inv_ref, p_ref, q_ref, kv_ref, a_ref, b_ref, cos_ref, sin_ref,
    dq_ref, dkv_ref, ka, kb, dka, dqa, db,
):
    t = q_ref.shape[1]
    unpack(kv_ref, ka, kb)
    db[...] = jnp.zeros_like(db)
    for side in range(2):
        first = side * KEY_ROWS + AK
        dkv_ref[first : first + BK, :] = jnp.zeros((BK, nblk * t), F32)

    def factor_back(dwide, side, p, lanes):
        for hh in range(2):
            d = dwide[hh * DH : (hh + 1) * DH] * (1.0 / RKV)
            for r in range(RKV):
                row = side * AK + r * H + 2 * p + hh
                first = side * KEY_ROWS + AK + r * DH
                b = kb[side * BK + r * DH : side * BK + (r + 1) * DH, lanes]
                dka[row, :, lanes] = jnp.sum(d * b, axis=0, keepdims=True)
                dkv_ref[first : first + DH, lanes] += d * ka[row, :, lanes]

    def pair(p, _):
        rows = pl.ds(pl.multiple_of(p * 2 * DH, 2 * DH), 2 * DH)
        da = da_ref[rows, :]
        inv = inv_ref[p][:1]
        dd = diagonal(da)
        dn = (dd * inv).astype(BF)
        dtot = -jnp.sum(dd * diagonal(af_ref[rows, :]), axis=0, keepdims=True) * inv
        qd = diagonal(q_ref[rows, :])

        def step(j, dq):
            lanes = lane_block(j, t)
            k = expand_pair(ka, kb, 0, p, lanes).astype(BF)
            v = expand_pair(ka, kb, 1, p, lanes).T.astype(BF)
            pb = p_ref[p, lanes, :]
            ds = (pb.astype(F32) * (nn(v, dn) + dtot)).astype(BF)
            dq = dq + nn(k, ds)
            factor_back(nt(qd, ds) * (DH**-0.5), 0, p, lanes)
            factor_back(nt(dn, pb), 1, p, lanes)
            return dq

        dq = undiagonal(blocks(nblk, step, jnp.zeros((2 * DH, 2 * t), F32)))
        dq = dq * (DH**-0.5 / RQ)
        for hh in range(2):
            d = dq[hh * DH : (hh + 1) * DH]
            for r in range(RQ):
                row = r * H + 2 * p + hh
                dqa[row] = jnp.sum(d * b_ref[r * DH : (r + 1) * DH, :], axis=0, keepdims=True)
                db[r * DH : (r + 1) * DH, :] += d * a_ref[row]
        serve(p)
        return _

    lax.fori_loop(0, H // 2, pair, 0)
    for i in range(AQ):
        dq_ref[i : i + 1, :] = dqa[i]
    for side in range(2):
        for i in range(AK):
            dkv_ref[side * KEY_ROWS + i : side * KEY_ROWS + i + 1, :] = dka[side * AK + i]
    dq_ref[AQ : AQ + BQ, :] = rope_back(db[...], cos_ref[...], sin_ref[...], RQ)


def front_kernel(
    n, nblk,
    len_ref, x_ref, cos_ref, sin_ref, fac_in, wo_in, gu_in, wd_in, cot_in,
    nt_ref, q_ref, a_ref, b_ref, kv_ref, at_ref, af_ref, inv_ref, p_ref,
    fac, wo, gu, wd, nm, cot, mid_ref,
    ka, kb, bias,
    own_sem, near_send, near_recv, ring_send, ring_recv, kv_send, kv_recv, sp_send, sp_recv,
):
    d, c, core, cd, xd = places()
    t = x_ref.shape[0]
    n_dp = 4
    locals_ = [
        pltpu.make_async_copy(fac_in, fac.at[d, c], own_sem.at[0]),
        pltpu.make_async_copy(wo_in, wo.at[d, c], own_sem.at[1]),
        pltpu.make_async_copy(gu_in.at[d], gu.at[:, d, c], own_sem.at[2]),
        pltpu.make_async_copy(wd_in, wd.at[c], own_sem.at[3]),
        pltpu.make_async_copy(cot_in, cot.at[d], own_sem.at[4]),
    ]
    for copy in locals_:
        copy.start()
    for k in range(1, nblk):
        @pl.when(c - k < 0)
        def _():
            kv_ref[:, (nblk - 1 - k) * t : (nblk - k) * t] = jnp.zeros((PACK, t), BF)
    meet(n, False)
    for copy in locals_:
        copy.wait()

    def ring(i, slot, half):
        return GatherRing(n, slot, half, ring_send.at[i], ring_recv.at[i])

    rows = fac_in.shape[0] // 2

    def shard(ref, dd):
        return (lambda o: ref.at[dd, o]), (lambda o, w: ref.at[dd, o, w * rows : (w + 1) * rows])

    fo, fx = ring(0, *shard(fac, d)), ring(1, *shard(fac, xd))
    oo, ox = ring(2, *shard(wo, d)), ring(3, *shard(wo, xd))
    cut = -(-wd_in.shape[0] // 16) * 8
    gr = ring(4, lambda o: gu.at[:, :, o], lambda o, w: gu.at[w, :, o])
    dr = ring(
        5, lambda o: wd.at[o],
        lambda o, w: wd.at[o, :cut] if w == 0 else wd.at[o, cut:],
    )
    fswap = remote(fac.at[d, c], fac.at[d, c], near_send.at[0], near_recv.at[0], (xd, c))
    oswap = remote(wo.at[d, c], wo.at[d, c], near_send.at[1], near_recv.at[1], (xd, c))
    fswap.start()
    fo.start(0)
    oswap.start()
    a2a = []
    for k in range(1, n_dp):
        to = (d + k) % n_dp
        a2a.append(
            (
                remote(gu_in.at[to], gu.at[:, d, c], near_send.at[1 + k], near_recv.at[1 + k], (to, c)),
                remote(
                    gu_in.at[to], gu.at[:, (d + n_dp - k) % n_dp, c],
                    near_send.at[1 + k], near_recv.at[1 + k], (to, c),
                ),
            )
        )
        a2a[-1][0].start()
    cots = Spread(cot, sp_send.at[0], sp_recv.at[0])
    nms = Spread(nm, sp_send.at[1], sp_recv.at[1])
    cots.start()
    fswap.wait_recv()
    fx.start(0)
    for s in range(1, n // 2 - 1) if n <= 8 else ():
        fo.step(s)
        fx.step(s)
    if n > 8:
        steps(1, n // 2 - 1, lambda s: (fo.step(s), fx.step(s)))
    fo.last()
    fx.last()
    oswap.wait_recv()
    for _, arrival in a2a:
        arrival.wait_recv()
    rest = (gr, dr, oo, ox)
    for one in rest:
        one.start(0)
    fo.arrive(n // 2 - 1)
    fx.arrive(n // 2 - 1)
    fcore = [
        (
            remote(fac.at[dd], fac.at[dd], near_send.at[5 + i], near_recv.at[5 + i], (cd, c)),
            remote(fac.at[da], fac.at[da], near_send.at[5 + i], near_recv.at[5 + i], (cd, c)),
        )
        for i, (dd, da) in enumerate(((d, cd), (xd, (cd + 2) % 4)))
    ]
    for out, _ in fcore:
        out.start()
    cots.forward()
    for _, arrival in fcore:
        arrival.wait_recv()

    width = x_ref.shape[1]
    x = x_ref[...].astype(F32)
    w = fac[...].reshape(width, FPAD)
    gains = w[:, FPAD - 128 :].astype(F32).T
    g1 = gains[FDIM - (FPAD - 128) : FDIM - (FPAD - 128) + 1]
    g2 = gains[FDIM - (FPAD - 128) + 1 : FDIM - (FPAD - 128) + 2]
    own_kv = kv_ref.at[:, (nblk - 1) * t : nblk * t]
    pre_part(x, g1, w, cos_ref[...], sin_ref[...], nt_ref, q_ref, own_kv, a_ref, b_ref)

    def kv_copy(k):
        dst = kv_ref.at[:, (nblk - 1 - k) * t : (nblk - k) * t]
        return remote(own_kv, dst, kv_send.at[k - 1], kv_recv.at[k - 1], (d, (c + k) % n))

    for k in range(1, nblk):
        @pl.when(c + k < n)
        def _():
            kv_copy(k).start()

    full = n // 2 - 1
    one_third = 1 + (full - 1) // 2

    def advance(lo, hi):
        steps(lo, hi, lambda s: [one.step(s) for one in rest])

    advance(1, one_third)
    for k in range(1, nblk):
        @pl.when(c - k >= 0)
        def _():
            kv_copy(k).wait_recv()
    attend_part(nblk, len_ref, q_ref, kv_ref, at_ref, af_ref, inv_ref, p_ref, ka, kb, bias)
    advance(one_third, full)
    for one in rest:
        one.last()
    for one in (oo, ox, gr, dr):
        one.arrive(n // 2 - 1)
    ocore = [
        (
            remote(wo.at[dd], wo.at[dd], near_send.at[7 + i], near_recv.at[7 + i], (cd, c)),
            remote(wo.at[da], wo.at[da], near_send.at[7 + i], near_recv.at[7 + i], (cd, c)),
        )
        for i, (dd, da) in enumerate(((d, cd), (xd, (cd + 2) % 4)))
    ]
    for out, _ in ocore:
        out.start()
    for _, arrival in ocore:
        arrival.wait_recv()
    middle = x + nn(at_ref[...].T, wo[...].reshape(width, width))
    mid_ref[...] = middle
    r2 = lax.rsqrt(jnp.mean(middle * middle, axis=-1, keepdims=True) + EPS)
    nm[d] = (middle * r2 * g2).astype(BF)
    nms.start()
    nms.forward()
    nms.finish()
    cots.finish()
    for k in range(1, nblk):
        @pl.when(c + k < n)
        def _():
            kv_copy(k).wait_send()
    fswap.wait_send()
    oswap.wait_send()
    for out, _ in a2a + fcore + ocore:
        out.wait_send()
    for one in (fo, fx, oo, ox, gr, dr):
        one.drain()


def mid_kernel(dn_in, out_in, dn_ref, out_ref, land, send, recv):
    d, c, core, cd, xd = places()
    barrier = pltpu.get_barrier_semaphore()
    for to in (cd, xd):
        pl.semaphore_signal(barrier, inc=1, device_id=(to, c), device_id_type=MESH)
    pl.semaphore_wait(barrier, 2)
    parts = (dn_in, out_in)
    first = []
    x = d // 2
    for i, part in enumerate(parts):
        for j, xx in enumerate((1 - x, x)):
            first.append(
                remote(part.at[2 * xx + 1 - core], land.at[i, j], send.at[i, j], recv.at[i, j], (cd, c))
            )
    for j in (0, 1):
        for i in range(2):
            first[2 * i + j].start()
    second = []
    for i, part in enumerate(parts):
        first[2 * i].wait_recv()
        land[i, 0] = (land[i, 0].astype(F32) + part[xd].astype(F32)).astype(BF)
        second.append(remote(land.at[i, 0], land.at[i, 2], send.at[i, 2], recv.at[i, 2], (xd, c)))
        second[-1].start()
    for i, (part, ref) in enumerate(zip(parts, (dn_ref, out_ref))):
        first[2 * i + 1].wait_recv()
        second[i].wait_recv()
        ref[...] = part[d].astype(F32) + land[i, 1].astype(F32) + land[i, 2].astype(F32)
    for copy in first + second:
        copy.wait_send()


def back_kernel(
    n, nblk,
    gu_part, wd_part, da_ref, af_ref, inv_ref, p_ref, q_ref, kv_ref, a_ref, b_ref, cos_ref, sin_ref,
    dq_ref, dp_ref, gu_ref, wd_ref,
    ka, kb, dka, dqa, db, dkv, dkv16, kv_land, gu_land, wd_land, gu_own,
    own_sem, ring_send, ring_recv, kv_send, kv_recv, near_send, near_recv,
):
    d, c, core, cd, xd = places()
    t = q_ref.shape[1]
    n_dp = 4
    meet(n, False)
    cut = -(-wd_part.shape[1] // 16) * 8

    def wd_half(ref, w):
        return ref.at[:cut] if w == 0 else ref.at[cut:]

    gr = ScatterRing(
        n, lambda o: gu_part.at[:, :, o], lambda o, w: gu_part.at[w, :, o], gu_land,
        None, lambda ref, w: ref.at[w], ring_send.at[0], ring_recv.at[0],
    )
    dr = ScatterRing(
        n, lambda o: wd_part.at[o], lambda o, w: wd_half(wd_part.at[o], w), wd_land,
        None, wd_half, ring_send.at[1], ring_recv.at[1],
    )
    rings = (gr, dr)
    for one in rings:
        one.start()

    def advance(s):
        for one in rings:
            one.step(s)

    h = n // 2
    pairs = H // 2

    def serve(p):
        @pl.when(p == 1)
        def _():
            advance(1)

        @pl.when(p > 1)
        def _():
            lo = 2 + (p - 2) * (h - 2) // (pairs - 2)
            hi = 2 + (p - 1) * (h - 2) // (pairs - 2)
            steps(lo, hi, advance)

    attend_back_part(
        nblk, serve, da_ref, af_ref, inv_ref, p_ref, q_ref, kv_ref, a_ref, b_ref, cos_ref, sin_ref,
        dq_ref, dkv, ka, kb, dka, dqa, db,
    )
    dkv16[...] = dkv[...].astype(BF)

    def kv_copy(k):
        src = dkv16.at[:, (nblk - 1 - k) * t : (nblk - k) * t]
        return remote(src, kv_land.at[k - 1], kv_send.at[k - 1], kv_recv.at[k - 1], (d, (c + n - k) % n))

    for k in range(1, nblk):
        @pl.when(c - k >= 0)
        def _():
            kv_copy(k).start()
    dp_ref[...] = dkv[:, (nblk - 1) * t :]
    for k in range(1, nblk):
        @pl.when(c + k < n)
        def _():
            kv_copy(k).wait_recv()
            dp_ref[...] += kv_land[k - 1].astype(F32)
    total = gr.result().astype(BF)
    for dd in range(n_dp):
        gu_own[dd] = total[:, dd]
    keep = pltpu.make_async_copy(gu_own.at[d], gu_ref.at[d], own_sem)
    keep.start()
    a2a = []
    for k in range(1, n_dp):
        to = (d + k) % n_dp
        a2a.append(
            (
                remote(gu_own.at[to], gu_ref.at[d], near_send.at[k - 1], near_recv.at[k - 1], (to, c)),
                remote(
                    gu_own.at[to], gu_ref.at[(d + n_dp - k) % n_dp],
                    near_send.at[k - 1], near_recv.at[k - 1], (to, c),
                ),
            )
        )
        a2a[-1][0].start()
    wd_ref[...] = dr.result()
    for out, arrival in a2a:
        arrival.wait_recv()
        out.wait_send()
    keep.wait()
    for k in range(1, nblk):
        @pl.when(c - k >= 0)
        def _():
            kv_copy(k).wait_send()
    for one in rings:
        one.drain()


def last_kernel(
    n, fac_part, wo_part, fac_ref, wo_ref,
    fac_core, wo_core, fac_land, wo_land, fac_x, wo_x,
    near_send, near_recv, ring_send, ring_recv,
):
    d, c, core, cd, xd = places()
    meet(n, True)
    x = d // 2
    rings, swaps = [], []
    for i, (part, held) in enumerate(((fac_part, fac_core), (wo_part, wo_core))):
        for xx in range(2):
            swaps.append(
                remote(
                    part.at[2 * xx + 1 - core], held.at[xx],
                    near_send.at[i, xx], near_recv.at[i, xx], (cd, c),
                )
            )
            swaps[-1].start()
    jobs = ((fac_part, fac_core, fac_land, fac_x, fac_ref), (wo_part, wo_core, wo_land, wo_x, wo_ref))
    for i, (part, held, land, _, _) in enumerate(jobs):
        for xx in range(2):
            swaps[2 * i + xx].wait_recv()
            held[xx] = (held[xx].astype(F32) + part[2 * xx + core].astype(F32)).astype(BF)
        ring = ScatterRing(
            n, lambda o, held=held: held.at[:, o], lambda o, w, held=held: held.at[w, o], land,
            None, lambda ref, w: ref.at[w], ring_send.at[i], ring_recv.at[i],
        )
        ring.start()
        rings.append(ring)
    h = n // 2
    for s in range(1, min(h, 2)):
        for ring in rings:
            ring.step(s)
    steps(2, h, lambda s: [ring.step(s) for ring in rings])
    ends = []
    for i, (ring, (part, held, land, xbuf, ref)) in enumerate(zip(rings, jobs)):
        total = ring.result()
        for xx in range(2):
            xbuf[xx] = total[xx].astype(BF)
        ends.append(remote(xbuf.at[1 - x], xbuf.at[2], near_send.at[i, 2], near_recv.at[i, 2], (xd, c)))
        ends[-1].start()
    for end, ring, (_, _, _, xbuf, ref) in zip(ends, rings, jobs):
        end.wait_recv()
        ref[...] = xbuf[x].astype(F32) + xbuf[2].astype(F32)
    for copy in swaps + ends:
        copy.wait_send()
    for ring in rings:
        ring.drain()


def vmem(n):
    return [pl.BlockSpec(memory_space=pltpu.VMEM)] * n


def hbm(n):
    return [pl.BlockSpec(memory_space=pl.ANY)] * n


SMEM = pl.BlockSpec(memory_space=pltpu.SMEM)
DMA = pltpu.SemaphoreType.DMA


def talks(i):
    return pltpu.CompilerParams(
        collective_id=i, has_side_effects=True, vmem_limit_bytes=60 * 1024 * 1024
    )


def silu_parts(gate):
    s = jax.nn.sigmoid(gate)
    return s, gate * s


def body(
    tokens,
    doc_lengths,
    first_gain,
    factor_weights,
    output_weights,
    second_gain,
    gate_weights,
    up_weights,
    down_weights,
    cotangent,
):
    _, t, width = tokens.shape
    n_ctx, n_dp = lax.axis_size("ctx"), lax.axis_size("dp")
    n_all = n_ctx * n_dp
    both = ("dp", "ctx")
    length = t * n_ctx
    nblk = min(n_ctx, -(-(length // 2 - 1) // t) + 1)
    ff = gate_weights.shape[1]
    ffq = ff // n_dp
    rows = width // n_all
    c = lax.axis_index("ctx")

    h = n_ctx // 2

    pack = jnp.concatenate(
        [factor_weights, first_gain[:, None], second_gain[:, None],
         jnp.zeros((rows, FPAD - FDIM - 2), F32)], axis=1).astype(BF)
    gu_in = jnp.stack([gate_weights, up_weights]).astype(BF).reshape(2, rows, n_dp, ffq)
    gu_in = gu_in.transpose(2, 0, 1, 3)

    half = DH // 2
    freq = 10000.0 ** (-(np.arange(half) * 2.0 / DH))
    pos = (c * t + jnp.arange(t, dtype=jnp.int32)).astype(F32)
    angles = jnp.asarray(freq, F32)[:, None] * pos[None, :]
    cosine, sine = jnp.cos(angles), jnp.sin(angles)

    x16 = tokens.reshape(t, width)
    cot_own = cotangent.reshape(t, width)
    sds = jax.ShapeDtypeStruct
    down_rows = down_weights.shape[0]
    (
        normed_t, q_t, a_t, b_t, kv, attn_t, attn_f, inv, probs, fac, wo, gu, wd, nm_all, cot, middle
    ) = pl.pallas_call(
        functools.partial(front_kernel, n_ctx, nblk),
        out_shape=(
            sds((width, t), BF),
            sds((H * DH, t), BF),
            sds((AQ, 1, t), F32),
            sds((BQ, t), F32),
            sds((PACK, nblk * t), BF),
            sds((H * DH, t), BF),
            sds((H * DH, t), F32),
            sds((H // 2, 8, 2 * t), F32),
            sds((H // 2, nblk * t, 2 * t), BF),
            sds((n_dp, n_ctx, rows, FPAD), BF),
            sds((n_dp, n_ctx, rows, width), BF),
            sds((2, n_dp, n_ctx, rows, ffq), BF),
            sds((n_ctx, down_rows, width), BF),
            sds((n_dp, t, width), BF),
            sds((n_dp, t, width), BF),
            sds((t, width), F32),
        ),
        in_specs=[SMEM] + vmem(5) + hbm(3),
        out_specs=tuple(vmem(11) + hbm(2) + vmem(1) + hbm(1) + vmem(1)),
        scratch_shapes=[
            pltpu.VMEM((2 * AK, 1, nblk * t), F32),
            pltpu.VMEM((2 * BK, nblk * t), F32),
            pltpu.VMEM((nblk * t, t), F32),
            DMA((5,)),
            DMA((9,)),
            DMA((9,)),
            DMA((6, 2, h)),
            DMA((6, 2, h)),
            DMA((nblk - 1,)),
            DMA((nblk - 1,)),
            DMA((2, 3)),
            DMA((2, 3)),
        ],
        compiler_params=talks(0),
        name="front",
    )(doc_lengths, x16, cosine, sine, pack, output_weights.astype(BF), gu_in,
      down_weights.astype(BF), cot_own)

    fac = fac.reshape(width, FPAD)
    wo = wo.reshape(width, width)
    gu = gu.reshape(2, width, ffq)
    wg, wu = gu[0], gu[1]
    wd = wd.reshape(n_ctx * down_rows, width)
    nm_all = nm_all.reshape(n_dp * t, width)
    cot = cot.reshape(n_dp * t, width)
    g1 = fac[:, FDIM].reshape(1, width).astype(F32)
    g2 = fac[:, FDIM + 1].reshape(1, width).astype(F32)

    x = x16.astype(F32)
    r2 = lax.rsqrt(jnp.mean(middle * middle, axis=-1, keepdims=True) + EPS)
    gate = nn(nm_all, wg)
    upward = nn(nm_all, wu)
    sig, act = silu_parts(gate)
    hidden = (act * upward).astype(BF)
    d_hidden = nt(cot, wd)
    d_gate = (d_hidden * upward * sig * (1.0 + gate * (1.0 - sig))).astype(BF)
    d_up = (d_hidden * act).astype(BF)
    dn_part = (nt(d_gate, wg) + nt(d_up, wu)).astype(BF).reshape(n_dp, t, width)
    out_part = nn(hidden, wd).astype(BF).reshape(n_dp, t, width)
    d_norm_mid, out_sum = pl.pallas_call(
        mid_kernel,
        out_shape=(sds((t, width), F32), sds((t, width), F32)),
        in_specs=vmem(2),
        out_specs=tuple(vmem(2)),
        scratch_shapes=[pltpu.VMEM((2, 3, t, width), BF), DMA((2, 3)), DMA((2, 3))],
        compiler_params=talks(1),
        name="mid",
    )(dn_part, out_part)
    layer_output = (middle + out_sum).astype(BF)

    def tn(a, b):
        return lax.dot_general(a, b, (((0,), (0,)), ((), ())), preferred_element_type=F32)

    gu_part = jnp.stack([tn(nm_all, d_gate), tn(nm_all, d_up)]).astype(BF)
    gu_part = gu_part.reshape(2, n_dp, n_ctx, rows, ffq)
    wd_part = tn(hidden, cot).astype(BF).reshape(n_ctx, down_rows, width)

    second_part = jnp.sum(d_norm_mid * middle * r2, axis=0)
    u2 = d_norm_mid * g2
    d_middle = (
        cot_own.astype(F32)
        + r2 * u2
        - middle * (r2**3 * jnp.mean(u2 * middle, axis=-1, keepdims=True))
    )
    d_branch = d_middle.astype(BF)
    d_attn_t = nt(wo, d_branch)
    out_grad_part = nn(attn_t, d_branch)

    dq_rows, d_packet, gu_own, down_sum = pl.pallas_call(
        functools.partial(back_kernel, n_ctx, nblk),
        out_shape=(
            sds((AQ + BQ, t), F32),
            sds((PACK, t), F32),
            sds((n_dp, 2, rows, ffq), BF),
            sds((down_rows, width), F32),
        ),
        in_specs=vmem(12),
        out_specs=tuple(vmem(4)),
        scratch_shapes=[
            pltpu.VMEM((2 * AK, 1, nblk * t), F32),
            pltpu.VMEM((2 * BK, nblk * t), F32),
            pltpu.VMEM((2 * AK, 1, nblk * t), F32),
            pltpu.VMEM((AQ, 1, t), F32),
            pltpu.VMEM((BQ, t), F32),
            pltpu.VMEM((PACK, nblk * t), F32),
            pltpu.VMEM((PACK, nblk * t), BF),
            pltpu.VMEM((nblk - 1, PACK, t), BF),
            pltpu.VMEM((2, h, 2, n_dp, rows, ffq), BF),
            pltpu.VMEM((2, h, down_rows, width), BF),
            pltpu.VMEM((n_dp, 2, rows, ffq), BF),
            DMA,
            DMA((2, 2, h)),
            DMA((2, 2, h)),
            DMA((nblk - 1,)),
            DMA((nblk - 1,)),
            DMA((3,)),
            DMA((3,)),
        ],
        compiler_params=talks(2),
        name="back",
    )(gu_part, wd_part, d_attn_t, attn_f, inv, probs, q_t, kv, a_t, b_t, cosine, sine)
    gu_own = gu_own.astype(F32).transpose(1, 2, 0, 3).reshape(2, rows, ff)

    d_bk = rope_back(d_packet[AK : AK + BK], cosine, sine, RKV)
    d_fac_t = jnp.concatenate([dq_rows, d_packet[:AK], d_bk, d_packet[KEY_ROWS:]], axis=0).astype(BF)
    d_fac = d_fac_t.T
    d_norm_in = nt(d_fac, fac[:, :FDIM])
    r1 = lax.rsqrt(jnp.mean(x * x, axis=-1, keepdims=True) + EPS)
    first_part = jnp.sum(d_norm_in * x * r1, axis=0)
    u1 = d_norm_in * g1
    input_grad = (
        d_middle + r1 * u1 - x * (r1**3 * jnp.mean(u1 * x, axis=-1, keepdims=True))
    ).astype(BF)
    fac_part = nt(normed_t, d_fac_t)
    last = jnp.concatenate(
        [fac_part, first_part[:, None], second_part[:, None],
         jnp.zeros((width, FPAD - FDIM - 2), F32)], axis=1).astype(BF)
    last_own, out_own = pl.pallas_call(
        functools.partial(last_kernel, n_ctx),
        out_shape=(sds((rows, FPAD), F32), sds((rows, width), F32)),
        in_specs=vmem(2),
        out_specs=tuple(vmem(2)),
        scratch_shapes=[
            pltpu.VMEM((2, n_ctx, rows, FPAD), BF),
            pltpu.VMEM((2, n_ctx, rows, width), BF),
            pltpu.VMEM((2, h, 2, rows, FPAD), BF),
            pltpu.VMEM((2, h, 2, rows, width), BF),
            pltpu.VMEM((3, rows, FPAD), BF),
            pltpu.VMEM((3, rows, width), BF),
            DMA((2, 3)),
            DMA((2, 3)),
            DMA((2, 2, h)),
            DMA((2, 2, h)),
        ],
        compiler_params=talks(3),
        name="last",
    )(last.reshape(n_dp, n_ctx, rows, FPAD), out_grad_part.astype(BF).reshape(n_dp, n_ctx, rows, width))
    return (
        layer_output.reshape(1, t, width),
        input_grad.reshape(1, t, width),
        last_own[:, FDIM],
        last_own[:, :FDIM],
        out_own,
        last_own[:, FDIM + 1],
        gu_own[0],
        gu_own[1],
        down_sum,
    )


def solution(mesh):
    return jax.shard_map(
        body,
        mesh=mesh,
        in_specs=(
            P("dp", "ctx", None),
            P("dp", None),
            P(("dp", "ctx")),
            P(("dp", "ctx"), None),
            P(("dp", "ctx"), None),
            P(("dp", "ctx")),
            P(("dp", "ctx"), None),
            P(("dp", "ctx"), None),
            P(("dp", "ctx"), None),
            P("dp", "ctx", None),
        ),
        out_specs=(
            P("dp", "ctx", None),
            P("dp", "ctx", None),
            P(("dp", "ctx")),
            P(("dp", "ctx"), None),
            P(("dp", "ctx"), None),
            P(("dp", "ctx")),
            P(("dp", "ctx"), None),
            P(("dp", "ctx"), None),
            P(("dp", "ctx"), None),
        ),
        check_vma=False,
    )
```

```python
import functools

import jax
import jax.numpy as jnp
import numpy as np
from jax import lax
from jax.experimental import pallas as pl
from jax.experimental.pallas import tpu as pltpu
from jax.sharding import PartitionSpec as P

H = 16
DH = 64
RQ = 6
RKV = 2
EPS = 1e-05
BF = jnp.bfloat16
F32 = jnp.float32
AQ = RQ * H
BQ = RQ * DH
AK = RKV * H
BK = RKV * DH
PACK = 2 * (AK + BK)
KEY_ROWS = AK + BK
FDIM = AQ + BQ + PACK
FPAD = 896
LOG2E = 1.4426950408889634
NEG = -1e30


def nt(a, b):
    return lax.dot_general(a, b, (((1,), (1,)), ((), ())), preferred_element_type=F32)


def nn(a, b):
    return jnp.dot(a, b, preferred_element_type=F32)

MESH = pl.DeviceIdType.MESH


def ring_place(c, n):
    z = c // 2
    return z + (c % 2) * (n - 1 - 2 * z)


def ring_index(p, n):
    p = (p + 2 * n) % n
    q = p // (n // 2)
    return (1 - q) * (2 * p) + q * (2 * (n - 1 - p) + 1)


def remote(src, dst, send, recv, dev):
    return pltpu.make_async_remote_copy(
        src_ref=src, dst_ref=dst, send_sem=send, recv_sem=recv, device_id=dev, device_id_type=MESH
    )


def places():
    d, c = lax.axis_index("dp"), lax.axis_index("ctx")
    core = d % 2
    return d, c, core, d + 1 - 2 * core, (d + 2) % 4


def meet(n, near):
    d, c, _, _, _ = places()
    barrier = pltpu.get_barrier_semaphore()
    count = 0
    n_dp = lax.axis_size("dp")
    for k in range(1, n_dp):
        pl.semaphore_signal(barrier, inc=1, device_id=((d + k) % n_dp, c), device_id_type=MESH)
        count += 1
    if near:
        r = ring_place(c, n)
        for way in (1, -1):
            pl.semaphore_signal(
                barrier, inc=1, device_id=(d, ring_index(r + way, n)), device_id_type=MESH
            )
            count += 1
    else:
        for k in range(1, n):
            pl.semaphore_signal(barrier, inc=1, device_id=(d, (c + k) % n), device_id_type=MESH)
            count += 1
    pl.semaphore_wait(barrier, count)


def steps(lo, hi, step):
    if isinstance(lo, int) and isinstance(hi, int) and hi - lo <= 4:
        for s in range(lo, hi):
            step(s)
    elif not (isinstance(lo, int) and isinstance(hi, int) and hi <= lo):
        lax.fori_loop(lo, hi, lambda s, _: (step(s), _)[1], 0)


class GatherRing:
    def __init__(self, n, slot, half, send, recv):
        self.n, self.h, self.slot, self.half, self.send, self.recv = n, n // 2, slot, half, send, recv
        self.d, c, _, _, _ = places()
        self.r = ring_place(c, n)

    def copy(self, s, i, arriving=False):
        way = 1 - 2 * i
        last = isinstance(s, int) and s == self.h - 1
        owner = ring_index(self.r - way * (s + (1 if arriving else 0)), self.n)
        ref = self.half(owner, i) if last else self.slot(owner)
        to = (self.d, ring_index(self.r + way, self.n))
        return remote(ref, ref, self.send.at[i, s], self.recv.at[i, s], to)

    def start(self, s):
        for i in range(2):
            self.copy(s, i).start()

    def arrive(self, s):
        for i in range(2):
            self.copy(s, i, True).wait_recv()

    def step(self, s):
        for i in range(2):
            self.copy(s - 1, i, True).wait_recv()
            self.copy(s, i).start()

    def last(self):
        self.step(self.h - 1)

    def drain(self):
        steps(0, self.h - 1, lambda s: [self.copy(s, i).wait_send() for i in range(2)])
        for i in range(2):
            self.copy(self.h - 1, i).wait_send()


class ScatterRing:
    def __init__(self, n, part, half, land, whole_of, half_of, send, recv):
        self.n, self.h, self.part, self.half = n, n // 2, part, half
        self.land, self.whole_of, self.half_of = land, whole_of, half_of
        self.send, self.recv = send, recv
        self.d, c, _, _, _ = places()
        self.c, self.r = c, ring_place(c, n)

    def copy(self, s, i):
        way = 1 - 2 * i
        to = (self.d, ring_index(self.r + way, self.n))
        first = isinstance(s, int) and s == 0
        if first:
            owner = ring_index(self.r + way * self.h, self.n)
            src, dst = self.half(owner, i), self.half_of(self.land.at[i, 0], i)
        else:
            src, dst = self.land.at[i, s - 1], self.land.at[i, s]
        return remote(src, dst, self.send.at[i, s], self.recv.at[i, s], to)

    def start(self):
        for i in range(2):
            self.copy(0, i).start()

    def step(self, s):
        first = isinstance(s, int) and s == 1
        for i in range(2):
            way = 1 - 2 * i
            self.copy(s - 1, i).wait_recv()
            owner = ring_index(self.r + way * (self.h - s), self.n)
            held = self.land.at[i, s - 1]
            if first:
                mine = self.half_of(held, i)
                mine[...] = (mine[...].astype(F32) + self.half(owner, i)[...].astype(F32)).astype(BF)
                self.half_of(held, 1 - i)[...] = self.half(owner, 1 - i)[...]
            else:
                held[...] = (held[...].astype(F32) + self.part(owner)[...].astype(F32)).astype(BF)
            self.copy(s, i).start()

    def rest(self, lo, hi):
        if lo == 1 and hi > 1:
            self.step(1)
            lo = 2
        steps(lo, hi, self.step)

    def result(self):
        for i in range(2):
            self.copy(self.h - 1, i).wait_recv()
        out = self.part(self.c)[...].astype(F32)
        for i in range(2):
            out = out + self.land[i, self.h - 1].astype(F32)
        return out

    def drain(self):
        for i in range(2):
            self.copy(0, i).wait_send()
        steps(1, self.h, lambda s: [self.copy(s, i).wait_send() for i in range(2)])


class Spread:
    def __init__(self, ref, send, recv):
        d, c, _, cd, xd = places()
        self.copies = [
            remote(ref.at[d], ref.at[d], send.at[0], recv.at[0], (cd, c)),
            remote(ref.at[d], ref.at[d], send.at[1], recv.at[1], (xd, c)),
            remote(ref.at[xd], ref.at[xd], send.at[2], recv.at[2], (cd, c)),
        ]

    def start(self):
        self.copies[1].start()
        self.copies[0].start()

    def forward(self):
        self.copies[1].wait_recv()
        self.copies[2].start()

    def finish(self):
        self.copies[0].wait_recv()
        self.copies[2].wait_recv()
        for copy in self.copies:
            copy.wait_send()


def blocks(count, step, state):
    if count <= 8:
        for j in range(count):
            state = step(j, state)
        return state
    return lax.fori_loop(0, count, step, state)


def lane_block(j, size):
    if isinstance(j, int):
        return pl.ds(j * size, size)
    return pl.ds(pl.multiple_of(j * size, size), size)


def rope(b, cosine, sine, ranks):
    parts = []
    half = DH // 2
    for r in range(ranks):
        u1 = b[r * DH : r * DH + half]
        u2 = b[r * DH + half : (r + 1) * DH]
        parts += [u1 * cosine - u2 * sine, u2 * cosine + u1 * sine]
    return jnp.concatenate(parts, axis=0)


def rope_back(v, cosine, sine, ranks):
    return rope(v, cosine, -sine, ranks)


def pre_part(x, g1, w, cosine, sine, nt_ref, q_ref, p_ref, a_ref, b_ref):
    r1 = lax.rsqrt(jnp.mean(x * x, axis=-1, keepdims=True) + EPS)
    n = (x * r1 * g1).astype(BF)
    nt_ref[...] = n.T
    ft = nn(n, w).T
    a = ft[:AQ]
    b = rope(ft[AQ : AQ + BQ], cosine, sine, RQ)
    for i in range(AQ):
        a_ref[i] = a[i : i + 1]
    b_ref[...] = b
    k0 = AQ + BQ
    bk = rope(ft[k0 + AK : k0 + AK + BK], cosine, sine, RKV)
    p_ref[...] = jnp.concatenate(
        [ft[k0 : k0 + AK], bk, ft[k0 + KEY_ROWS : k0 + PACK]], axis=0
    ).astype(BF)
    for h in range(H):
        acc = a[h : h + 1] * b[:DH]
        for r in range(1, RQ):
            acc = acc + a[r * H + h : r * H + h + 1] * b[r * DH : (r + 1) * DH]
        q_ref[h * DH : (h + 1) * DH, :] = (acc * (1.0 / RQ)).astype(BF)


def expand_pair(ka, kb, side, p, lanes):
    rows = []
    for hh in range(2):
        acc = 0.0
        for r in range(RKV):
            a = ka[side * AK + r * H + 2 * p + hh, :, lanes]
            b = kb[side * BK + r * DH : side * BK + (r + 1) * DH, lanes]
            acc = acc + a * b
        rows.append(acc * (1.0 / RKV))
    return jnp.concatenate(rows, axis=0)


def unpack(kv_ref, ka, kb):
    for side in range(2):
        first = side * KEY_ROWS
        a = kv_ref[first : first + AK, :].astype(F32)
        for i in range(AK):
            ka[side * AK + i] = a[i : i + 1]
        kb[side * BK : (side + 1) * BK, :] = kv_ref[first + AK : first + KEY_ROWS, :].astype(F32)


def diagonal(pair):
    zero = jnp.zeros((DH, pair.shape[1]), pair.dtype)
    left = jnp.concatenate([pair[:DH], zero], axis=0)
    right = jnp.concatenate([zero, pair[DH:]], axis=0)
    return jnp.concatenate([left, right], axis=1)


def undiagonal(wide):
    t = wide.shape[1] // 2
    return jnp.concatenate([wide[:DH, :t], wide[DH:, t:]], axis=0)


def attend_part(nblk, len_ref, q_ref, kv_ref, at_ref, af_ref, inv_ref, p_ref, ka, kb, bias):
    t = q_ref.shape[1]
    c = lax.axis_index("ctx")
    tpos = c * t + lax.broadcasted_iota(jnp.int32, (1, t), 1)
    start = jnp.zeros((1, t), jnp.int32)
    run = jnp.int32(0)
    for j in range(len_ref.shape[1]):
        start = jnp.where(tpos >= run, run, start)
        run = run + len_ref[0, j]
    unpack(kv_ref, ka, kb)

    def bias_block(j, _):
        spos = (c - nblk + 1 + j) * t + lax.broadcasted_iota(jnp.int32, (t, t), 0)
        ok = (spos >= start) & (spos <= tpos)
        bias[lane_block(j, t), :] = jnp.where(ok, 0.0, NEG)
        return _

    blocks(nblk, bias_block, 0)

    def pair(p, _):
        rows = pl.ds(pl.multiple_of(p * 2 * DH, 2 * DH), 2 * DH)
        qd = diagonal(q_ref[rows, :])

        def step(j, state):
            num, tot = state
            lanes = lane_block(j, t)
            k = expand_pair(ka, kb, 0, p, lanes).T.astype(BF)
            v = expand_pair(ka, kb, 1, p, lanes).astype(BF)
            b = bias[lanes, :]
            s = nn(k, qd) * (LOG2E * DH**-0.5) + jnp.concatenate([b, b], axis=1)
            e = jnp.exp2(s)
            tot = tot + jnp.sum(e, axis=0, keepdims=True)
            pb = e.astype(BF)
            p_ref[p, lanes, :] = pb
            return (num + nn(v, pb), tot)

        num, tot = blocks(
            nblk, step, (jnp.zeros((2 * DH, 2 * t), F32), jnp.zeros((1, 2 * t), F32))
        )
        inv = 1.0 / tot
        af = undiagonal(num * inv)
        af_ref[rows, :] = af
        at_ref[rows, :] = af.astype(BF)
        inv_ref[p] = jnp.broadcast_to(inv, (8, 2 * t))
        return _

    lax.fori_loop(0, H // 2, pair, 0)


def attend_back_part(
    nblk, serve, da_ref, af_ref, inv_ref, p_copy, pbuf, q_ref, kv_ref, a_ref, b_ref, cos_ref, sin_ref,
    dq_ref, dkv_ref, ka, kb, dka, dqa, db,
):
    t = q_ref.shape[1]
    unpack(kv_ref, ka, kb)
    db[...] = jnp.zeros_like(db)
    for side in range(2):
        first = side * KEY_ROWS + AK
        dkv_ref[first : first + BK, :] = jnp.zeros((BK, nblk * t), F32)

    def factor_back(dwide, side, p, lanes):
        for hh in range(2):
            d = dwide[hh * DH : (hh + 1) * DH] * (1.0 / RKV)
            for r in range(RKV):
                row = side * AK + r * H + 2 * p + hh
                first = side * KEY_ROWS + AK + r * DH
                b = kb[side * BK + r * DH : side * BK + (r + 1) * DH, lanes]
                dka[row, :, lanes] = jnp.sum(d * b, axis=0, keepdims=True)
                dkv_ref[first : first + DH, lanes] += d * ka[row, :, lanes]

    def pair(p, carry):
        @pl.when(p + 1 < H // 2)
        def _():
            p_copy(p + 1).start()

        p_copy(p).wait()
        rows = pl.ds(pl.multiple_of(p * 2 * DH, 2 * DH), 2 * DH)
        da = da_ref[rows, :]
        inv = inv_ref[p][:1]
        dd = diagonal(da)
        dn = (dd * inv).astype(BF)
        dtot = -jnp.sum(dd * diagonal(af_ref[rows, :]), axis=0, keepdims=True) * inv
        qd = diagonal(q_ref[rows, :])

        def step(j, dq):
            lanes = lane_block(j, t)
            k = expand_pair(ka, kb, 0, p, lanes).astype(BF)
            v = expand_pair(ka, kb, 1, p, lanes).T.astype(BF)
            pb = pbuf[p % 2, lanes, :]
            ds = (pb.astype(F32) * (nn(v, dn) + dtot)).astype(BF)
            dq = dq + nn(k, ds)
            factor_back(nt(qd, ds) * (DH**-0.5), 0, p, lanes)
            factor_back(nt(dn, pb), 1, p, lanes)
            return dq

        dq = undiagonal(blocks(nblk, step, jnp.zeros((2 * DH, 2 * t), F32)))
        dq = dq * (DH**-0.5 / RQ)
        for hh in range(2):
            d = dq[hh * DH : (hh + 1) * DH]
            for r in range(RQ):
                row = r * H + 2 * p + hh
                dqa[row] = jnp.sum(d * b_ref[r * DH : (r + 1) * DH, :], axis=0, keepdims=True)
                db[r * DH : (r + 1) * DH, :] += d * a_ref[row]
        serve(p)
        return carry

    lax.fori_loop(0, H // 2, pair, 0)
    for i in range(AQ):
        dq_ref[i : i + 1, :] = dqa[i]
    for side in range(2):
        for i in range(AK):
            dkv_ref[side * KEY_ROWS + i : side * KEY_ROWS + i + 1, :] = dka[side * AK + i]
    dq_ref[AQ : AQ + BQ, :] = rope_back(db[...], cos_ref[...], sin_ref[...], RQ)


def front_kernel(
    n, nblk,
    len_ref, x_ref, cos_ref, sin_ref, fac_in, wo_in, gu_in, wd_in, cot_in,
    nt_ref, q_ref, a_ref, b_ref, kv_ref, at_ref, af_ref, inv_ref, p_ref,
    fac, wo, gu, wd, nm, cot, mid_ref,
    ka, kb, bias,
    own_sem, near_send, near_recv, ring_send, ring_recv, kv_send, kv_recv, sp_send, sp_recv,
):
    d, c, core, cd, xd = places()
    t = x_ref.shape[0]
    n_dp = 4
    locals_ = [
        pltpu.make_async_copy(fac_in, fac.at[d, c], own_sem.at[0]),
        pltpu.make_async_copy(wo_in, wo.at[d, c], own_sem.at[1]),
        pltpu.make_async_copy(gu_in.at[d], gu.at[:, d, c], own_sem.at[2]),
        pltpu.make_async_copy(wd_in, wd.at[c], own_sem.at[3]),
        pltpu.make_async_copy(cot_in, cot.at[d], own_sem.at[4]),
    ]
    for copy in locals_:
        copy.start()
    for k in range(1, nblk):
        @pl.when(c - k < 0)
        def _():
            kv_ref[:, (nblk - 1 - k) * t : (nblk - k) * t] = jnp.zeros((PACK, t), BF)
    meet(n, False)
    for copy in locals_:
        copy.wait()

    def ring(i, slot, half):
        return GatherRing(n, slot, half, ring_send.at[i], ring_recv.at[i])

    rows = fac_in.shape[0] // 2

    def shard(ref, dd):
        return (lambda o: ref.at[dd, o]), (lambda o, w: ref.at[dd, o, w * rows : (w + 1) * rows])

    fo, fx = ring(0, *shard(fac, d)), ring(1, *shard(fac, xd))
    oo, ox = ring(2, *shard(wo, d)), ring(3, *shard(wo, xd))
    cut = -(-wd_in.shape[0] // 16) * 8
    gr = ring(4, lambda o: gu.at[:, :, o], lambda o, w: gu.at[w, :, o])
    dr = ring(
        5, lambda o: wd.at[o],
        lambda o, w: wd.at[o, :cut] if w == 0 else wd.at[o, cut:],
    )
    small, large = (fo, fx, oo, ox), (gr, dr)
    fswap = remote(fac.at[d, c], fac.at[d, c], near_send.at[0], near_recv.at[0], (xd, c))
    oswap = remote(wo.at[d, c], wo.at[d, c], near_send.at[1], near_recv.at[1], (xd, c))
    fswap.start()
    oswap.start()
    fo.start(0)
    oo.start(0)
    a2a = []
    for k in range(1, n_dp):
        to = (d + k) % n_dp
        a2a.append(
            (
                remote(gu_in.at[to], gu.at[:, d, c], near_send.at[1 + k], near_recv.at[1 + k], (to, c)),
                remote(
                    gu_in.at[to], gu.at[:, (d + n_dp - k) % n_dp, c],
                    near_send.at[1 + k], near_recv.at[1 + k], (to, c),
                ),
            )
        )
        a2a[-1][0].start()
    cots = Spread(cot, sp_send.at[0], sp_recv.at[0])
    nms = Spread(nm, sp_send.at[1], sp_recv.at[1])
    cots.start()
    fswap.wait_recv()
    fx.start(0)
    oswap.wait_recv()
    ox.start(0)
    steps(1, n // 2 - 1, lambda s: [one.step(s) for one in small])
    for one in small:
        one.last()
    for _, arrival in a2a:
        arrival.wait_recv()
    for one in large:
        one.start(0)
    def core_swap(ref, i, dd, da):
        return (
            remote(ref.at[dd], ref.at[dd], near_send.at[5 + i], near_recv.at[5 + i], (cd, c)),
            remote(ref.at[da], ref.at[da], near_send.at[5 + i], near_recv.at[5 + i], (cd, c)),
        )

    near = []
    for i, (one, ref, dd, da) in enumerate(
        ((fo, fac, d, cd), (fx, fac, xd, (cd + 2) % 4), (oo, wo, d, cd), (ox, wo, xd, (cd + 2) % 4))
    ):
        one.arrive(n // 2 - 1)
        near.append(core_swap(ref, i, dd, da))
        near[-1][0].start()
    cots.forward()
    for _, arrival in near[:2]:
        arrival.wait_recv()

    width = x_ref.shape[1]
    x = x_ref[...].astype(F32)
    w = fac[...].reshape(width, FPAD)
    g1, g2 = gain_rows(w)
    own_kv = kv_ref.at[:, (nblk - 1) * t : nblk * t]
    pre_part(x, g1, w, cos_ref[...], sin_ref[...], nt_ref, q_ref, own_kv, a_ref, b_ref)

    def kv_copy(k):
        dst = kv_ref.at[:, (nblk - 1 - k) * t : (nblk - k) * t]
        return remote(own_kv, dst, kv_send.at[k - 1], kv_recv.at[k - 1], (d, (c + k) % n))

    for k in range(1, nblk):
        @pl.when(c + k < n)
        def _():
            kv_copy(k).start()
    for k in range(1, nblk):
        @pl.when(c - k >= 0)
        def _():
            kv_copy(k).wait_recv()
    attend_part(nblk, len_ref, q_ref, kv_ref, at_ref, af_ref, inv_ref, p_ref, ka, kb, bias)

    full = n // 2 - 1
    middle_step = 1 + full // 2
    steps(1, middle_step, lambda s: [one.step(s) for one in large])
    for _, arrival in near[2:]:
        arrival.wait_recv()
    middle = x + nn(at_ref[...].T, wo[...].reshape(width, width))
    mid_ref[...] = middle
    r2 = lax.rsqrt(jnp.mean(middle * middle, axis=-1, keepdims=True) + EPS)
    nm[d] = (middle * r2 * g2).astype(BF)
    nms.start()
    nms.forward()
    nms.finish()
    cots.finish()
    steps(middle_step, full, lambda s: [one.step(s) for one in large])
    for one in large:
        one.last()
    for one in large:
        one.arrive(n // 2 - 1)
    for k in range(1, nblk):
        @pl.when(c + k < n)
        def _():
            kv_copy(k).wait_send()
    fswap.wait_send()
    oswap.wait_send()
    for out, _ in a2a + near:
        out.wait_send()
    for one in small + large:
        one.drain()


def gain_rows(w):
    first = FPAD - 128
    gains = w[:, first:].astype(F32).T
    return gains[FDIM - first : FDIM - first + 1], gains[FDIM - first + 1 : FDIM - first + 2]


class PairScatter:
    def __init__(self, n, part, held, land, own, send, recv, ring_send, ring_recv):
        d, c, core, cd, xd = places()
        self.core, self.x, self.part, self.held, self.own = core, d // 2, part, held, own
        self.swaps = [
            remote(part.at[2 * xx + 1 - core], held.at[xx], send.at[xx], recv.at[xx], (cd, c))
            for xx in range(2)
        ]
        self.end = remote(own.at[1 - self.x], own.at[2], send.at[2], recv.at[2], (xd, c))
        self.ring = ScatterRing(
            n, lambda o: held.at[:, o], lambda o, w: held.at[w, o], land,
            None, lambda ref, w: ref.at[w], ring_send, ring_recv,
        )

    def start(self):
        for swap in self.swaps:
            swap.start()

    def enter(self):
        for xx in range(2):
            self.swaps[xx].wait_recv()
            mine = self.part[2 * xx + self.core].astype(F32)
            self.held[xx] = (self.held[xx].astype(F32) + mine).astype(BF)
        self.ring.start()

    def leave(self):
        total = self.ring.result()
        for xx in range(2):
            self.own[xx] = total[xx].astype(BF)
        self.end.start()

    def result(self):
        self.end.wait_recv()
        return self.own[self.x].astype(F32) + self.own[2].astype(F32)

    def drain(self):
        for copy in self.swaps + [self.end]:
            copy.wait_send()
        self.ring.drain()


def back_kernel(
    n, nblk,
    gu_part, wd_part, dn_in, out_in, mid_ref, cot_ref, x_ref, fac, wo, at_ref, nt_ref,
    af_ref, inv_ref, p_ref, q_ref, kv_ref, a_ref, b_ref, cos_ref, sin_ref,
    y_ref, dx_ref, fac_ref, wo_ref, gu_ref, wd_ref,
    ka, kb, dka, dqa, db, dkv, dkv16, kv_land, gu_land, wd_land, gu_own,
    da_ref, dq_ref, dmid_ref, dp_land, fac_part, wo_part, fac_held, wo_held, fac_land, wo_land,
    fac_own, wo_own,
    own_sem, ring_send, ring_recv, kv_send, kv_recv, near_send, near_recv, dp_send, dp_recv,
    pair_send, pair_recv, pbuf, p_sem,
):
    d, c, core, cd, xd = places()
    x_at = d // 2
    t = q_ref.shape[1]
    n_dp = 4
    width = x_ref.shape[1]

    def p_copy(p):
        return pltpu.make_async_copy(p_ref.at[p], pbuf.at[p % 2], p_sem.at[p % 2])

    p_copy(0).start()
    meet(n, False)
    parts = (dn_in, out_in)
    first = []
    for i, part in enumerate(parts):
        for j, xx in enumerate((1 - x_at, x_at)):
            first.append(
                remote(
                    part.at[2 * xx + 1 - core], dp_land.at[i, j],
                    dp_send.at[i, j], dp_recv.at[i, j], (cd, c),
                )
            )
    for j in (0, 1):
        for i in range(2):
            first[2 * i + j].start()
    cut = -(-wd_part.shape[1] // 16) * 8

    def wd_half(ref, w):
        return ref.at[:cut] if w == 0 else ref.at[cut:]

    gr = ScatterRing(
        n, lambda o: gu_part.at[:, :, o], lambda o, w: gu_part.at[w, :, o], gu_land,
        None, lambda ref, w: ref.at[w], ring_send.at[0], ring_recv.at[0],
    )
    dr = ScatterRing(
        n, lambda o: wd_part.at[o], lambda o, w: wd_half(wd_part.at[o], w), wd_land,
        None, wd_half, ring_send.at[1], ring_recv.at[1],
    )
    large = (gr, dr)
    for one in large:
        one.start()
    second = []
    for i, part in enumerate(parts):
        first[2 * i].wait_recv()
        dp_land[i, 0] = (dp_land[i, 0].astype(F32) + part[xd].astype(F32)).astype(BF)
        second.append(
            remote(dp_land.at[i, 0], dp_land.at[i, 2], dp_send.at[i, 2], dp_recv.at[i, 2], (xd, c))
        )
        second[-1].start()
    fs = PairScatter(
        n, fac_part, fac_held, fac_land, fac_own, pair_send.at[0], pair_recv.at[0],
        ring_send.at[2], ring_recv.at[2],
    )
    ws = PairScatter(
        n, wo_part, wo_held, wo_land, wo_own, pair_send.at[1], pair_recv.at[1],
        ring_send.at[3], ring_recv.at[3],
    )
    h = n // 2

    def advance(s):
        for one in large:
            one.step(s)

    advance(1)
    for i in range(2):
        first[2 * i + 1].wait_recv()
    second[0].wait_recv()
    middle = mid_ref[...]
    r2 = lax.rsqrt(jnp.mean(middle * middle, axis=-1, keepdims=True) + EPS)
    w = fac[...].reshape(width, FPAD)
    g1, g2 = gain_rows(w)
    dn = dn_in[d].astype(F32) + dp_land[0, 1].astype(F32) + dp_land[0, 2].astype(F32)
    second_part = jnp.sum(dn * middle * r2, axis=0, keepdims=True)
    u2 = dn * g2
    d_middle = (
        cot_ref[...].astype(F32)
        + r2 * u2
        - middle * (r2 * r2 * r2 * jnp.mean(u2 * middle, axis=-1, keepdims=True))
    )
    dmid_ref[...] = d_middle
    d_branch = d_middle.astype(BF)
    wo_part[...] = nn(at_ref[...], d_branch).astype(BF).reshape(wo_part.shape)
    ws.start()
    da_ref[...] = nt(wo[...].reshape(width, width), d_branch)
    second[1].wait_recv()
    y_ref[...] = (
        mid_ref[...]
        + (out_in[d].astype(F32) + dp_land[1, 1].astype(F32) + dp_land[1, 2].astype(F32))
    ).astype(BF)
    ws.enter()
    points = 3

    def serve(k):
        steps(2 + -(-(k - 1) * (h - 2) // points), 2 + -(-k * (h - 2) // points), advance)

    serve(1)

    def serve_pair(p):
        @pl.when(p == H // 2 - 3)
        def _():
            ws.ring.step(1)
            serve(2)

    attend_back_part(
        nblk, serve_pair, da_ref, af_ref, inv_ref, p_copy, pbuf, q_ref, kv_ref, a_ref, b_ref,
        cos_ref, sin_ref, dq_ref, dkv, ka, kb, dka, dqa, db,
    )
    dkv16[...] = dkv[...].astype(BF)

    def kv_copy(k):
        src = dkv16.at[:, (nblk - 1 - k) * t : (nblk - k) * t]
        return remote(src, kv_land.at[k - 1], kv_send.at[k - 1], kv_recv.at[k - 1], (d, (c + n - k) % n))

    for k in range(1, nblk):
        @pl.when(c - k >= 0)
        def _():
            kv_copy(k).start()
    own_kv = dkv.at[:, (nblk - 1) * t :]
    serve(3)
    for k in range(1, nblk):
        @pl.when(c + k < n)
        def _():
            kv_copy(k).wait_recv()
            own_kv[...] += kv_land[k - 1].astype(F32)
    steps(2, h, ws.ring.step)
    dp = own_kv[...]
    d_bk = rope_back(dp[AK : AK + BK], cos_ref[...], sin_ref[...], RKV)
    d_fac_t = jnp.concatenate(
        [dq_ref[...], dp[:AK], d_bk, dp[KEY_ROWS:], jnp.zeros((FPAD - FDIM, t), F32)], axis=0
    ).astype(BF)
    x = x_ref[...].astype(F32)
    r1 = lax.rsqrt(jnp.mean(x * x, axis=-1, keepdims=True) + EPS)
    d_norm_in = nt(d_fac_t.T, w)
    first_part = jnp.sum(d_norm_in * x * r1, axis=0, keepdims=True)
    tail = FPAD - 128
    gains = jnp.concatenate(
        [jnp.zeros((FDIM - tail, width), F32), first_part, second_part,
         jnp.zeros((FPAD - FDIM - 2, width), F32)], axis=0).T
    product = nt(nt_ref[...], d_fac_t)
    shape = fac_part.shape[:3]
    fac_part[:, :, :, :tail] = product[:, :tail].astype(BF).reshape(shape + (tail,))
    fac_part[:, :, :, tail:] = (product[:, tail:] + gains).astype(BF).reshape(shape + (128,))
    fs.start()
    u1 = d_norm_in * g1
    dx_ref[...] = (
        dmid_ref[...] + r1 * u1 - x * (r1 * r1 * r1 * jnp.mean(u1 * x, axis=-1, keepdims=True))
    ).astype(BF)
    fs.enter()
    total = gr.result().astype(BF)
    for dd in range(n_dp):
        gu_own[dd] = total[:, dd]
    keep = pltpu.make_async_copy(gu_own.at[d], gu_ref.at[d], own_sem)
    keep.start()
    a2a = []
    for k in range(1, n_dp):
        to = (d + k) % n_dp
        a2a.append(
            (
                remote(gu_own.at[to], gu_ref.at[d], near_send.at[k - 1], near_recv.at[k - 1], (to, c)),
                remote(
                    gu_own.at[to], gu_ref.at[(d + n_dp - k) % n_dp],
                    near_send.at[k - 1], near_recv.at[k - 1], (to, c),
                ),
            )
        )
        a2a[-1][0].start()
    ws.leave()
    fs.ring.step(1)
    wd_ref[...] = dr.result()
    steps(2, h, fs.ring.step)
    wo_ref[...] = ws.result()
    fs.leave()
    for out, arrival in a2a:
        arrival.wait_recv()
        out.wait_send()
    keep.wait()
    fac_ref[...] = fs.result()
    for k in range(1, nblk):
        @pl.when(c - k >= 0)
        def _():
            kv_copy(k).wait_send()
    for copy in first + second:
        copy.wait_send()
    for one in large + (ws, fs):
        one.drain()


def vmem(n):
    return [pl.BlockSpec(memory_space=pltpu.VMEM)] * n


def hbm(n):
    return [pl.BlockSpec(memory_space=pl.ANY)] * n


SMEM = pl.BlockSpec(memory_space=pltpu.SMEM)
DMA = pltpu.SemaphoreType.DMA


def talks(i):
    return pltpu.CompilerParams(
        collective_id=i, has_side_effects=True, vmem_limit_bytes=60 * 1024 * 1024
    )


def silu_parts(gate):
    s = jax.nn.sigmoid(gate)
    return s, gate * s


def body(
    tokens,
    doc_lengths,
    first_gain,
    factor_weights,
    output_weights,
    second_gain,
    gate_weights,
    up_weights,
    down_weights,
    cotangent,
):
    _, t, width = tokens.shape
    n_ctx, n_dp = lax.axis_size("ctx"), lax.axis_size("dp")
    n_all = n_ctx * n_dp
    both = ("dp", "ctx")
    length = t * n_ctx
    nblk = min(n_ctx, -(-(length // 2 - 1) // t) + 1)
    ff = gate_weights.shape[1]
    ffq = ff // n_dp
    rows = width // n_all
    c = lax.axis_index("ctx")

    h = n_ctx // 2

    pack = jnp.concatenate(
        [factor_weights, first_gain[:, None], second_gain[:, None],
         jnp.zeros((rows, FPAD - FDIM - 2), F32)], axis=1).astype(BF)
    gu_in = jnp.stack([gate_weights, up_weights]).astype(BF).reshape(2, rows, n_dp, ffq)
    gu_in = gu_in.transpose(2, 0, 1, 3)

    half = DH // 2
    freq = 10000.0 ** (-(np.arange(half) * 2.0 / DH))
    pos = (c * t + jnp.arange(t, dtype=jnp.int32)).astype(F32)
    angles = jnp.asarray(freq, F32)[:, None] * pos[None, :]
    cosine, sine = jnp.cos(angles), jnp.sin(angles)

    x16 = tokens.reshape(t, width)
    cot_own = cotangent.reshape(t, width)
    sds = jax.ShapeDtypeStruct
    down_rows = down_weights.shape[0]
    (
        normed_t, q_t, a_t, b_t, kv, attn_t, attn_f, inv, probs, fac, wo, gu, wd, nm_all, cot, middle
    ) = pl.pallas_call(
        functools.partial(front_kernel, n_ctx, nblk),
        out_shape=(
            sds((width, t), BF),
            sds((H * DH, t), BF),
            sds((AQ, 1, t), F32),
            sds((BQ, t), F32),
            sds((PACK, nblk * t), BF),
            sds((H * DH, t), BF),
            sds((H * DH, t), F32),
            sds((H // 2, 8, 2 * t), F32),
            sds((H // 2, nblk * t, 2 * t), BF),
            sds((n_dp, n_ctx, rows, FPAD), BF),
            sds((n_dp, n_ctx, rows, width), BF),
            sds((2, n_dp, n_ctx, rows, ffq), BF),
            sds((n_ctx, down_rows, width), BF),
            sds((n_dp, t, width), BF),
            sds((n_dp, t, width), BF),
            sds((t, width), F32),
        ),
        in_specs=[SMEM] + vmem(8),
        out_specs=tuple(vmem(16)),
        scratch_shapes=[
            pltpu.VMEM((2 * AK, 1, nblk * t), F32),
            pltpu.VMEM((2 * BK, nblk * t), F32),
            pltpu.VMEM((nblk * t, t), F32),
            DMA((5,)),
            DMA((9,)),
            DMA((9,)),
            DMA((6, 2, h)),
            DMA((6, 2, h)),
            DMA((nblk - 1,)),
            DMA((nblk - 1,)),
            DMA((2, 3)),
            DMA((2, 3)),
        ],
        compiler_params=talks(0),
        name="front",
    )(doc_lengths, x16, cosine, sine, pack, output_weights.astype(BF), gu_in,
      down_weights.astype(BF), cot_own)

    gu = gu.reshape(2, width, ffq)
    wg, wu = gu[0], gu[1]
    wd = wd.reshape(n_ctx * down_rows, width)
    nm_all = nm_all.reshape(n_dp * t, width)
    cot = cot.reshape(n_dp * t, width)

    gate = nn(nm_all, wg)
    upward = nn(nm_all, wu)
    sig, act = silu_parts(gate)
    hidden = (act * upward).astype(BF)
    d_hidden = nt(cot, wd)
    d_gate = (d_hidden * upward * sig * (1.0 + gate * (1.0 - sig))).astype(BF)
    d_up = (d_hidden * act).astype(BF)
    dn_part = (nt(d_gate, wg) + nt(d_up, wu)).astype(BF).reshape(n_dp, t, width)
    out_part = nn(hidden, wd).astype(BF).reshape(n_dp, t, width)

    def tn(a, b):
        return lax.dot_general(a, b, (((0,), (0,)), ((), ())), preferred_element_type=F32)

    gu_part = jnp.stack([tn(nm_all, d_gate), tn(nm_all, d_up)]).astype(BF)
    gu_part = gu_part.reshape(2, n_dp, n_ctx, rows, ffq)
    wd_part = tn(hidden, cot).astype(BF).reshape(n_ctx, down_rows, width)

    layer_output, input_grad, last_own, out_own, gu_own, down_sum = pl.pallas_call(
        functools.partial(back_kernel, n_ctx, nblk),
        out_shape=(
            sds((t, width), BF),
            sds((t, width), BF),
            sds((rows, FPAD), F32),
            sds((rows, width), F32),
            sds((n_dp, 2, rows, ffq), BF),
            sds((down_rows, width), F32),
        ),
        in_specs=vmem(13) + hbm(1) + vmem(6),
        out_specs=tuple(vmem(6)),
        scratch_shapes=[
            pltpu.VMEM((2 * AK, 1, nblk * t), F32),
            pltpu.VMEM((2 * BK, nblk * t), F32),
            pltpu.VMEM((2 * AK, 1, nblk * t), F32),
            pltpu.VMEM((AQ, 1, t), F32),
            pltpu.VMEM((BQ, t), F32),
            pltpu.VMEM((PACK, nblk * t), F32),
            pltpu.VMEM((PACK, nblk * t), BF),
            pltpu.VMEM((nblk - 1, PACK, t), BF),
            pltpu.VMEM((2, h, 2, n_dp, rows, ffq), BF),
            pltpu.VMEM((2, h, down_rows, width), BF),
            pltpu.VMEM((n_dp, 2, rows, ffq), BF),
            pltpu.VMEM((H * DH, t), F32),
            pltpu.VMEM((AQ + BQ, t), F32),
            pltpu.VMEM((t, width), F32),
            pltpu.VMEM((2, 3, t, width), BF),
            pltpu.VMEM((n_dp, n_ctx, rows, FPAD), BF),
            pltpu.VMEM((n_dp, n_ctx, rows, width), BF),
            pltpu.VMEM((2, n_ctx, rows, FPAD), BF),
            pltpu.VMEM((2, n_ctx, rows, width), BF),
            pltpu.VMEM((2, h, 2, rows, FPAD), BF),
            pltpu.VMEM((2, h, 2, rows, width), BF),
            pltpu.VMEM((3, rows, FPAD), BF),
            pltpu.VMEM((3, rows, width), BF),
            DMA,
            DMA((4, 2, h)),
            DMA((4, 2, h)),
            DMA((nblk - 1,)),
            DMA((nblk - 1,)),
            DMA((3,)),
            DMA((3,)),
            DMA((2, 3)),
            DMA((2, 3)),
            DMA((2, 3)),
            DMA((2, 3)),
            pltpu.VMEM((2, nblk * t, 2 * t), BF),
            DMA((2,)),
        ],
        compiler_params=talks(1),
        name="back",
    )(gu_part, wd_part, dn_part, out_part, middle, cot_own, x16, fac, wo, attn_t, normed_t,
      attn_f, inv, probs, q_t, kv, a_t, b_t, cosine, sine)
    gu_own = gu_own.astype(F32).transpose(1, 2, 0, 3).reshape(2, rows, ff)
    return (
        layer_output.reshape(1, t, width),
        input_grad.reshape(1, t, width),
        last_own[:, FDIM],
        last_own[:, :FDIM],
        out_own,
        last_own[:, FDIM + 1],
        gu_own[0],
        gu_own[1],
        down_sum,
    )


def solution(mesh):
    return jax.shard_map(
        body,
        mesh=mesh,
        in_specs=(
            P("dp", "ctx", None),
            P("dp", None),
            P(("dp", "ctx")),
            P(("dp", "ctx"), None),
            P(("dp", "ctx"), None),
            P(("dp", "ctx")),
            P(("dp", "ctx"), None),
            P(("dp", "ctx"), None),
            P(("dp", "ctx"), None),
            P("dp", "ctx", None),
        ),
        out_specs=(
            P("dp", "ctx", None),
            P("dp", "ctx", None),
            P(("dp", "ctx")),
            P(("dp", "ctx"), None),
            P(("dp", "ctx"), None),
            P(("dp", "ctx")),
            P(("dp", "ctx"), None),
            P(("dp", "ctx"), None),
            P(("dp", "ctx"), None),
        ),
        check_vma=False,
    )
```

```python
import functools

import jax
import jax.numpy as jnp
import numpy as np
from jax import lax
from jax.experimental import pallas as pl
from jax.experimental.pallas import tpu as pltpu
from jax.sharding import PartitionSpec as P

H = 16
DH = 64
RQ = 6
RKV = 2
EPS = 1e-05
BF = jnp.bfloat16
F32 = jnp.float32
AQ = RQ * H
BQ = RQ * DH
AK = RKV * H
BK = RKV * DH
PACK = 2 * (AK + BK)
KEY_ROWS = AK + BK
FDIM = AQ + BQ + PACK
FPAD = 896
LOG2E = 1.4426950408889634
NEG = -1e30


def nt(a, b):
    return lax.dot_general(a, b, (((1,), (1,)), ((), ())), preferred_element_type=F32)


def nn(a, b):
    return jnp.dot(a, b, preferred_element_type=F32)

MESH = pl.DeviceIdType.MESH


def ring_place(c, n):
    z = c // 2
    return z + (c % 2) * (n - 1 - 2 * z)


def ring_index(p, n):
    p = (p + 2 * n) % n
    q = p // (n // 2)
    return (1 - q) * (2 * p) + q * (2 * (n - 1 - p) + 1)


def remote(src, dst, send, recv, dev):
    return pltpu.make_async_remote_copy(
        src_ref=src, dst_ref=dst, send_sem=send, recv_sem=recv, device_id=dev, device_id_type=MESH
    )


def places():
    d, c = lax.axis_index("dp"), lax.axis_index("ctx")
    core = d % 2
    return d, c, core, d + 1 - 2 * core, (d + 2) % 4


def meet(n, near):
    d, c, _, _, _ = places()
    barrier = pltpu.get_barrier_semaphore()
    count = 0
    n_dp = lax.axis_size("dp")
    for k in range(1, n_dp):
        pl.semaphore_signal(barrier, inc=1, device_id=((d + k) % n_dp, c), device_id_type=MESH)
        count += 1
    if near:
        r = ring_place(c, n)
        for way in (1, -1):
            pl.semaphore_signal(
                barrier, inc=1, device_id=(d, ring_index(r + way, n)), device_id_type=MESH
            )
            count += 1
    else:
        for k in range(1, n):
            pl.semaphore_signal(barrier, inc=1, device_id=(d, (c + k) % n), device_id_type=MESH)
            count += 1
    pl.semaphore_wait(barrier, count)


def steps(lo, hi, step):
    if isinstance(lo, int) and isinstance(hi, int) and hi - lo <= 4:
        for s in range(lo, hi):
            step(s)
    elif not (isinstance(lo, int) and isinstance(hi, int) and hi <= lo):
        lax.fori_loop(lo, hi, lambda s, _: (step(s), _)[1], 0)


class GatherRing:
    def __init__(self, n, slot, half, send, recv):
        self.n, self.h, self.slot, self.half, self.send, self.recv = n, n // 2, slot, half, send, recv
        self.d, c, _, _, _ = places()
        self.r = ring_place(c, n)

    def copy(self, s, i, arriving=False):
        way = 1 - 2 * i
        last = isinstance(s, int) and s == self.h - 1
        owner = ring_index(self.r - way * (s + (1 if arriving else 0)), self.n)
        ref = self.half(owner, i) if last else self.slot(owner)
        to = (self.d, ring_index(self.r + way, self.n))
        return remote(ref, ref, self.send.at[i, s], self.recv.at[i, s], to)

    def start(self, s):
        for i in range(2):
            self.copy(s, i).start()

    def arrive(self, s):
        for i in range(2):
            self.copy(s, i, True).wait_recv()

    def step(self, s):
        for i in range(2):
            self.copy(s - 1, i, True).wait_recv()
            self.copy(s, i).start()

    def last(self):
        self.step(self.h - 1)

    def drain(self):
        steps(0, self.h - 1, lambda s: [self.copy(s, i).wait_send() for i in range(2)])
        for i in range(2):
            self.copy(self.h - 1, i).wait_send()


class ScatterRing:
    def __init__(self, n, part, half, land, whole_of, half_of, send, recv):
        self.n, self.h, self.part, self.half = n, n // 2, part, half
        self.land, self.whole_of, self.half_of = land, whole_of, half_of
        self.send, self.recv = send, recv
        self.d, c, _, _, _ = places()
        self.c, self.r = c, ring_place(c, n)

    def copy(self, s, i):
        way = 1 - 2 * i
        to = (self.d, ring_index(self.r + way, self.n))
        first = isinstance(s, int) and s == 0
        if first:
            owner = ring_index(self.r + way * self.h, self.n)
            src, dst = self.half(owner, i), self.half_of(self.land.at[i, 0], i)
        else:
            src, dst = self.land.at[i, s - 1], self.land.at[i, s]
        return remote(src, dst, self.send.at[i, s], self.recv.at[i, s], to)

    def start(self):
        for i in range(2):
            self.copy(0, i).start()

    def step(self, s):
        first = isinstance(s, int) and s == 1
        for i in range(2):
            way = 1 - 2 * i
            self.copy(s - 1, i).wait_recv()
            owner = ring_index(self.r + way * (self.h - s), self.n)
            held = self.land.at[i, s - 1]
            if first:
                mine = self.half_of(held, i)
                mine[...] = (mine[...].astype(F32) + self.half(owner, i)[...].astype(F32)).astype(BF)
                self.half_of(held, 1 - i)[...] = self.half(owner, 1 - i)[...]
            else:
                held[...] = (held[...].astype(F32) + self.part(owner)[...].astype(F32)).astype(BF)
            self.copy(s, i).start()

    def rest(self, lo, hi):
        if lo == 1 and hi > 1:
            self.step(1)
            lo = 2
        steps(lo, hi, self.step)

    def result(self):
        for i in range(2):
            self.copy(self.h - 1, i).wait_recv()
        out = self.part(self.c)[...].astype(F32)
        for i in range(2):
            out = out + self.land[i, self.h - 1].astype(F32)
        return out

    def drain(self):
        for i in range(2):
            self.copy(0, i).wait_send()
        steps(1, self.h, lambda s: [self.copy(s, i).wait_send() for i in range(2)])


class Spread:
    def __init__(self, ref, send, recv):
        d, c, _, cd, xd = places()
        self.copies = [
            remote(ref.at[d], ref.at[d], send.at[0], recv.at[0], (cd, c)),
            remote(ref.at[d], ref.at[d], send.at[1], recv.at[1], (xd, c)),
            remote(ref.at[xd], ref.at[xd], send.at[2], recv.at[2], (cd, c)),
        ]

    def start(self):
        self.copies[1].start()
        self.copies[0].start()

    def forward(self):
        self.copies[1].wait_recv()
        self.copies[2].start()

    def finish(self):
        self.copies[0].wait_recv()
        self.copies[2].wait_recv()
        for copy in self.copies:
            copy.wait_send()


def blocks(count, step, state):
    if count <= 8:
        for j in range(count):
            state = step(j, state)
        return state
    return lax.fori_loop(0, count, step, state)


def lane_block(j, size):
    if isinstance(j, int):
        return pl.ds(j * size, size)
    return pl.ds(pl.multiple_of(j * size, size), size)


def rope(b, cosine, sine, ranks):
    parts = []
    half = DH // 2
    for r in range(ranks):
        u1 = b[r * DH : r * DH + half]
        u2 = b[r * DH + half : (r + 1) * DH]
        parts += [u1 * cosine - u2 * sine, u2 * cosine + u1 * sine]
    return jnp.concatenate(parts, axis=0)


def rope_back(v, cosine, sine, ranks):
    return rope(v, cosine, -sine, ranks)


def pre_part(x, g1, w, cosine, sine, nt_ref, q_ref, p_ref, a_ref, b_ref):
    r1 = lax.rsqrt(jnp.mean(x * x, axis=-1, keepdims=True) + EPS)
    n = (x * r1 * g1).astype(BF)
    nt_ref[...] = n.T
    ft = nn(n, w).T
    a = ft[:AQ]
    b = rope(ft[AQ : AQ + BQ], cosine, sine, RQ)
    for i in range(AQ):
        a_ref[i] = a[i : i + 1]
    b_ref[...] = b
    k0 = AQ + BQ
    bk = rope(ft[k0 + AK : k0 + AK + BK], cosine, sine, RKV)
    p_ref[...] = jnp.concatenate(
        [ft[k0 : k0 + AK], bk, ft[k0 + KEY_ROWS : k0 + PACK]], axis=0
    ).astype(BF)
    for h in range(H):
        acc = a[h : h + 1] * b[:DH]
        for r in range(1, RQ):
            acc = acc + a[r * H + h : r * H + h + 1] * b[r * DH : (r + 1) * DH]
        q_ref[h * DH : (h + 1) * DH, :] = (acc * (1.0 / RQ)).astype(BF)


def vectors(kv_ref, side, r, lanes):
    first = side * KEY_ROWS + AK + r * DH
    return kv_ref[first : first + DH, lanes].astype(F32)


def expand_pair(ka, kv_ref, side, p, lanes):
    rows = []
    for hh in range(2):
        acc = 0.0
        for r in range(RKV):
            a = ka[side * AK + r * H + 2 * p + hh, :, lanes]
            b = vectors(kv_ref, side, r, lanes)
            acc = acc + a * b
        rows.append(acc * (1.0 / RKV))
    return jnp.concatenate(rows, axis=0)


def unpack(kv_ref, ka):
    for side in range(2):
        first = side * KEY_ROWS
        a = kv_ref[first : first + AK, :].astype(F32)
        for i in range(AK):
            ka[side * AK + i] = a[i : i + 1]


def diagonal(pair):
    zero = jnp.zeros((DH, pair.shape[1]), pair.dtype)
    left = jnp.concatenate([pair[:DH], zero], axis=0)
    right = jnp.concatenate([zero, pair[DH:]], axis=0)
    return jnp.concatenate([left, right], axis=1)


def undiagonal(wide):
    t = wide.shape[1] // 2
    return jnp.concatenate([wide[:DH, :t], wide[DH:, t:]], axis=0)


def attend_part(nblk, len_ref, q_ref, kv_ref, at_ref, af_ref, inv_ref, p_out, pbuf, ka, bias):
    t = q_ref.shape[1]
    c = lax.axis_index("ctx")
    tpos = c * t + lax.broadcasted_iota(jnp.int32, (1, t), 1)
    start = jnp.zeros((1, t), jnp.int32)
    run = jnp.int32(0)
    for j in range(len_ref.shape[1]):
        start = jnp.where(tpos >= run, run, start)
        run = run + len_ref[0, j]
    unpack(kv_ref, ka)

    def bias_block(j, _):
        spos = (c - nblk + 1 + j) * t + lax.broadcasted_iota(jnp.int32, (t, t), 0)
        ok = (spos >= start) & (spos <= tpos)
        bias[lane_block(j, t), :] = jnp.where(ok, 0.0, NEG)
        return _

    blocks(nblk, bias_block, 0)

    def pair(p, carry):
        @pl.when(p > 1)
        def _():
            p_out(p - 2).wait()

        rows = pl.ds(pl.multiple_of(p * 2 * DH, 2 * DH), 2 * DH)
        qd = diagonal(q_ref[rows, :])

        def step(j, state):
            num, tot = state
            lanes = lane_block(j, t)
            k = expand_pair(ka, kv_ref, 0, p, lanes).T.astype(BF)
            v = expand_pair(ka, kv_ref, 1, p, lanes).astype(BF)
            b = bias[lanes, :]
            s = nn(k, qd) * (LOG2E * DH**-0.5) + jnp.concatenate([b, b], axis=1)
            e = jnp.exp2(s)
            tot = tot + jnp.sum(e, axis=0, keepdims=True)
            pb = e.astype(BF)
            pbuf[p % 2, lanes, :] = pb
            return (num + nn(v, pb), tot)

        num, tot = blocks(
            nblk, step, (jnp.zeros((2 * DH, 2 * t), F32), jnp.zeros((1, 2 * t), F32))
        )
        inv = 1.0 / tot
        af = undiagonal(num * inv)
        af_ref[rows, :] = af
        at_ref[rows, :] = af.astype(BF)
        p_out(p).start()
        inv_ref[p] = jnp.broadcast_to(inv, (8, 2 * t))
        return carry

    lax.fori_loop(0, H // 2, pair, 0)
    for p in range(H // 2 - 2, H // 2):
        p_out(p).wait()


def attend_back_part(
    nblk, serve, da_ref, af_ref, inv_ref, p_copy, pbuf, q_ref, kv_ref, a_ref, b_ref, cos_ref, sin_ref,
    dq_ref, dkv_ref, ka, dka, dqa, db,
):
    t = q_ref.shape[1]
    unpack(kv_ref, ka)
    db[...] = jnp.zeros_like(db)
    for side in range(2):
        first = side * KEY_ROWS + AK
        dkv_ref[first : first + BK, :] = jnp.zeros((BK, nblk * t), F32)

    def factor_back(dwide, side, p, lanes):
        for hh in range(2):
            d = dwide[hh * DH : (hh + 1) * DH] * (1.0 / RKV)
            for r in range(RKV):
                row = side * AK + r * H + 2 * p + hh
                first = side * KEY_ROWS + AK + r * DH
                b = vectors(kv_ref, side, r, lanes)
                dka[row, :, lanes] = jnp.sum(d * b, axis=0, keepdims=True)
                dkv_ref[first : first + DH, lanes] += d * ka[row, :, lanes]

    def pair(p, carry):
        @pl.when(p + 1 < H // 2)
        def _():
            p_copy(p + 1).start()

        p_copy(p).wait()
        rows = pl.ds(pl.multiple_of(p * 2 * DH, 2 * DH), 2 * DH)
        da = da_ref[rows, :]
        inv = inv_ref[p][:1]
        dd = diagonal(da)
        dn = (dd * inv).astype(BF)
        dtot = -jnp.sum(dd * diagonal(af_ref[rows, :]), axis=0, keepdims=True) * inv
        qd = diagonal(q_ref[rows, :])

        def step(j, dq):
            lanes = lane_block(j, t)
            k = expand_pair(ka, kv_ref, 0, p, lanes).astype(BF)
            v = expand_pair(ka, kv_ref, 1, p, lanes).T.astype(BF)
            pb = pbuf[p % 2, lanes, :]
            ds = (pb.astype(F32) * (nn(v, dn) + dtot)).astype(BF)
            dq = dq + nn(k, ds)
            factor_back(nt(qd, ds) * (DH**-0.5), 0, p, lanes)
            factor_back(nt(dn, pb), 1, p, lanes)
            return dq

        dq = undiagonal(blocks(nblk, step, jnp.zeros((2 * DH, 2 * t), F32)))
        dq = dq * (DH**-0.5 / RQ)
        for hh in range(2):
            d = dq[hh * DH : (hh + 1) * DH]
            for r in range(RQ):
                row = r * H + 2 * p + hh
                dqa[row] = jnp.sum(d * b_ref[r * DH : (r + 1) * DH, :], axis=0, keepdims=True)
                db[r * DH : (r + 1) * DH, :] += d * a_ref[row]
        serve(p)
        return carry

    lax.fori_loop(0, H // 2, pair, 0)
    for i in range(AQ):
        dq_ref[i : i + 1, :] = dqa[i]
    for side in range(2):
        for i in range(AK):
            dkv_ref[side * KEY_ROWS + i : side * KEY_ROWS + i + 1, :] = dka[side * AK + i]
    dq_ref[AQ : AQ + BQ, :] = rope_back(db[...], cos_ref[...], sin_ref[...], RQ)


def gain_rows(w):
    first = FPAD - 128
    gains = w[:, first:].astype(F32).T
    return gains[FDIM - first : FDIM - first + 1], gains[FDIM - first + 1 : FDIM - first + 2]


class PairScatter:
    def __init__(self, n, part, held, land, own, send, recv, ring_send, ring_recv):
        d, c, core, cd, xd = places()
        self.core, self.x, self.part, self.held, self.own = core, d // 2, part, held, own
        self.swaps = [
            remote(part.at[2 * xx + 1 - core], held.at[xx], send.at[xx], recv.at[xx], (cd, c))
            for xx in range(2)
        ]
        self.end = remote(own.at[1 - self.x], own.at[2], send.at[2], recv.at[2], (xd, c))
        self.ring = ScatterRing(
            n, lambda o: held.at[:, o], lambda o, w: held.at[w, o], land,
            None, lambda ref, w: ref.at[w], ring_send, ring_recv,
        )

    def start(self):
        for swap in self.swaps:
            swap.start()

    def enter(self):
        for xx in range(2):
            self.swaps[xx].wait_recv()
            mine = self.part[2 * xx + self.core].astype(F32)
            self.held[xx] = (self.held[xx].astype(F32) + mine).astype(BF)
        self.ring.start()

    def leave(self):
        total = self.ring.result()
        for xx in range(2):
            self.own[xx] = total[xx].astype(BF)
        self.end.start()

    def result(self):
        self.end.wait_recv()
        return self.own[self.x].astype(F32) + self.own[2].astype(F32)

    def drain(self):
        for copy in self.swaps + [self.end]:
            copy.wait_send()
        self.ring.drain()


def block_kernel(
    n, nblk,
    len_ref, x_ref, cos_ref, sin_ref, fac_in, wo_in, gu_in, wd_in, cot_in,
    y_ref, dx_ref, fac_ref, wo_ref, gu_ref, wd_ref, p_ref,
    nt_ref, q_ref, a_ref, b_ref, kv_ref, at_ref, af_ref, inv_ref, pbuf,
    fac, wo, gu, wd, nm, cot, mid_ref, dn_in, out_in, gu_part, wd_part,
    kv_land, gu_land, wd_land, gu_own, da_ref, dq_ref, dmid_ref, dp_land,
    fac_part, wo_part, fac_held, wo_held, fac_land, wo_land, fac_own, wo_own,
    own_sem, near_send, near_recv, ring_send, ring_recv, kv_send, kv_recv, sp_send, sp_recv,
    dkv_send, dkv_recv, end_send, end_recv, dp_send, dp_recv, pair_send, pair_recv, p_sem, own_dkv,
):
    d, c, core, cd, xd = places()
    t = x_ref.shape[0]
    n_dp = 4
    locals_ = [
        pltpu.make_async_copy(fac_in, fac.at[d, c], own_sem.at[0]),
        pltpu.make_async_copy(wo_in, wo.at[d, c], own_sem.at[1]),
        pltpu.make_async_copy(gu_in.at[d], gu.at[:, d, c], own_sem.at[2]),
        pltpu.make_async_copy(wd_in, wd.at[c], own_sem.at[3]),
        pltpu.make_async_copy(cot_in, cot.at[d], own_sem.at[4]),
    ]
    for copy in locals_:
        copy.start()
    for k in range(1, nblk):
        @pl.when(c - k < 0)
        def _():
            kv_ref[:, (nblk - 1 - k) * t : (nblk - k) * t] = jnp.zeros((PACK, t), BF)
    meet(n, False)
    for copy in locals_:
        copy.wait()

    def ring(i, slot, half):
        return GatherRing(n, slot, half, ring_send.at[i], ring_recv.at[i])

    rows = fac_in.shape[0] // 2

    def shard(ref, dd):
        return (lambda o: ref.at[dd, o]), (lambda o, w: ref.at[dd, o, w * rows : (w + 1) * rows])

    fo, fx = ring(0, *shard(fac, d)), ring(1, *shard(fac, xd))
    oo, ox = ring(2, *shard(wo, d)), ring(3, *shard(wo, xd))
    cut = -(-wd_in.shape[0] // 16) * 8
    gr = ring(4, lambda o: gu.at[:, :, o], lambda o, w: gu.at[w, :, o])
    dr = ring(
        5, lambda o: wd.at[o],
        lambda o, w: wd.at[o, :cut] if w == 0 else wd.at[o, cut:],
    )
    small, large = (fo, fx, oo, ox), (gr, dr)
    fswap = remote(fac.at[d, c], fac.at[d, c], near_send.at[0], near_recv.at[0], (xd, c))
    oswap = remote(wo.at[d, c], wo.at[d, c], near_send.at[1], near_recv.at[1], (xd, c))
    fswap.start()
    oswap.start()
    fo.start(0)
    oo.start(0)
    a2a = []
    for k in range(1, n_dp):
        to = (d + k) % n_dp
        a2a.append(
            (
                remote(gu_in.at[to], gu.at[:, d, c], near_send.at[1 + k], near_recv.at[1 + k], (to, c)),
                remote(
                    gu_in.at[to], gu.at[:, (d + n_dp - k) % n_dp, c],
                    near_send.at[1 + k], near_recv.at[1 + k], (to, c),
                ),
            )
        )
        a2a[-1][0].start()
    cots = Spread(cot, sp_send.at[0], sp_recv.at[0])
    nms = Spread(nm, sp_send.at[1], sp_recv.at[1])
    cots.start()
    fswap.wait_recv()
    fx.start(0)
    oswap.wait_recv()
    ox.start(0)
    steps(1, n // 2 - 1, lambda s: [one.step(s) for one in small])
    for one in small:
        one.last()
    for _, arrival in a2a:
        arrival.wait_recv()
    for one in large:
        one.start(0)
    def core_swap(ref, i, dd, da):
        return (
            remote(ref.at[dd], ref.at[dd], near_send.at[5 + i], near_recv.at[5 + i], (cd, c)),
            remote(ref.at[da], ref.at[da], near_send.at[5 + i], near_recv.at[5 + i], (cd, c)),
        )

    near = []
    for i, (one, ref, dd, da) in enumerate(
        ((fo, fac, d, cd), (fx, fac, xd, (cd + 2) % 4), (oo, wo, d, cd), (ox, wo, xd, (cd + 2) % 4))
    ):
        one.arrive(n // 2 - 1)
        near.append(core_swap(ref, i, dd, da))
        near[-1][0].start()
    cots.forward()
    for _, arrival in near[:2]:
        arrival.wait_recv()

    width = x_ref.shape[1]
    x = x_ref[...].astype(F32)
    w = fac[...].reshape(width, FPAD)
    g1, g2 = gain_rows(w)
    own_kv = kv_ref.at[:, (nblk - 1) * t : nblk * t]
    pre_part(x, g1, w, cos_ref[...], sin_ref[...], nt_ref, q_ref, own_kv, a_ref, b_ref)

    def kv_copy(k):
        dst = kv_ref.at[:, (nblk - 1 - k) * t : (nblk - k) * t]
        return remote(own_kv, dst, kv_send.at[k - 1], kv_recv.at[k - 1], (d, (c + k) % n))

    for k in range(1, nblk):
        @pl.when(c + k < n)
        def _():
            kv_copy(k).start()
    for k in range(1, nblk):
        @pl.when(c - k >= 0)
        def _():
            kv_copy(k).wait_recv()

    def p_out(p):
        return pltpu.make_async_copy(pbuf.at[p % 2], p_ref.at[p], p_sem.at[p % 2])

    pl.run_scoped(
        functools.partial(
            attend_part, nblk, len_ref, q_ref, kv_ref, at_ref, af_ref, inv_ref, p_out, pbuf
        ),
        pltpu.VMEM((2 * AK, 1, nblk * t), F32),
        pltpu.VMEM((nblk * t, t), F32),
    )

    full = n // 2 - 1
    middle_step = 1 + full // 2
    steps(1, middle_step, lambda s: [one.step(s) for one in large])
    for _, arrival in near[2:]:
        arrival.wait_recv()
    middle = x + nn(at_ref[...].T, wo[...].reshape(width, width))
    mid_ref[...] = middle
    r2 = lax.rsqrt(jnp.mean(middle * middle, axis=-1, keepdims=True) + EPS)
    nm[d] = (middle * r2 * g2).astype(BF)
    nms.start()
    nms.forward()
    nms.finish()
    cots.finish()
    steps(middle_step, full, lambda s: [one.step(s) for one in large])
    for one in large:
        one.last()
    for one in large:
        one.arrive(n // 2 - 1)

    x_at = d // 2
    parts = (dn_in, out_in)
    first = []
    for i, part in enumerate(parts):
        for j, xx in enumerate((1 - x_at, x_at)):
            first.append(
                remote(
                    part.at[2 * xx + 1 - core], dp_land.at[i, j],
                    dp_send.at[i, j], dp_recv.at[i, j], (cd, c),
                )
            )
    ffq = gu_in.shape[3]

    def feed(gate, up, dh, hid, dg, du):
        wg, wu = (gu.at[side] for side in range(2))

        def matrix(ref):
            return ref[...].reshape(width, ffq)

        down = wd[...].reshape(ffq, width)

        def pair_rows(i, carry):
            xx = i * x_at + (1 - i) * (1 - x_at)
            two = pl.ds(2 * xx, 2)
            both = 2 * t
            nm_two = nm[two].reshape(both, width)
            gate[...] = nn(nm_two, matrix(wg))
            up[...] = nn(nm_two, matrix(wu))
            dh[...] = nt(cot[two].reshape(both, width), down)
            base = pl.multiple_of(xx * both, both)

            def rows_of(k, carry):
                some = pl.ds(pl.multiple_of(k * 32, 32), 32)
                to = pl.ds(pl.multiple_of(base + k * 32, 32), 32)
                v, u, g = gate[some, :], up[some, :], dh[some, :]
                sig, act = silu_parts(v)
                hid[to, :] = (act * u).astype(BF)
                dg[to, :] = (g * u * sig * (1.0 + v * (1.0 - sig))).astype(BF)
                du[to, :] = (g * act).astype(BF)
                return carry

            lax.fori_loop(0, both // 32, rows_of, 0)
            all_rows = pl.ds(base, both)
            dn = nt(dg[all_rows, :], matrix(wg)) + nt(du[all_rows, :], matrix(wu))
            dn_in[two] = dn.astype(BF).reshape(2, t, width)
            out_in[two] = nn(hid[all_rows, :], down).astype(BF).reshape(2, t, width)

            @pl.when(i == 0)
            def _():
                first[0].start()
                first[2].start()

            return carry

        lax.fori_loop(0, 2, pair_rows, 0)
        first[1].start()
        first[3].start()
        for i, part in enumerate(parts):
            first[2 * i].wait_recv()
            dp_land[i, 0] = (dp_land[i, 0].astype(F32) + part[xd].astype(F32)).astype(BF)
            dp_next(i).start()

        def tn(a, b):
            return lax.dot_general(a, b, (((0,), (0,)), ((), ())), preferred_element_type=F32)

        quarter = width // n_dp

        def columns(j, carry):
            lanes = pl.ds(pl.multiple_of(j * quarter, quarter), quarter)
            some = nm[:, :, lanes].reshape(n_dp * t, quarter)
            shape = gu_part.shape[2:]
            gu_part[0, j] = tn(some, dg[...]).astype(BF).reshape(shape)
            gu_part[1, j] = tn(some, du[...]).astype(BF).reshape(shape)
            c_some = cot[:, :, lanes].reshape(n_dp * t, quarter)
            wd_part[:, :, lanes] = tn(hid[...], c_some).astype(BF).reshape(wd_part.shape[:2] + (quarter,))
            return carry

        lax.fori_loop(0, n_dp, columns, 0)

    def dp_next(i):
        return remote(dp_land.at[i, 0], dp_land.at[i, 2], dp_send.at[i, 2], dp_recv.at[i, 2], (xd, c))

    pl.run_scoped(
        feed,
        *[pltpu.VMEM((2 * t, ffq), F32)] * 3,
        *[pltpu.VMEM((n_dp * t, ffq), BF)] * 3,
    )
    second = [dp_next(i) for i in range(2)]
    cut = -(-wd_part.shape[1] // 16) * 8

    def wd_half(ref, w):
        return ref.at[:cut] if w == 0 else ref.at[cut:]

    gs = ScatterRing(
        n, lambda o: gu_part.at[:, :, o], lambda o, w: gu_part.at[w, :, o], gu_land,
        None, lambda ref, w: ref.at[w], ring_send.at[6], ring_recv.at[6],
    )
    ds_ = ScatterRing(
        n, lambda o: wd_part.at[o], lambda o, w: wd_half(wd_part.at[o], w), wd_land,
        None, wd_half, ring_send.at[7], ring_recv.at[7],
    )
    scatter = (gs, ds_)
    for one in scatter:
        one.start()
    fs = PairScatter(
        n, fac_part, fac_held, fac_land, fac_own, pair_send.at[0], pair_recv.at[0],
        ring_send.at[8], ring_recv.at[8],
    )
    ws = PairScatter(
        n, wo_part, wo_held, wo_land, wo_own, pair_send.at[1], pair_recv.at[1],
        ring_send.at[9], ring_recv.at[9],
    )
    h = n // 2

    def advance(s):
        for one in scatter:
            one.step(s)

    advance(1)
    for i in range(2):
        first[2 * i + 1].wait_recv()
    second[0].wait_recv()
    middle = mid_ref[...]
    dn = dn_in[d].astype(F32) + dp_land[0, 1].astype(F32) + dp_land[0, 2].astype(F32)
    second_part = jnp.sum(dn * middle * r2, axis=0, keepdims=True)
    u2 = dn * g2
    d_middle = (
        cot_in[...].astype(F32)
        + r2 * u2
        - middle * (r2 * r2 * r2 * jnp.mean(u2 * middle, axis=-1, keepdims=True))
    )
    dmid_ref[...] = d_middle
    d_branch = d_middle.astype(BF)
    wo_part[...] = nn(at_ref[...], d_branch).astype(BF).reshape(wo_part.shape)
    ws.start()
    da_ref[...] = nt(wo[...].reshape(width, width), d_branch)
    second[1].wait_recv()
    y_ref[...] = (
        mid_ref[...]
        + (out_in[d].astype(F32) + dp_land[1, 1].astype(F32) + dp_land[1, 2].astype(F32))
    ).astype(BF)
    ws.enter()
    points = 3

    def serve(k):
        steps(2 + -(-(k - 1) * (h - 2) // points), 2 + -(-k * (h - 2) // points), advance)

    serve(1)

    def serve_pair(p):
        @pl.when(p == H // 2 - 3)
        def _():
            ws.ring.step(1)
            serve(2)

    def p_copy(p):
        return pltpu.make_async_copy(p_ref.at[p], pbuf.at[p % 2], p_sem.at[p % 2])

    p_copy(0).start()

    def attention_back(ka, dka, dqa, db, dkv, dkv16):
        attend_back_part(
            nblk, serve_pair, da_ref, af_ref, inv_ref, p_copy, pbuf, q_ref, kv_ref, a_ref, b_ref,
            cos_ref, sin_ref, dq_ref, dkv, ka, dka, dqa, db,
        )
        dkv16[...] = dkv[...].astype(BF)

        def dkv_copy(k):
            src = dkv16.at[:, (nblk - 1 - k) * t : (nblk - k) * t]
            return remote(
                src, kv_land.at[k - 1], dkv_send.at[k - 1], dkv_recv.at[k - 1], (d, (c + n - k) % n)
            )

        for k in range(1, nblk):
            @pl.when(c - k >= 0)
            def _():
                dkv_copy(k).start()
        serve(3)
        own_dkv[...] = dkv[:, (nblk - 1) * t :]
        for k in range(1, nblk):
            @pl.when(c + k < n)
            def _():
                dkv_copy(k).wait_recv()
                own_dkv[...] += kv_land[k - 1].astype(F32)
        for k in range(1, nblk):
            @pl.when(c - k >= 0)
            def _():
                dkv_copy(k).wait_send()

    pl.run_scoped(
        attention_back,
        pltpu.VMEM((2 * AK, 1, nblk * t), F32),
        pltpu.VMEM((2 * AK, 1, nblk * t), F32),
        pltpu.VMEM((AQ, 1, t), F32),
        pltpu.VMEM((BQ, t), F32),
        pltpu.VMEM((PACK, nblk * t), F32),
        pltpu.VMEM((PACK, nblk * t), BF),
    )
    steps(2, h, ws.ring.step)
    dp = own_dkv[...]
    d_bk = rope_back(dp[AK : AK + BK], cos_ref[...], sin_ref[...], RKV)
    d_fac_t = jnp.concatenate(
        [dq_ref[...], dp[:AK], d_bk, dp[KEY_ROWS:], jnp.zeros((FPAD - FDIM, t), F32)], axis=0
    ).astype(BF)
    x = x_ref[...].astype(F32)
    r1 = lax.rsqrt(jnp.mean(x * x, axis=-1, keepdims=True) + EPS)
    d_norm_in = nt(d_fac_t.T, w)
    first_part = jnp.sum(d_norm_in * x * r1, axis=0, keepdims=True)
    tail = FPAD - 128
    gains = jnp.concatenate(
        [jnp.zeros((FDIM - tail, width), F32), first_part, second_part,
         jnp.zeros((FPAD - FDIM - 2, width), F32)], axis=0).T
    product = nt(nt_ref[...], d_fac_t)
    shape = fac_part.shape[:3]
    fac_part[:, :, :, :tail] = product[:, :tail].astype(BF).reshape(shape + (tail,))
    fac_part[:, :, :, tail:] = (product[:, tail:] + gains).astype(BF).reshape(shape + (128,))
    fs.start()
    u1 = d_norm_in * g1
    dx_ref[...] = (
        dmid_ref[...] + r1 * u1 - x * (r1 * r1 * r1 * jnp.mean(u1 * x, axis=-1, keepdims=True))
    ).astype(BF)
    fs.enter()
    total = gs.result().astype(BF)
    for dd in range(n_dp):
        gu_own[dd] = total[:, dd]
    keep = pltpu.make_async_copy(gu_own.at[d], gu_ref.at[d], own_sem.at[0])
    keep.start()
    last = []
    for k in range(1, n_dp):
        to = (d + k) % n_dp
        last.append(
            (
                remote(gu_own.at[to], gu_ref.at[d], end_send.at[k - 1], end_recv.at[k - 1], (to, c)),
                remote(
                    gu_own.at[to], gu_ref.at[(d + n_dp - k) % n_dp],
                    end_send.at[k - 1], end_recv.at[k - 1], (to, c),
                ),
            )
        )
        last[-1][0].start()
    ws.leave()
    fs.ring.step(1)
    wd_ref[...] = ds_.result()
    steps(2, h, fs.ring.step)
    wo_ref[...] = ws.result()
    fs.leave()
    for out, arrival in last:
        arrival.wait_recv()
        out.wait_send()
    keep.wait()
    fac_ref[...] = fs.result()
    for copy in first + second:
        copy.wait_send()
    for one in scatter + (ws, fs):
        one.drain()
    for k in range(1, nblk):
        @pl.when(c + k < n)
        def _():
            kv_copy(k).wait_send()
    fswap.wait_send()
    oswap.wait_send()
    for out, _ in a2a + near:
        out.wait_send()
    for one in small + large:
        one.drain()


def vmem(n):
    return [pl.BlockSpec(memory_space=pltpu.VMEM)] * n


def hbm(n):
    return [pl.BlockSpec(memory_space=pl.ANY)] * n


SMEM = pl.BlockSpec(memory_space=pltpu.SMEM)
DMA = pltpu.SemaphoreType.DMA


def talks(i):
    return pltpu.CompilerParams(
        collective_id=i, has_side_effects=True, vmem_limit_bytes=63 * 1024 * 1024
    )


def silu_parts(gate):
    s = jax.nn.sigmoid(gate)
    return s, gate * s


def body(
    tokens,
    doc_lengths,
    first_gain,
    factor_weights,
    output_weights,
    second_gain,
    gate_weights,
    up_weights,
    down_weights,
    cotangent,
):
    _, t, width = tokens.shape
    n_ctx, n_dp = lax.axis_size("ctx"), lax.axis_size("dp")
    n_all = n_ctx * n_dp
    both = ("dp", "ctx")
    length = t * n_ctx
    nblk = min(n_ctx, -(-(length // 2 - 1) // t) + 1)
    ff = gate_weights.shape[1]
    ffq = ff // n_dp
    rows = width // n_all
    c = lax.axis_index("ctx")

    h = n_ctx // 2

    pack = jnp.concatenate(
        [factor_weights, first_gain[:, None], second_gain[:, None],
         jnp.zeros((rows, FPAD - FDIM - 2), F32)], axis=1).astype(BF)
    gu_in = jnp.stack([gate_weights, up_weights]).astype(BF).reshape(2, rows, n_dp, ffq)
    gu_in = gu_in.transpose(2, 0, 1, 3)

    half = DH // 2
    freq = 10000.0 ** (-(np.arange(half) * 2.0 / DH))
    pos = (c * t + jnp.arange(t, dtype=jnp.int32)).astype(F32)
    angles = jnp.asarray(freq, F32)[:, None] * pos[None, :]
    cosine, sine = jnp.cos(angles), jnp.sin(angles)

    x16 = tokens.reshape(t, width)
    cot_own = cotangent.reshape(t, width)
    sds = jax.ShapeDtypeStruct
    down_rows = down_weights.shape[0]
    outs = pl.pallas_call(
        functools.partial(block_kernel, n_ctx, nblk),
        out_shape=(
            sds((t, width), BF),
            sds((t, width), BF),
            sds((rows, FPAD), F32),
            sds((rows, width), F32),
            sds((n_dp, 2, rows, ffq), BF),
            sds((down_rows, width), F32),
            sds((H // 2, nblk * t, 2 * t), BF),
        ),
        in_specs=[SMEM] + vmem(8),
        out_specs=tuple(vmem(6) + hbm(1)),
        scratch_shapes=[
            pltpu.VMEM((width, t), BF),
            pltpu.VMEM((H * DH, t), BF),
            pltpu.VMEM((AQ, 1, t), F32),
            pltpu.VMEM((BQ, t), F32),
            pltpu.VMEM((PACK, nblk * t), BF),
            pltpu.VMEM((H * DH, t), BF),
            pltpu.VMEM((H * DH, t), F32),
            pltpu.VMEM((H // 2, 8, 2 * t), F32),
            pltpu.VMEM((2, nblk * t, 2 * t), BF),
            pltpu.VMEM((n_dp, n_ctx, rows, FPAD), BF),
            pltpu.VMEM((n_dp, n_ctx, rows, width), BF),
            pltpu.VMEM((2, n_dp, n_ctx, rows, ffq), BF),
            pltpu.VMEM((n_ctx, down_rows, width), BF),
            pltpu.VMEM((n_dp, t, width), BF),
            pltpu.VMEM((n_dp, t, width), BF),
            pltpu.VMEM((t, width), F32),
            pltpu.VMEM((n_dp, t, width), BF),
            pltpu.VMEM((n_dp, t, width), BF),
            pltpu.VMEM((2, n_dp, n_ctx, rows, ffq), BF),
            pltpu.VMEM((n_ctx, down_rows, width), BF),
            pltpu.VMEM((nblk - 1, PACK, t), BF),
            pltpu.VMEM((2, h, 2, n_dp, rows, ffq), BF),
            pltpu.VMEM((2, h, down_rows, width), BF),
            pltpu.VMEM((n_dp, 2, rows, ffq), BF),
            pltpu.VMEM((H * DH, t), F32),
            pltpu.VMEM((AQ + BQ, t), F32),
            pltpu.VMEM((t, width), F32),
            pltpu.VMEM((2, 3, t, width), BF),
            pltpu.VMEM((n_dp, n_ctx, rows, FPAD), BF),
            pltpu.VMEM((n_dp, n_ctx, rows, width), BF),
            pltpu.VMEM((2, n_ctx, rows, FPAD), BF),
            pltpu.VMEM((2, n_ctx, rows, width), BF),
            pltpu.VMEM((2, h, 2, rows, FPAD), BF),
            pltpu.VMEM((2, h, 2, rows, width), BF),
            pltpu.VMEM((3, rows, FPAD), BF),
            pltpu.VMEM((3, rows, width), BF),
            DMA((5,)),
            DMA((9,)),
            DMA((9,)),
            DMA((10, 2, h)),
            DMA((10, 2, h)),
            DMA((nblk - 1,)),
            DMA((nblk - 1,)),
            DMA((2, 3)),
            DMA((2, 3)),
            DMA((nblk - 1,)),
            DMA((nblk - 1,)),
            DMA((3,)),
            DMA((3,)),
            DMA((2, 3)),
            DMA((2, 3)),
            DMA((2, 3)),
            DMA((2, 3)),
            DMA((2,)),
            pltpu.VMEM((PACK, t), F32),
        ],
        compiler_params=talks(0),
        name="block",
    )(doc_lengths, x16, cosine, sine, pack, output_weights.astype(BF), gu_in,
      down_weights.astype(BF), cot_own)
    layer_output, input_grad, last_own, out_own, gu_own, down_sum = outs[:6]
    gu_own = gu_own.astype(F32).transpose(1, 2, 0, 3).reshape(2, rows, ff)
    return (
        layer_output.reshape(1, t, width),
        input_grad.reshape(1, t, width),
        last_own[:, FDIM],
        last_own[:, :FDIM],
        out_own,
        last_own[:, FDIM + 1],
        gu_own[0],
        gu_own[1],
        down_sum,
    )


def solution(mesh):
    return jax.shard_map(
        body,
        mesh=mesh,
        in_specs=(
            P("dp", "ctx", None),
            P("dp", None),
            P(("dp", "ctx")),
            P(("dp", "ctx"), None),
            P(("dp", "ctx"), None),
            P(("dp", "ctx")),
            P(("dp", "ctx"), None),
            P(("dp", "ctx"), None),
            P(("dp", "ctx"), None),
            P("dp", "ctx", None),
        ),
        out_specs=(
            P("dp", "ctx", None),
            P("dp", "ctx", None),
            P(("dp", "ctx")),
            P(("dp", "ctx"), None),
            P(("dp", "ctx"), None),
            P(("dp", "ctx")),
            P(("dp", "ctx"), None),
            P(("dp", "ctx"), None),
            P(("dp", "ctx"), None),
        ),
        check_vma=False,
    )
```

```python
import functools

import jax
import jax.numpy as jnp
import numpy as np
from jax import lax
from jax.experimental import pallas as pl
from jax.experimental.pallas import tpu as pltpu
from jax.sharding import PartitionSpec as P

H = 16
DH = 64
RQ = 6
RKV = 2
EPS = 1e-05
BF = jnp.bfloat16
F32 = jnp.float32
AQ = RQ * H
BQ = RQ * DH
AK = RKV * H
BK = RKV * DH
PACK = 2 * (AK + BK)
KEY_ROWS = AK + BK
FDIM = AQ + BQ + PACK
FPAD = 896
LOG2E = 1.4426950408889634
NEG = -1e30


def nt(a, b):
    return lax.dot_general(a, b, (((1,), (1,)), ((), ())), preferred_element_type=F32)


def nn(a, b):
    return jnp.dot(a, b, preferred_element_type=F32)

MESH = pl.DeviceIdType.MESH


def ring_place(c, n):
    z = c // 2
    return z + (c % 2) * (n - 1 - 2 * z)


def ring_index(p, n):
    p = (p + 2 * n) % n
    q = p // (n // 2)
    return (1 - q) * (2 * p) + q * (2 * (n - 1 - p) + 1)


def remote(src, dst, send, recv, dev):
    return pltpu.make_async_remote_copy(
        src_ref=src, dst_ref=dst, send_sem=send, recv_sem=recv, device_id=dev, device_id_type=MESH
    )


def places():
    d, c = lax.axis_index("dp"), lax.axis_index("ctx")
    core = d % 2
    return d, c, core, d + 1 - 2 * core, (d + 2) % 4


def greet(n):
    d, c, _, _, _ = places()
    barrier = pltpu.get_barrier_semaphore()
    n_dp = lax.axis_size("dp")
    for k in range(1, n_dp):
        pl.semaphore_signal(barrier, inc=1, device_id=((d + k) % n_dp, c), device_id_type=MESH)
    for k in range(1, n):
        pl.semaphore_signal(barrier, inc=1, device_id=(d, (c + k) % n), device_id_type=MESH)


def met(n):
    pl.semaphore_wait(pltpu.get_barrier_semaphore(), n + lax.axis_size("dp") - 2)


def steps(lo, hi, step):
    if isinstance(lo, int) and isinstance(hi, int) and hi - lo <= 4:
        for s in range(lo, hi):
            step(s)
    elif not (isinstance(lo, int) and isinstance(hi, int) and hi <= lo):
        lax.fori_loop(lo, hi, lambda s, _: (step(s), _)[1], 0)


class GatherRing:
    def __init__(self, n, slot, half, send, recv):
        self.n, self.h, self.slot, self.half, self.send, self.recv = n, n // 2, slot, half, send, recv
        self.d, c, _, _, _ = places()
        self.r = ring_place(c, n)

    def copy(self, s, i, arriving=False):
        way = 1 - 2 * i
        last = isinstance(s, int) and s == self.h - 1
        owner = ring_index(self.r - way * (s + (1 if arriving else 0)), self.n)
        ref = self.half(owner, i) if last else self.slot(owner)
        to = (self.d, ring_index(self.r + way, self.n))
        return remote(ref, ref, self.send.at[i, s], self.recv.at[i, s], to)

    def start(self, s):
        for i in range(2):
            self.copy(s, i).start()

    def arrive(self, s):
        for i in range(2):
            self.copy(s, i, True).wait_recv()

    def step(self, s):
        for i in range(2):
            self.copy(s - 1, i, True).wait_recv()
            self.copy(s, i).start()

    def last(self):
        self.step(self.h - 1)

    def drain(self):
        steps(0, self.h - 1, lambda s: [self.copy(s, i).wait_send() for i in range(2)])
        for i in range(2):
            self.copy(self.h - 1, i).wait_send()


class WideGather:
    def __init__(self, n, ref, half, send, recv, x_send, x_recv):
        self.d, self.c, _, _, self.xd = places()
        self.n, self.h, self.ref = n, n // 2, ref
        self.x_send, self.x_recv = x_send, x_recv
        self.ring = GatherRing(
            n, lambda o: ref.at[self.d, o], lambda o, w: half(ref.at[self.d, o], w), send, recv
        )

    def pass_on(self, i, owner, arriving=False):
        ref = self.ref.at[self.xd if arriving else self.d, owner]
        return remote(ref, ref, self.x_send.at[i], self.x_recv.at[i], (self.xd, self.c))

    def owner(self, s, i):
        return ring_index(self.ring.r - (1 - 2 * i) * (s + 1), self.n)

    def start(self, now):
        if now:
            self.pass_on(0, self.c).start()
        self.ring.start(0)

    def step(self, s, now):
        self.ring.step(s)
        if now:
            for i in range(2):
                self.pass_on(2 * s - 1 + i, self.owner(s - 1, i)).start()

    def finish(self, now):
        self.ring.arrive(self.h - 1)
        if now:
            self.pass_on(self.n - 1, self.owner(self.h - 1, 0)).start()
        else:
            self.passed(lambda i, o: self.pass_on(i, o).start())

    def passed(self, wait):
        wait(0, self.c)
        steps(0, self.h - 1, lambda s: [wait(1 + 2 * s + i, self.owner(s, i)) for i in range(2)])
        wait(self.n - 1, self.owner(self.h - 1, 0))

    def arrive(self):
        self.passed(lambda i, o: self.pass_on(i, o, True).wait_recv())

    def drain(self):
        self.ring.drain()
        self.passed(lambda i, o: self.pass_on(i, o).wait_send())


class ScatterRing:
    def __init__(self, n, part, half, land, whole_of, half_of, send, recv):
        self.n, self.h, self.part, self.half = n, n // 2, part, half
        self.land, self.whole_of, self.half_of = land, whole_of, half_of
        self.send, self.recv = send, recv
        self.d, c, _, _, _ = places()
        self.c, self.r = c, ring_place(c, n)

    def copy(self, s, i):
        way = 1 - 2 * i
        to = (self.d, ring_index(self.r + way, self.n))
        first = isinstance(s, int) and s == 0
        if first:
            owner = ring_index(self.r + way * self.h, self.n)
            src, dst = self.half(owner, i), self.half_of(self.land.at[i, 0], i)
        else:
            src, dst = self.land.at[i, s - 1], self.land.at[i, s]
        return remote(src, dst, self.send.at[i, s], self.recv.at[i, s], to)

    def start(self):
        for i in range(2):
            self.copy(0, i).start()

    def step(self, s):
        first = isinstance(s, int) and s == 1
        for i in range(2):
            way = 1 - 2 * i
            self.copy(s - 1, i).wait_recv()
            owner = ring_index(self.r + way * (self.h - s), self.n)
            held = self.land.at[i, s - 1]
            if first:
                mine = self.half_of(held, i)
                mine[...] = (mine[...].astype(F32) + self.half(owner, i)[...].astype(F32)).astype(BF)
                self.half_of(held, 1 - i)[...] = self.half(owner, 1 - i)[...]
            else:
                held[...] = (held[...].astype(F32) + self.part(owner)[...].astype(F32)).astype(BF)
            self.copy(s, i).start()

    def rest(self, lo, hi):
        if lo == 1 and hi > 1:
            self.step(1)
            lo = 2
        steps(lo, hi, self.step)

    def result(self):
        for i in range(2):
            self.copy(self.h - 1, i).wait_recv()
        out = self.part(self.c)[...].astype(F32)
        for i in range(2):
            out = out + self.land[i, self.h - 1].astype(F32)
        return out

    def drain(self):
        for i in range(2):
            self.copy(0, i).wait_send()
        steps(1, self.h, lambda s: [self.copy(s, i).wait_send() for i in range(2)])


class Spread:
    def __init__(self, ref, send, recv):
        d, c, _, cd, xd = places()
        self.copies = [
            remote(ref.at[d], ref.at[d], send.at[0], recv.at[0], (cd, c)),
            remote(ref.at[d], ref.at[d], send.at[1], recv.at[1], (xd, c)),
            remote(ref.at[xd], ref.at[xd], send.at[2], recv.at[2], (cd, c)),
        ]

    def start(self):
        self.copies[1].start()
        self.copies[0].start()

    def forward(self):
        self.copies[1].wait_recv()
        self.copies[2].start()

    def finish(self):
        self.copies[0].wait_recv()
        self.copies[2].wait_recv()
        for copy in self.copies:
            copy.wait_send()


def blocks(count, step, state):
    if count <= 8:
        for j in range(count):
            state = step(j, state)
        return state
    return lax.fori_loop(0, count, step, state)


def lane_block(j, size):
    if isinstance(j, int):
        return pl.ds(j * size, size)
    return pl.ds(pl.multiple_of(j * size, size), size)


def rope(b, cosine, sine, ranks):
    parts = []
    half = DH // 2
    for r in range(ranks):
        u1 = b[r * DH : r * DH + half]
        u2 = b[r * DH + half : (r + 1) * DH]
        parts += [u1 * cosine - u2 * sine, u2 * cosine + u1 * sine]
    return jnp.concatenate(parts, axis=0)


def rope_back(v, cosine, sine, ranks):
    return rope(v, cosine, -sine, ranks)


def pre_part(x, g1, w, cosine, sine, nt_ref, q_ref, p_ref, a_ref, b_ref):
    r1 = lax.rsqrt(jnp.mean(x * x, axis=-1, keepdims=True) + EPS)
    n = (x * r1 * g1).astype(BF)
    nt_ref[...] = n.T
    ft = nn(n, w).T
    a = ft[:AQ]
    b = rope(ft[AQ : AQ + BQ], cosine, sine, RQ)
    for i in range(AQ):
        a_ref[i] = a[i : i + 1]
    b_ref[...] = b
    k0 = AQ + BQ
    bk = rope(ft[k0 + AK : k0 + AK + BK], cosine, sine, RKV)
    p_ref[...] = jnp.concatenate(
        [ft[k0 : k0 + AK], bk, ft[k0 + KEY_ROWS : k0 + PACK]], axis=0
    ).astype(BF)
    for h in range(H):
        acc = a[h : h + 1] * b[:DH]
        for r in range(1, RQ):
            acc = acc + a[r * H + h : r * H + h + 1] * b[r * DH : (r + 1) * DH]
        q_ref[h * DH : (h + 1) * DH, :] = (acc * (1.0 / RQ)).astype(BF)


def vectors(kv_ref, side, r, lanes):
    first = side * KEY_ROWS + AK + r * DH
    return kv_ref[first : first + DH, lanes].astype(F32)


def expand_pair(ka, kv_ref, side, p, lanes):
    rows = []
    for hh in range(2):
        acc = 0.0
        for r in range(RKV):
            a = ka[side * AK + r * H + 2 * p + hh, :, lanes]
            b = vectors(kv_ref, side, r, lanes)
            acc = acc + a * b
        rows.append(acc * (1.0 / RKV))
    return jnp.concatenate(rows, axis=0)


def unpack(kv_ref, ka):
    for side in range(2):
        first = side * KEY_ROWS
        a = kv_ref[first : first + AK, :].astype(F32)
        for i in range(AK):
            ka[side * AK + i] = a[i : i + 1]


def diagonal(pair):
    zero = jnp.zeros((DH, pair.shape[1]), pair.dtype)
    left = jnp.concatenate([pair[:DH], zero], axis=0)
    right = jnp.concatenate([zero, pair[DH:]], axis=0)
    return jnp.concatenate([left, right], axis=1)


def undiagonal(wide):
    t = wide.shape[1] // 2
    return jnp.concatenate([wide[:DH, :t], wide[DH:, t:]], axis=0)


def attend_part(nblk, len_ref, q_ref, kv_ref, at_ref, af_ref, inv_ref, p_out, pbuf, ka, bias):
    t = q_ref.shape[1]
    c = lax.axis_index("ctx")
    tpos = c * t + lax.broadcasted_iota(jnp.int32, (1, t), 1)
    start = jnp.zeros((1, t), jnp.int32)
    run = jnp.int32(0)
    for j in range(len_ref.shape[1]):
        start = jnp.where(tpos >= run, run, start)
        run = run + len_ref[0, j]
    unpack(kv_ref, ka)

    def bias_block(j, _):
        spos = (c - nblk + 1 + j) * t + lax.broadcasted_iota(jnp.int32, (t, t), 0)
        ok = (spos >= start) & (spos <= tpos)
        bias[lane_block(j, t), :] = jnp.where(ok, 0.0, NEG)
        return _

    blocks(nblk, bias_block, 0)

    def pair(p, carry):
        @pl.when(p > 1)
        def _():
            p_out(p - 2).wait()

        rows = pl.ds(pl.multiple_of(p * 2 * DH, 2 * DH), 2 * DH)
        qd = diagonal(q_ref[rows, :])

        def step(j, state):
            num, tot = state
            lanes = lane_block(j, t)
            k = expand_pair(ka, kv_ref, 0, p, lanes).T.astype(BF)
            v = expand_pair(ka, kv_ref, 1, p, lanes).astype(BF)
            b = bias[lanes, :]
            s = nn(k, qd) * (LOG2E * DH**-0.5) + jnp.concatenate([b, b], axis=1)
            e = jnp.exp2(s)
            tot = tot + jnp.sum(e, axis=0, keepdims=True)
            pb = e.astype(BF)
            pbuf[p % 2, lanes, :] = pb
            return (num + nn(v, pb), tot)

        num, tot = blocks(
            nblk, step, (jnp.zeros((2 * DH, 2 * t), F32), jnp.zeros((1, 2 * t), F32))
        )
        inv = 1.0 / tot
        af = undiagonal(num * inv)
        af_ref[rows, :] = af
        at_ref[rows, :] = af.astype(BF)
        p_out(p).start()
        inv_ref[p] = jnp.broadcast_to(inv, (8, 2 * t))
        return carry

    lax.fori_loop(0, H // 2, pair, 0)
    for p in range(H // 2 - 2, H // 2):
        p_out(p).wait()


def attend_back_part(
    nblk, serve, da_ref, af_ref, inv_ref, p_copy, pbuf, q_ref, kv_ref, a_ref, b_ref, cos_ref, sin_ref,
    dq_ref, dkv_ref, ka, dka, dqa, db,
):
    t = q_ref.shape[1]
    unpack(kv_ref, ka)
    db[...] = jnp.zeros_like(db)
    for side in range(2):
        first = side * KEY_ROWS + AK
        dkv_ref[first : first + BK, :] = jnp.zeros((BK, nblk * t), F32)

    def factor_back(dwide, side, p, lanes):
        for hh in range(2):
            d = dwide[hh * DH : (hh + 1) * DH] * (1.0 / RKV)
            for r in range(RKV):
                row = side * AK + r * H + 2 * p + hh
                first = side * KEY_ROWS + AK + r * DH
                b = vectors(kv_ref, side, r, lanes)
                dka[row, :, lanes] = jnp.sum(d * b, axis=0, keepdims=True)
                dkv_ref[first : first + DH, lanes] += d * ka[row, :, lanes]

    def pair(p, carry):
        @pl.when(p + 1 < H // 2)
        def _():
            p_copy(p + 1).start()

        p_copy(p).wait()
        rows = pl.ds(pl.multiple_of(p * 2 * DH, 2 * DH), 2 * DH)
        da = da_ref[rows, :]
        inv = inv_ref[p][:1]
        dd = diagonal(da)
        dn = (dd * inv).astype(BF)
        dtot = -jnp.sum(dd * diagonal(af_ref[rows, :]), axis=0, keepdims=True) * inv
        qd = diagonal(q_ref[rows, :])

        def step(j, dq):
            lanes = lane_block(j, t)
            k = expand_pair(ka, kv_ref, 0, p, lanes).astype(BF)
            v = expand_pair(ka, kv_ref, 1, p, lanes).T.astype(BF)
            pb = pbuf[p % 2, lanes, :]
            ds = (pb.astype(F32) * (nn(v, dn) + dtot)).astype(BF)
            dq = dq + nn(k, ds)
            factor_back(nt(qd, ds) * (DH**-0.5), 0, p, lanes)
            factor_back(nt(dn, pb), 1, p, lanes)
            return dq

        dq = undiagonal(blocks(nblk, step, jnp.zeros((2 * DH, 2 * t), F32)))
        dq = dq * (DH**-0.5 / RQ)
        for hh in range(2):
            d = dq[hh * DH : (hh + 1) * DH]
            for r in range(RQ):
                row = r * H + 2 * p + hh
                dqa[row] = jnp.sum(d * b_ref[r * DH : (r + 1) * DH, :], axis=0, keepdims=True)
                db[r * DH : (r + 1) * DH, :] += d * a_ref[row]
        serve(p)
        return carry

    lax.fori_loop(0, H // 2, pair, 0)
    for i in range(AQ):
        dq_ref[i : i + 1, :] = dqa[i]
    for side in range(2):
        for i in range(AK):
            dkv_ref[side * KEY_ROWS + i : side * KEY_ROWS + i + 1, :] = dka[side * AK + i]
    dq_ref[AQ : AQ + BQ, :] = rope_back(db[...], cos_ref[...], sin_ref[...], RQ)


def gain_rows(w):
    first = FPAD - 128
    gains = w[:, first:].astype(F32).T
    return gains[FDIM - first : FDIM - first + 1], gains[FDIM - first + 1 : FDIM - first + 2]


def lane_half(ref, w):
    return ref.at[:, :512] if w == 0 else ref.at[:, 512:]


class PairScatter:
    def __init__(self, n, part, held, land, own, send, recv, ring_send, ring_recv, x_first=None):
        d, c, core, cd, xd = places()
        self.x_first = x_first
        self.core, self.x, self.part, self.held, self.own = core, d // 2, part, held, own
        self.swaps = [
            remote(part.at[2 * xx + 1 - core], held.at[xx], send.at[xx], recv.at[xx], (cd, c))
            for xx in range(2)
        ]
        if x_first is not None:
            self.end = remote(held.at[1 - self.x], x_first, send.at[2], recv.at[2], (xd, c))
            self.ring = ScatterRing(
                n, lambda o: x_first.at[o], lambda o, w: lane_half(x_first.at[o], w), land,
                None, lane_half, ring_send, ring_recv,
            )
            return
        self.end = remote(own.at[1 - self.x], own.at[2], send.at[2], recv.at[2], (xd, c))
        self.ring = ScatterRing(
            n, lambda o: held.at[:, o], lambda o, w: held.at[w, o], land,
            None, lambda ref, w: ref.at[w], ring_send, ring_recv,
        )

    def start(self):
        for swap in self.swaps:
            swap.start()

    def enter(self):
        for xx in range(2):
            self.swaps[xx].wait_recv()
            mine = self.part[2 * xx + self.core].astype(F32)
            self.held[xx] = (self.held[xx].astype(F32) + mine).astype(BF)
        if self.x_first is None:
            self.ring.start()
        else:
            self.end.start()

    def across(self):
        self.end.wait_recv()
        total = self.x_first[...].astype(F32) + self.held[self.x].astype(F32)
        self.x_first[...] = total.astype(BF)
        self.ring.start()

    def leave(self):
        total = self.ring.result()
        for xx in range(2):
            self.own[xx] = total[xx].astype(BF)
        self.end.start()

    def result(self):
        self.end.wait_recv()
        return self.own[self.x].astype(F32) + self.own[2].astype(F32)

    def drain(self):
        for copy in self.swaps + [self.end]:
            copy.wait_send()
        self.ring.drain()


def block_kernel(
    n, nblk,
    len_ref, x_ref, cos_ref, sin_ref, fw_ref, g1_ref, g2_ref, ow_ref, gw_ref, uw_ref, dw_ref, cot_in,
    y_ref, dx_ref, fac_ref, gain1_ref, gain2_ref, wo_ref, gate_ref, up_ref, wd_ref, p_ref,
    nt_ref, q_ref, a_ref, b_ref, kv_ref, at_ref, af_ref, inv_ref, pbuf,
    fac, wo, gu, wd, nm, cot, mid_ref, dn_in, out_in, gu_part, wd_part,
    kv_land, gu_land, wd_land, gu_own, da_ref, dq_ref, dmid_ref, dp_land,
    fac_part, wo_part, fac_held, wo_held, fac_land, wo_land, fac_own, wo_own,
    own_sem, near_send, near_recv, ring_send, ring_recv, kv_send, kv_recv, sp_send, sp_recv,
    dkv_send, dkv_recv, end_send, end_recv, dp_send, dp_recv, pair_send, pair_recv, p_sem, own_dkv,
    gu_in, gu_ref, x_send, x_recv,
):
    d, c, core, cd, xd = places()
    t = x_ref.shape[0]
    n_dp = 4
    rows, ffq = gu_in.shape[1], gu_in.shape[2] // 2
    greet(n)
    keep_cot = pltpu.make_async_copy(cot_in, cot.at[d], own_sem.at[4])
    keep_cot.start()
    tail = FPAD - 128
    lane = lax.broadcasted_iota(jnp.int32, (rows, 128), 1)
    diag = lax.broadcasted_iota(jnp.int32, (rows, rows), 0) == lax.broadcasted_iota(
        jnp.int32, (rows, rows), 1
    )

    def column(ref):
        return jnp.sum(jnp.where(diag, ref[...], 0.0), axis=1, keepdims=True)

    gains = jnp.where(lane == FDIM - tail, column(g1_ref), 0.0)
    gains = jnp.where(lane == FDIM + 1 - tail, column(g2_ref), gains)
    fac[d, c, :, :tail] = fw_ref[:, :tail].astype(BF)
    fac[d, c, :, tail:] = gains.astype(BF)
    fac[d, c, :, tail:FDIM] = fw_ref[:, tail:].astype(BF)
    wo[d, c] = ow_ref[...].astype(BF)
    wd[c] = dw_ref[...].astype(BF)
    for dd in range(n_dp):
        for side, ref in enumerate((gw_ref, uw_ref)):
            gu_in[dd, :, side * ffq : (side + 1) * ffq] = ref[:, dd * ffq : (dd + 1) * ffq].astype(BF)
    keep_gu = pltpu.make_async_copy(gu_in.at[d], gu.at[d, c], own_sem.at[2])
    keep_gu.start()
    for k in range(1, nblk):
        @pl.when(c - k < 0)
        def _():
            kv_ref[:, (nblk - 1 - k) * t : (nblk - k) * t] = jnp.zeros((PACK, t), BF)
    met(n)

    fo = WideGather(n, fac, lane_half, ring_send.at[0], ring_recv.at[0], x_send.at[0], x_recv.at[0])
    oo = WideGather(n, wo, lane_half, ring_send.at[1], ring_recv.at[1], x_send.at[1], x_recv.at[1])
    cut = -(-dw_ref.shape[0] // 16) * 8
    gr = GatherRing(
        n, lambda o: gu.at[:, o], lambda o, w: gu.at[2 * w : 2 * w + 2, o],
        ring_send.at[4], ring_recv.at[4],
    )
    dr = GatherRing(
        n, lambda o: wd.at[o], lambda o, w: wd.at[o, :cut] if w == 0 else wd.at[o, cut:],
        ring_send.at[5], ring_recv.at[5],
    )
    small, large = (fo, oo), (gr, dr)
    fo.start(True)
    oo.start(False)
    a2a = []
    for k in range(1, n_dp):
        to = (d + k) % n_dp
        a2a.append(
            (
                remote(gu_in.at[to], gu.at[d, c], near_send.at[1 + k], near_recv.at[1 + k], (to, c)),
                remote(
                    gu_in.at[to], gu.at[(d + n_dp - k) % n_dp, c],
                    near_send.at[1 + k], near_recv.at[1 + k], (to, c),
                ),
            )
        )
        a2a[-1][0].start()
    cots = Spread(cot, sp_send.at[0], sp_recv.at[0])
    nms = Spread(nm, sp_send.at[1], sp_recv.at[1])
    steps(1, n // 2 - 1, lambda s: (fo.step(s, True), oo.step(s, False)))
    fo.step(n // 2 - 1, True)
    oo.step(n // 2 - 1, False)
    keep_gu.wait()
    for _, arrival in a2a:
        arrival.wait_recv()
    gr.start(0)

    def core_swap(ref, i, dd, da):
        return (
            remote(ref.at[dd], ref.at[dd], near_send.at[5 + i], near_recv.at[5 + i], (cd, c)),
            remote(ref.at[da], ref.at[da], near_send.at[5 + i], near_recv.at[5 + i], (cd, c)),
        )

    near = []

    def swap(i, ref, dd, da):
        near.append(core_swap(ref, i, dd, da))
        near[-1][0].start()

    fo.finish(True)
    swap(0, fac, d, cd)
    oo.finish(False)
    swap(2, wo, d, cd)
    fo.arrive()
    swap(1, fac, xd, (cd + 2) % 4)
    keep_cot.wait()
    cots.start()
    for _, arrival in (near[0], near[2]):
        arrival.wait_recv()

    width = x_ref.shape[1]
    x = x_ref[...].astype(F32)
    w = fac[...].reshape(width, FPAD)
    g1, g2 = gain_rows(w)
    own_kv = kv_ref.at[:, (nblk - 1) * t : nblk * t]
    pre_part(x, g1, w, cos_ref[...], sin_ref[...], nt_ref, q_ref, own_kv, a_ref, b_ref)

    def kv_copy(k):
        dst = kv_ref.at[:, (nblk - 1 - k) * t : (nblk - k) * t]
        return remote(own_kv, dst, kv_send.at[k - 1], kv_recv.at[k - 1], (d, (c + k) % n))

    for k in range(1, nblk):
        @pl.when(c + k < n)
        def _():
            kv_copy(k).start()
    dr.start(0)
    oo.arrive()
    swap(3, wo, xd, (cd + 2) % 4)
    for k in range(1, nblk):
        @pl.when(c - k >= 0)
        def _():
            kv_copy(k).wait_recv()
    full = n // 2 - 1
    middle_step = 1 + full // 2
    steps(1, middle_step, lambda s: [one.step(s) for one in large])

    def p_out(p):
        return pltpu.make_async_copy(pbuf.at[p % 2], p_ref.at[p], p_sem.at[p % 2])

    pl.run_scoped(
        functools.partial(
            attend_part, nblk, len_ref, q_ref, kv_ref, at_ref, af_ref, inv_ref, p_out, pbuf
        ),
        pltpu.VMEM((2 * AK, 1, nblk * t), F32),
        pltpu.VMEM((nblk * t, t), F32),
    )

    for _, arrival in (near[1], near[3]):
        arrival.wait_recv()
    middle = x + nn(at_ref[...].T, wo[...].reshape(width, width))
    mid_ref[...] = middle
    r2 = lax.rsqrt(jnp.mean(middle * middle, axis=-1, keepdims=True) + EPS)
    nm[d] = (middle * r2 * g2).astype(BF)
    nms.start()
    cots.forward()
    steps(middle_step, full, lambda s: [one.step(s) for one in large])
    nms.forward()
    nms.finish()
    cots.finish()
    for one in large:
        one.last()
    for one in large:
        one.arrive(n // 2 - 1)

    x_at = d // 2
    parts = (dn_in, out_in)
    first = []
    for i, part in enumerate(parts):
        for j, xx in enumerate((1 - x_at, x_at)):
            first.append(
                remote(
                    part.at[2 * xx + 1 - core], dp_land.at[i, j],
                    dp_send.at[i, j], dp_recv.at[i, j], (cd, c),
                )
            )

    def feed(both_ff, dh, hid, dgu):
        down = wd[...].reshape(ffq, width)

        def matrix():
            return gu[...].reshape(width, 2 * ffq)

        def pair_rows(i, carry):
            xx = i * x_at + (1 - i) * (1 - x_at)
            two = pl.ds(2 * xx, 2)
            both = 2 * t
            both_ff[...] = nn(nm[two].reshape(both, width), matrix())
            dh[...] = nt(cot[two].reshape(both, width), down)
            base = pl.multiple_of(xx * both, both)

            def rows_of(k, carry):
                some = pl.ds(pl.multiple_of(k * 32, 32), 32)
                to = pl.ds(pl.multiple_of(base + k * 32, 32), 32)
                v, u, g = both_ff[some, :ffq], both_ff[some, ffq:], dh[some, :]
                sig, act = silu_parts(v)
                hid[to, :] = (act * u).astype(BF)
                dgu[to, :ffq] = (g * u * sig * (1.0 + v * (1.0 - sig))).astype(BF)
                dgu[to, ffq:] = (g * act).astype(BF)
                return carry

            lax.fori_loop(0, both // 32, rows_of, 0)
            all_rows = pl.ds(base, both)
            dn_in[two] = nt(dgu[all_rows, :], matrix()).astype(BF).reshape(2, t, width)
            out_in[two] = nn(hid[all_rows, :], down).astype(BF).reshape(2, t, width)

            @pl.when(i == 0)
            def _():
                first[0].start()
                first[2].start()

            return carry

        lax.fori_loop(0, 2, pair_rows, 0)
        first[1].start()
        first[3].start()
        for i, part in enumerate(parts):
            first[2 * i].wait_recv()
            dp_land[i, 0] = (dp_land[i, 0].astype(F32) + part[xd].astype(F32)).astype(BF)
            dp_next(i).start()

        def tn(a, b):
            return lax.dot_general(a, b, (((0,), (0,)), ((), ())), preferred_element_type=F32)

        quarter = width // n_dp

        def columns(j, carry):
            lanes = pl.ds(pl.multiple_of(j * quarter, quarter), quarter)
            some = nm[:, :, lanes].reshape(n_dp * t, quarter)
            gu_part[j] = tn(some, dgu[...]).astype(BF).reshape(gu_part.shape[1:])
            c_some = cot[:, :, lanes].reshape(n_dp * t, quarter)
            wd_part[:, :, lanes] = tn(hid[...], c_some).astype(BF).reshape(wd_part.shape[:2] + (quarter,))
            return carry

        lax.fori_loop(0, n_dp, columns, 0)

    def dp_next(i):
        return remote(dp_land.at[i, 0], dp_land.at[i, 2], dp_send.at[i, 2], dp_recv.at[i, 2], (xd, c))

    pl.run_scoped(
        feed,
        pltpu.VMEM((2 * t, 2 * ffq), F32),
        pltpu.VMEM((2 * t, ffq), F32),
        pltpu.VMEM((n_dp * t, ffq), BF),
        pltpu.VMEM((n_dp * t, 2 * ffq), BF),
    )
    second = [dp_next(i) for i in range(2)]
    cut = -(-wd_part.shape[1] // 16) * 8

    def wd_half(ref, w):
        return ref.at[:cut] if w == 0 else ref.at[cut:]

    gs = ScatterRing(
        n, lambda o: gu_part.at[:, o], lambda o, w: gu_part.at[2 * w : 2 * w + 2, o], gu_land,
        None, lambda ref, w: ref.at[2 * w : 2 * w + 2], ring_send.at[6], ring_recv.at[6],
    )
    ds_ = ScatterRing(
        n, lambda o: wd_part.at[o], lambda o, w: wd_half(wd_part.at[o], w), wd_land,
        None, wd_half, ring_send.at[7], ring_recv.at[7],
    )
    scatter = (gs, ds_)
    for one in scatter:
        one.start()
    fs = PairScatter(
        n, fac_part, fac_held, fac_land, fac_own, pair_send.at[0], pair_recv.at[0],
        ring_send.at[8], ring_recv.at[8],
    )
    ws = PairScatter(
        n, wo_part, wo_held, wo_land, wo_own, pair_send.at[1], pair_recv.at[1],
        ring_send.at[9], ring_recv.at[9], wo_own,
    )
    h = n // 2

    def advance(s):
        for one in scatter:
            one.step(s)

    advance(1)
    for i in range(2):
        first[2 * i + 1].wait_recv()
    second[0].wait_recv()
    middle = mid_ref[...]
    dn = dn_in[d].astype(F32) + dp_land[0, 1].astype(F32) + dp_land[0, 2].astype(F32)
    second_part = jnp.sum(dn * middle * r2, axis=0, keepdims=True)
    u2 = dn * g2
    d_middle = (
        cot_in[...].astype(F32)
        + r2 * u2
        - middle * (r2 * r2 * r2 * jnp.mean(u2 * middle, axis=-1, keepdims=True))
    )
    dmid_ref[...] = d_middle
    d_branch = d_middle.astype(BF)
    wo_part[...] = nn(at_ref[...], d_branch).astype(BF).reshape(wo_part.shape)
    ws.start()
    da_ref[...] = nt(wo[...].reshape(width, width), d_branch)
    second[1].wait_recv()
    y_ref[...] = (
        mid_ref[...]
        + (out_in[d].astype(F32) + dp_land[1, 1].astype(F32) + dp_land[1, 2].astype(F32))
    ).astype(BF)
    ws.enter()
    points = 3

    def serve(k):
        steps(2 + -(-(k - 1) * (h - 2) // points), 2 + -(-k * (h - 2) // points), advance)

    serve(1)

    def serve_pair(p):
        @pl.when(p == H // 2 - 3)
        def _():
            serve(2)
            ws.across()

    def p_copy(p):
        return pltpu.make_async_copy(p_ref.at[p], pbuf.at[p % 2], p_sem.at[p % 2])

    p_copy(0).start()

    def attention_back(ka, dka, dqa, db, dkv, dkv16):
        attend_back_part(
            nblk, serve_pair, da_ref, af_ref, inv_ref, p_copy, pbuf, q_ref, kv_ref, a_ref, b_ref,
            cos_ref, sin_ref, dq_ref, dkv, ka, dka, dqa, db,
        )
        dkv16[...] = dkv[...].astype(BF)

        def dkv_copy(k):
            src = dkv16.at[:, (nblk - 1 - k) * t : (nblk - k) * t]
            return remote(
                src, kv_land.at[k - 1], dkv_send.at[k - 1], dkv_recv.at[k - 1], (d, (c + n - k) % n)
            )

        for k in range(1, nblk):
            @pl.when(c - k >= 0)
            def _():
                dkv_copy(k).start()
        serve(3)
        own_dkv[...] = dkv[:, (nblk - 1) * t :]
        for k in range(1, nblk):
            @pl.when(c + k < n)
            def _():
                dkv_copy(k).wait_recv()
                own_dkv[...] += kv_land[k - 1].astype(F32)
        for k in range(1, nblk):
            @pl.when(c - k >= 0)
            def _():
                dkv_copy(k).wait_send()

    pl.run_scoped(
        attention_back,
        pltpu.VMEM((2 * AK, 1, nblk * t), F32),
        pltpu.VMEM((2 * AK, 1, nblk * t), F32),
        pltpu.VMEM((AQ, 1, t), F32),
        pltpu.VMEM((BQ, t), F32),
        pltpu.VMEM((PACK, nblk * t), F32),
        pltpu.VMEM((PACK, nblk * t), BF),
    )
    ws.ring.step(1)
    steps(2, h - 1, ws.ring.step)
    dp = own_dkv[...]
    d_bk = rope_back(dp[AK : AK + BK], cos_ref[...], sin_ref[...], RKV)
    d_fac_t = jnp.concatenate(
        [dq_ref[...], dp[:AK], d_bk, dp[KEY_ROWS:], jnp.zeros((FPAD - FDIM, t), F32)], axis=0
    ).astype(BF)
    x = x_ref[...].astype(F32)
    r1 = lax.rsqrt(jnp.mean(x * x, axis=-1, keepdims=True) + EPS)
    d_norm_in = nt(d_fac_t.T, w)
    first_part = jnp.sum(d_norm_in * x * r1, axis=0, keepdims=True)
    tail = FPAD - 128
    gains = jnp.concatenate(
        [jnp.zeros((FDIM - tail, width), F32), first_part, second_part,
         jnp.zeros((FPAD - FDIM - 2, width), F32)], axis=0).T
    product = nt(nt_ref[...], d_fac_t)
    shape = fac_part.shape[:3]
    fac_part[:, :, :, :tail] = product[:, :tail].astype(BF).reshape(shape + (tail,))
    fac_part[:, :, :, tail:] = (product[:, tail:] + gains).astype(BF).reshape(shape + (128,))
    fs.start()
    u1 = d_norm_in * g1
    dx_ref[...] = (
        dmid_ref[...] + r1 * u1 - x * (r1 * r1 * r1 * jnp.mean(u1 * x, axis=-1, keepdims=True))
    ).astype(BF)
    fs.enter()
    gu_own[...] = gs.result().astype(BF)
    keep = pltpu.make_async_copy(gu_own.at[d], gu_ref.at[d], own_sem.at[0])
    keep.start()
    last = []
    for k in range(1, n_dp):
        to = (d + k) % n_dp
        last.append(
            (
                remote(gu_own.at[to], gu_ref.at[d], end_send.at[k - 1], end_recv.at[k - 1], (to, c)),
                remote(
                    gu_own.at[to], gu_ref.at[(d + n_dp - k) % n_dp],
                    end_send.at[k - 1], end_recv.at[k - 1], (to, c),
                ),
            )
        )
        last[-1][0].start()
    ws.ring.step(h - 1)
    fs.ring.step(1)
    wd_ref[...] = ds_.result()
    steps(2, h, fs.ring.step)
    wo_ref[...] = ws.ring.result()
    fs.leave()
    for out, arrival in last:
        arrival.wait_recv()
        out.wait_send()
    keep.wait()
    for dd in range(n_dp):
        lanes = slice(dd * ffq, (dd + 1) * ffq)
        gate_ref[:, lanes] = gu_ref[dd, :, :ffq].astype(F32)
        up_ref[:, lanes] = gu_ref[dd, :, ffq:].astype(F32)
    total = fs.result()
    fac_ref[...] = total[:, :FDIM]
    for i, ref in enumerate((gain1_ref, gain2_ref)):
        one = total[:, FDIM + i : FDIM + i + 1]
        ref[...] = jnp.sum(jnp.where(diag, one, 0.0), axis=0, keepdims=True)
    for copy in first + second:
        copy.wait_send()
    for one in scatter + (ws, fs):
        one.drain()
    for k in range(1, nblk):
        @pl.when(c + k < n)
        def _():
            kv_copy(k).wait_send()
    for out, _ in a2a + near:
        out.wait_send()
    for one in small + large:
        one.drain()


def emit_kernel(*refs):
    k = (len(refs) - 2) // 3
    ins, outs, bufs, sems = refs[:k], refs[k : 2 * k], refs[2 * k : 3 * k], refs[3 * k :]
    into = [pltpu.make_async_copy(a, b, sems[0].at[i]) for i, (a, b) in enumerate(zip(ins, bufs))]
    out = [pltpu.make_async_copy(a, b, sems[1].at[i]) for i, (a, b) in enumerate(zip(bufs, outs))]
    for copy in into:
        copy.start()
    for one, two in zip(into, out):
        one.wait()
        two.start()
    for copy in out:
        copy.wait()


def vmem(n):
    return [pl.BlockSpec(memory_space=pltpu.VMEM)] * n


def hbm(n):
    return [pl.BlockSpec(memory_space=pl.ANY)] * n


SMEM = pl.BlockSpec(memory_space=pltpu.SMEM)
DMA = pltpu.SemaphoreType.DMA


def talks(i):
    return pltpu.CompilerParams(
        collective_id=i, has_side_effects=True, vmem_limit_bytes=63 * 1024 * 1024
    )


def silu_parts(gate):
    s = jax.nn.sigmoid(gate)
    return s, gate * s


def body(
    tokens,
    doc_lengths,
    first_gain,
    factor_weights,
    output_weights,
    second_gain,
    gate_weights,
    up_weights,
    down_weights,
    cotangent,
):
    _, t, width = tokens.shape
    n_ctx, n_dp = lax.axis_size("ctx"), lax.axis_size("dp")
    n_all = n_ctx * n_dp
    both = ("dp", "ctx")
    length = t * n_ctx
    nblk = min(n_ctx, -(-(length // 2 - 1) // t) + 1)
    ff = gate_weights.shape[1]
    ffq = ff // n_dp
    rows = width // n_all
    c = lax.axis_index("ctx")

    h = n_ctx // 2

    half = DH // 2
    freq = 10000.0 ** (-(np.arange(half) * 2.0 / DH))
    pos = (c * t + jnp.arange(t, dtype=jnp.int32)).astype(F32)
    angles = jnp.asarray(freq, F32)[:, None] * pos[None, :]
    cosine, sine = jnp.cos(angles), jnp.sin(angles)

    x16 = tokens.reshape(t, width)
    cot_own = cotangent.reshape(t, width)
    sds = jax.ShapeDtypeStruct
    down_rows = down_weights.shape[0]
    outs = pl.pallas_call(
        functools.partial(block_kernel, n_ctx, nblk),
        out_shape=(
            sds((t, width), BF),
            sds((t, width), BF),
            sds((rows, FDIM), F32),
            sds((1, rows), F32),
            sds((1, rows), F32),
            sds((rows, width), F32),
            sds((rows, ff), F32),
            sds((rows, ff), F32),
            sds((down_rows, width), F32),
            sds((H // 2, nblk * t, 2 * t), BF),
        ),
        in_specs=[SMEM] + vmem(11),
        out_specs=tuple(vmem(9) + hbm(1)),
        scratch_shapes=[
            pltpu.VMEM((width, t), BF),
            pltpu.VMEM((H * DH, t), BF),
            pltpu.VMEM((AQ, 1, t), F32),
            pltpu.VMEM((BQ, t), F32),
            pltpu.VMEM((PACK, nblk * t), BF),
            pltpu.VMEM((H * DH, t), BF),
            pltpu.VMEM((H * DH, t), F32),
            pltpu.VMEM((H // 2, 8, 2 * t), F32),
            pltpu.VMEM((2, nblk * t, 2 * t), BF),
            pltpu.VMEM((n_dp, n_ctx, rows, FPAD), BF),
            pltpu.VMEM((n_dp, n_ctx, rows, width), BF),
            pltpu.VMEM((n_dp, n_ctx, rows, 2 * ffq), BF),
            pltpu.VMEM((n_ctx, down_rows, width), BF),
            pltpu.VMEM((n_dp, t, width), BF),
            pltpu.VMEM((n_dp, t, width), BF),
            pltpu.VMEM((t, width), F32),
            pltpu.VMEM((n_dp, t, width), BF),
            pltpu.VMEM((n_dp, t, width), BF),
            pltpu.VMEM((n_dp, n_ctx, rows, 2 * ffq), BF),
            pltpu.VMEM((n_ctx, down_rows, width), BF),
            pltpu.VMEM((nblk - 1, PACK, t), BF),
            pltpu.VMEM((2, h, n_dp, rows, 2 * ffq), BF),
            pltpu.VMEM((2, h, down_rows, width), BF),
            pltpu.VMEM((n_dp, rows, 2 * ffq), BF),
            pltpu.VMEM((H * DH, t), F32),
            pltpu.VMEM((AQ + BQ, t), F32),
            pltpu.VMEM((t, width), F32),
            pltpu.VMEM((2, 3, t, width), BF),
            pltpu.VMEM((n_dp, n_ctx, rows, FPAD), BF),
            pltpu.VMEM((n_dp, n_ctx, rows, width), BF),
            pltpu.VMEM((2, n_ctx, rows, FPAD), BF),
            pltpu.VMEM((2, n_ctx, rows, width), BF),
            pltpu.VMEM((2, h, 2, rows, FPAD), BF),
            pltpu.VMEM((2, h, rows, width), BF),
            pltpu.VMEM((3, rows, FPAD), BF),
            pltpu.VMEM((n_ctx, rows, width), BF),
            DMA((5,)),
            DMA((9,)),
            DMA((9,)),
            DMA((10, 2, h)),
            DMA((10, 2, h)),
            DMA((nblk - 1,)),
            DMA((nblk - 1,)),
            DMA((2, 3)),
            DMA((2, 3)),
            DMA((nblk - 1,)),
            DMA((nblk - 1,)),
            DMA((3,)),
            DMA((3,)),
            DMA((2, 3)),
            DMA((2, 3)),
            DMA((2, 3)),
            DMA((2, 3)),
            DMA((2,)),
            pltpu.VMEM((PACK, t), F32),
            pltpu.VMEM((n_dp, rows, 2 * ffq), BF),
            pltpu.VMEM((n_dp, rows, 2 * ffq), BF),
            DMA((2, n_ctx)),
            DMA((2, n_ctx)),
        ],
        compiler_params=talks(0),
        name="block",
    )(doc_lengths, x16, cosine, sine, factor_weights, first_gain.reshape(1, rows),
      second_gain.reshape(1, rows), output_weights, gate_weights, up_weights, down_weights, cot_own)
    outs = outs[:9]
    y, dx, fac_own, gain1, gain2, out_own, gate_own, up_own, down_own = pl.pallas_call(
        emit_kernel,
        out_shape=tuple(sds(o.shape, o.dtype) for o in outs),
        in_specs=hbm(9),
        out_specs=tuple(hbm(9)),
        scratch_shapes=[pltpu.VMEM(o.shape, o.dtype) for o in outs] + [DMA((9,)), DMA((9,))],
        name="emit",
    )(*outs)
    return (
        y.reshape(1, t, width),
        dx.reshape(1, t, width),
        gain1.reshape(rows),
        fac_own,
        out_own,
        gain2.reshape(rows),
        gate_own,
        up_own,
        down_own,
    )


def solution(mesh):
    return jax.shard_map(
        body,
        mesh=mesh,
        in_specs=(
            P("dp", "ctx", None),
            P("dp", None),
            P(("dp", "ctx")),
            P(("dp", "ctx"), None),
            P(("dp", "ctx"), None),
            P(("dp", "ctx")),
            P(("dp", "ctx"), None),
            P(("dp", "ctx"), None),
            P(("dp", "ctx"), None),
            P("dp", "ctx", None),
        ),
        out_specs=(
            P("dp", "ctx", None),
            P("dp", "ctx", None),
            P(("dp", "ctx")),
            P(("dp", "ctx"), None),
            P(("dp", "ctx"), None),
            P(("dp", "ctx")),
            P(("dp", "ctx"), None),
            P(("dp", "ctx"), None),
            P(("dp", "ctx"), None),
        ),
        check_vma=False,
    )
```

```python
import functools

import jax
import jax.numpy as jnp
import numpy as np
from jax import lax
from jax.experimental import pallas as pl
from jax.experimental.pallas import tpu as pltpu
from jax.sharding import PartitionSpec as P

H = 16
DH = 64
RQ = 6
RKV = 2
EPS = 1e-05
BF = jnp.bfloat16
F32 = jnp.float32
AQ = RQ * H
BQ = RQ * DH
AK = RKV * H
BK = RKV * DH
PACK = 2 * (AK + BK)
KEY_ROWS = AK + BK
FDIM = AQ + BQ + PACK
FPAD = 896
LOG2E = 1.4426950408889634
NEG = -1e30


def nt(a, b):
    return lax.dot_general(a, b, (((1,), (1,)), ((), ())), preferred_element_type=F32)


def nn(a, b):
    return jnp.dot(a, b, preferred_element_type=F32)

MESH = pl.DeviceIdType.MESH


def ring_place(c, n):
    z = c // 2
    return z + (c % 2) * (n - 1 - 2 * z)


def ring_index(p, n):
    p = (p + 2 * n) % n
    q = p // (n // 2)
    return (1 - q) * (2 * p) + q * (2 * (n - 1 - p) + 1)


def remote(src, dst, send, recv, dev):
    return pltpu.make_async_remote_copy(
        src_ref=src, dst_ref=dst, send_sem=send, recv_sem=recv, device_id=dev, device_id_type=MESH
    )


def places():
    d, c = lax.axis_index("dp"), lax.axis_index("ctx")
    core = d % 2
    return d, c, core, d + 1 - 2 * core, (d + 2) % 4


def greet(n):
    d, c, _, _, _ = places()
    barrier = pltpu.get_barrier_semaphore()
    n_dp = lax.axis_size("dp")
    for k in range(1, n_dp):
        pl.semaphore_signal(barrier, inc=1, device_id=((d + k) % n_dp, c), device_id_type=MESH)
    for k in range(1, n):
        pl.semaphore_signal(barrier, inc=1, device_id=(d, (c + k) % n), device_id_type=MESH)


def met(n):
    pl.semaphore_wait(pltpu.get_barrier_semaphore(), n + lax.axis_size("dp") - 2)


def steps(lo, hi, step):
    if isinstance(lo, int) and isinstance(hi, int) and hi - lo <= 4:
        for s in range(lo, hi):
            step(s)
    elif not (isinstance(lo, int) and isinstance(hi, int) and hi <= lo):
        lax.fori_loop(lo, hi, lambda s, _: (step(s), _)[1], 0)


class GatherRing:
    def __init__(self, n, slot, half, send, recv):
        self.n, self.h, self.slot, self.half, self.send, self.recv = n, n // 2, slot, half, send, recv
        self.d, c, _, _, _ = places()
        self.r = ring_place(c, n)

    def copy(self, s, i, arriving=False):
        way = 1 - 2 * i
        last = isinstance(s, int) and s == self.h - 1
        owner = ring_index(self.r - way * (s + (1 if arriving else 0)), self.n)
        ref = self.half(owner, i) if last else self.slot(owner)
        to = (self.d, ring_index(self.r + way, self.n))
        return remote(ref, ref, self.send.at[i, s], self.recv.at[i, s], to)

    def start(self, s):
        for i in range(2):
            self.copy(s, i).start()

    def arrive(self, s):
        for i in range(2):
            self.copy(s, i, True).wait_recv()

    def step(self, s):
        for i in range(2):
            self.copy(s - 1, i, True).wait_recv()
            self.copy(s, i).start()

    def last(self):
        self.step(self.h - 1)

    def drain(self):
        steps(0, self.h - 1, lambda s: [self.copy(s, i).wait_send() for i in range(2)])
        for i in range(2):
            self.copy(self.h - 1, i).wait_send()


class WideGather:
    def __init__(self, n, ref, half, send, recv, x_send, x_recv):
        self.d, self.c, _, _, self.xd = places()
        self.n, self.h, self.ref = n, n // 2, ref
        self.x_send, self.x_recv = x_send, x_recv
        self.ring = GatherRing(
            n, lambda o: ref.at[self.d, o], lambda o, w: half(ref.at[self.d, o], w), send, recv
        )

    def pass_on(self, i, owner, arriving=False):
        ref = self.ref.at[self.xd if arriving else self.d, owner]
        return remote(ref, ref, self.x_send.at[i], self.x_recv.at[i], (self.xd, self.c))

    def owner(self, s, i):
        return ring_index(self.ring.r - (1 - 2 * i) * (s + 1), self.n)

    def start(self, now):
        if now:
            self.pass_on(0, self.c).start()
        self.ring.start(0)

    def step(self, s, now):
        self.ring.step(s)
        if now:
            for i in range(2):
                self.pass_on(2 * s - 1 + i, self.owner(s - 1, i)).start()

    def finish(self, now):
        self.ring.arrive(self.h - 1)
        if now:
            self.pass_on(self.n - 1, self.owner(self.h - 1, 0)).start()
        else:
            self.passed(lambda i, o: self.pass_on(i, o).start())

    def passed(self, wait):
        wait(0, self.c)
        steps(0, self.h - 1, lambda s: [wait(1 + 2 * s + i, self.owner(s, i)) for i in range(2)])
        wait(self.n - 1, self.owner(self.h - 1, 0))

    def arrive(self):
        self.passed(lambda i, o: self.pass_on(i, o, True).wait_recv())

    def drain(self):
        self.ring.drain()
        self.passed(lambda i, o: self.pass_on(i, o).wait_send())


class ScatterRing:
    def __init__(self, n, part, half, land, whole_of, half_of, send, recv):
        self.n, self.h, self.part, self.half = n, n // 2, part, half
        self.land, self.whole_of, self.half_of = land, whole_of, half_of
        self.send, self.recv = send, recv
        self.d, c, _, _, _ = places()
        self.c, self.r = c, ring_place(c, n)

    def copy(self, s, i):
        way = 1 - 2 * i
        to = (self.d, ring_index(self.r + way, self.n))
        first = isinstance(s, int) and s == 0
        if first:
            owner = ring_index(self.r + way * self.h, self.n)
            src, dst = self.half(owner, i), self.half_of(self.land.at[i, 0], i)
        else:
            src, dst = self.land.at[i, s - 1], self.land.at[i, s]
        return remote(src, dst, self.send.at[i, s], self.recv.at[i, s], to)

    def start(self):
        for i in range(2):
            self.copy(0, i).start()

    def step(self, s):
        first = isinstance(s, int) and s == 1
        for i in range(2):
            way = 1 - 2 * i
            self.copy(s - 1, i).wait_recv()
            owner = ring_index(self.r + way * (self.h - s), self.n)
            held = self.land.at[i, s - 1]
            if first:
                mine = self.half_of(held, i)
                mine[...] = (mine[...].astype(F32) + self.half(owner, i)[...].astype(F32)).astype(BF)
                self.half_of(held, 1 - i)[...] = self.half(owner, 1 - i)[...]
            else:
                held[...] = (held[...].astype(F32) + self.part(owner)[...].astype(F32)).astype(BF)
            self.copy(s, i).start()

    def rest(self, lo, hi):
        if lo == 1 and hi > 1:
            self.step(1)
            lo = 2
        steps(lo, hi, self.step)

    def result(self):
        for i in range(2):
            self.copy(self.h - 1, i).wait_recv()
        out = self.part(self.c)[...].astype(F32)
        for i in range(2):
            out = out + self.land[i, self.h - 1].astype(F32)
        return out

    def drain(self):
        for i in range(2):
            self.copy(0, i).wait_send()
        steps(1, self.h, lambda s: [self.copy(s, i).wait_send() for i in range(2)])


class Spread:
    def __init__(self, ref, send, recv):
        d, c, _, cd, xd = places()
        self.copies = [
            remote(ref.at[d], ref.at[d], send.at[0], recv.at[0], (cd, c)),
            remote(ref.at[d], ref.at[d], send.at[1], recv.at[1], (xd, c)),
            remote(ref.at[xd], ref.at[xd], send.at[2], recv.at[2], (cd, c)),
        ]

    def start(self):
        self.copies[1].start()
        self.copies[0].start()

    def forward(self):
        self.copies[1].wait_recv()
        self.copies[2].start()

    def finish(self):
        self.copies[0].wait_recv()
        self.copies[2].wait_recv()
        for copy in self.copies:
            copy.wait_send()


def blocks(count, step, state):
    if count <= 8:
        for j in range(count):
            state = step(j, state)
        return state
    return lax.fori_loop(0, count, step, state)


def lane_block(j, size):
    if isinstance(j, int):
        return pl.ds(j * size, size)
    return pl.ds(pl.multiple_of(j * size, size), size)


def rope(b, cosine, sine, ranks):
    parts = []
    half = DH // 2
    for r in range(ranks):
        u1 = b[r * DH : r * DH + half]
        u2 = b[r * DH + half : (r + 1) * DH]
        parts += [u1 * cosine - u2 * sine, u2 * cosine + u1 * sine]
    return jnp.concatenate(parts, axis=0)


def rope_back(v, cosine, sine, ranks):
    return rope(v, cosine, -sine, ranks)


def pre_part(x, g1, w, cosine, sine, nt_ref, q_ref, p_ref, a_ref, b_ref):
    r1 = lax.rsqrt(jnp.mean(x * x, axis=-1, keepdims=True) + EPS)
    n = (x * r1 * g1).astype(BF)
    nt_ref[...] = n.T
    ft = nn(n, w).T
    a = ft[:AQ]
    b = rope(ft[AQ : AQ + BQ], cosine, sine, RQ)
    for i in range(AQ):
        a_ref[i] = a[i : i + 1]
    b_ref[...] = b
    k0 = AQ + BQ
    bk = rope(ft[k0 + AK : k0 + AK + BK], cosine, sine, RKV)
    p_ref[...] = jnp.concatenate(
        [ft[k0 : k0 + AK], bk, ft[k0 + KEY_ROWS : k0 + PACK]], axis=0
    ).astype(BF)
    for h in range(H):
        acc = a[h : h + 1] * b[:DH]
        for r in range(1, RQ):
            acc = acc + a[r * H + h : r * H + h + 1] * b[r * DH : (r + 1) * DH]
        q_ref[h * DH : (h + 1) * DH, :] = (acc * (1.0 / RQ)).astype(BF)


def vectors(kv_ref, side, r, lanes):
    first = side * KEY_ROWS + AK + r * DH
    return kv_ref[first : first + DH, lanes].astype(F32)


def expand_pair(ka, kv_ref, side, p, lanes):
    rows = []
    for hh in range(2):
        acc = 0.0
        for r in range(RKV):
            acc = acc + ka[side * AK + r * H + 2 * p + hh] * vectors(kv_ref, side, r, lanes)
        rows.append(acc * (1.0 / RKV))
    return jnp.concatenate(rows, axis=0)


def unpack(kv_ref, ka, lanes):
    for side in range(2):
        first = side * KEY_ROWS
        a = kv_ref[first : first + AK, lanes].astype(F32)
        for i in range(AK):
            ka[side * AK + i] = a[i : i + 1]


def unrolled(pair, some):
    def group(q, carry):
        for u in range(some):
            pair(q * some + u, carry)
        return carry

    lax.fori_loop(0, H // 2 // some, group, 0)


def when(condition, run):
    if isinstance(condition, bool):
        if condition:
            run()
    else:
        pl.when(condition)(run)


def diagonal(pair):
    zero = jnp.zeros((DH, pair.shape[1]), pair.dtype)
    left = jnp.concatenate([pair[:DH], zero], axis=0)
    right = jnp.concatenate([zero, pair[DH:]], axis=0)
    return jnp.concatenate([left, right], axis=1)


def undiagonal(wide):
    t = wide.shape[1] // 2
    return jnp.concatenate([wide[:DH, :t], wide[DH:, t:]], axis=0)


def attend_part(
    nblk, arrive, len_ref, q_ref, kv_ref, at_ref, af_ref, inv_ref, p_out, pbuf, ka, bias, qd_ref,
    num_ref, tot_ref,
):
    t = q_ref.shape[1]
    c = lax.axis_index("ctx")
    tpos = c * t + lax.broadcasted_iota(jnp.int32, (1, t), 1)
    start = jnp.zeros((1, t), jnp.int32)
    run = jnp.int32(0)
    for j in range(len_ref.shape[1]):
        start = jnp.where(tpos >= run, run, start)
        run = run + len_ref[0, j]

    def prepare(p, carry):
        rows = pl.ds(pl.multiple_of(p * 2 * DH, 2 * DH), 2 * DH)
        qd_ref[p] = diagonal(q_ref[rows, :])
        return carry

    lax.fori_loop(0, H // 2, prepare, 0)
    num_ref[...] = jnp.zeros_like(num_ref)
    tot_ref[...] = jnp.zeros_like(tot_ref)

    def block(i, carry):
        j = nblk - 1 - i
        when(i > 0, lambda: arrive(i))
        when(i > 1, lambda: p_out(j + 2).wait())
        lanes = lane_block(j, t)
        unpack(kv_ref, ka, lanes)
        spos = (c - i) * t + lax.broadcasted_iota(jnp.int32, (t, t), 0)
        ok = (spos >= start) & (spos <= tpos)
        bias[...] = jnp.where(ok, 0.0, NEG)

        def pair(p, carry):
            k = expand_pair(ka, kv_ref, 0, p, lanes).T.astype(BF)
            v = expand_pair(ka, kv_ref, 1, p, lanes).astype(BF)
            b = bias[...]
            s = nn(k, qd_ref[p]) * (LOG2E * DH**-0.5) + jnp.concatenate([b, b], axis=1)
            e = jnp.exp2(s)
            tot_ref[p] += jnp.sum(e, axis=0, keepdims=True)
            pb = e.astype(BF)
            pbuf[j % 2, p] = pb
            num_ref[p] += nn(v, pb)
            return carry

        unrolled(pair, 4)
        p_out(j).start()
        return carry

    blocks(nblk, block, 0)

    def finish(p, carry):
        rows = pl.ds(pl.multiple_of(p * 2 * DH, 2 * DH), 2 * DH)
        inv = 1.0 / tot_ref[p]
        af = undiagonal(num_ref[p] * inv)
        af_ref[rows, :] = af
        at_ref[rows, :] = af.astype(BF)
        inv_ref[p] = inv
        return carry

    lax.fori_loop(0, H // 2, finish, 0)
    for j in range(2):
        p_out(j).wait()


def attend_back_part(
    nblk, serve, ship, da_ref, af_ref, inv_ref, p_copy, pbuf, q_ref, kv_ref, a_ref, b_ref,
    cos_ref, sin_ref, dq_ref, ka, dka, dqa, db, dkv, qd_ref, dn_ref, dtot_ref, dqs,
):
    t = q_ref.shape[1]

    def factor_back(dwide, side, p, lanes):
        for hh in range(2):
            d = dwide[hh * DH : (hh + 1) * DH] * (1.0 / RKV)
            for r in range(RKV):
                row = side * AK + r * H + 2 * p + hh
                first = side * KEY_ROWS + AK + r * DH
                b = vectors(kv_ref, side, r, lanes)
                dka[row] = jnp.sum(d * b, axis=0, keepdims=True)
                dkv[first : first + DH, :] += d * ka[row]

    def prepare(p, carry):
        rows = pl.ds(pl.multiple_of(p * 2 * DH, 2 * DH), 2 * DH)
        inv = inv_ref[p]
        dd = diagonal(da_ref[rows, :])
        dn_ref[p] = (dd * inv).astype(BF)
        dtot_ref[p] = -jnp.sum(dd * diagonal(af_ref[rows, :]), axis=0, keepdims=True) * inv
        qd_ref[p] = diagonal(q_ref[rows, :])
        return carry

    lax.fori_loop(0, H // 2, prepare, 0)
    dqs[...] = jnp.zeros_like(dqs)

    def block(j, carry):
        when(j + 1 < nblk, lambda: p_copy(j + 1).start())
        p_copy(j).wait()
        lanes = lane_block(j, t)
        unpack(kv_ref, ka, lanes)
        for side in range(2):
            first = side * KEY_ROWS + AK
            dkv[first : first + BK, :] = jnp.zeros((BK, t), F32)

        def pair(p, carry):
            rows = pl.ds(pl.multiple_of(p * 2 * DH, 2 * DH), 2 * DH)
            k = expand_pair(ka, kv_ref, 0, p, lanes).astype(BF)
            v = expand_pair(ka, kv_ref, 1, p, lanes).T.astype(BF)
            pb = pbuf[j % 2, p]
            dn = dn_ref[p]
            ds = (pb.astype(F32) * (nn(v, dn) + dtot_ref[p])).astype(BF)
            dqs[rows, :] += undiagonal(nn(k, ds))
            factor_back(nt(qd_ref[p], ds) * (DH**-0.5), 0, p, lanes)
            factor_back(nt(dn, pb), 1, p, lanes)
            return carry

        unrolled(pair, 4)
        for side in range(2):
            for i in range(AK):
                dkv[side * KEY_ROWS + i : side * KEY_ROWS + i + 1, :] = dka[side * AK + i]
        ship(j)
        serve(j)
        return carry

    blocks(nblk, block, 0)
    db[...] = jnp.zeros_like(db)

    def pair_q(p, carry):
        rows = pl.ds(pl.multiple_of(p * 2 * DH, 2 * DH), 2 * DH)
        dq = dqs[rows, :] * (DH**-0.5 / RQ)
        for hh in range(2):
            d = dq[hh * DH : (hh + 1) * DH]
            for r in range(RQ):
                row = r * H + 2 * p + hh
                dqa[row] = jnp.sum(d * b_ref[r * DH : (r + 1) * DH, :], axis=0, keepdims=True)
                db[r * DH : (r + 1) * DH, :] += d * a_ref[row]
        return carry

    lax.fori_loop(0, H // 2, pair_q, 0)
    for i in range(AQ):
        dq_ref[i : i + 1, :] = dqa[i]
    dq_ref[AQ : AQ + BQ, :] = rope_back(db[...], cos_ref[...], sin_ref[...], RQ)


def gain_rows(w):
    first = FPAD - 128
    gains = w[:, first:].astype(F32).T
    return gains[FDIM - first : FDIM - first + 1], gains[FDIM - first + 1 : FDIM - first + 2]


def lane_half(ref, w):
    return ref.at[:, :512] if w == 0 else ref.at[:, 512:]


class PairScatter:
    def __init__(self, n, part, held, land, own, send, recv, ring_send, ring_recv, x_first=None):
        d, c, core, cd, xd = places()
        self.x_first = x_first
        self.core, self.x, self.part, self.held, self.own = core, d // 2, part, held, own
        self.swaps = [
            remote(part.at[2 * xx + 1 - core], held.at[xx], send.at[xx], recv.at[xx], (cd, c))
            for xx in range(2)
        ]
        if x_first is not None:
            self.end = remote(held.at[1 - self.x], x_first, send.at[2], recv.at[2], (xd, c))
            self.ring = ScatterRing(
                n, lambda o: x_first.at[o], lambda o, w: lane_half(x_first.at[o], w), land,
                None, lane_half, ring_send, ring_recv,
            )
            return
        self.end = remote(own.at[1 - self.x], own.at[2], send.at[2], recv.at[2], (xd, c))
        self.ring = ScatterRing(
            n, lambda o: held.at[:, o], lambda o, w: held.at[w, o], land,
            None, lambda ref, w: ref.at[w], ring_send, ring_recv,
        )

    def start(self):
        for swap in self.swaps:
            swap.start()

    def enter(self):
        for xx in range(2):
            self.swaps[xx].wait_recv()
            mine = self.part[2 * xx + self.core].astype(F32)
            self.held[xx] = (self.held[xx].astype(F32) + mine).astype(BF)
        if self.x_first is None:
            self.ring.start()
        else:
            self.end.start()

    def across(self):
        self.end.wait_recv()
        total = self.x_first[...].astype(F32) + self.held[self.x].astype(F32)
        self.x_first[...] = total.astype(BF)
        self.ring.start()

    def leave(self):
        total = self.ring.result()
        for xx in range(2):
            self.own[xx] = total[xx].astype(BF)
        self.end.start()

    def result(self):
        self.end.wait_recv()
        return self.own[self.x].astype(F32) + self.own[2].astype(F32)

    def drain(self):
        for copy in self.swaps + [self.end]:
            copy.wait_send()
        self.ring.drain()


def block_kernel(
    n, nblk,
    len_ref, x_ref, cos_ref, sin_ref, fw_ref, g1_ref, g2_ref, ow_ref, gw_ref, uw_ref, dw_ref, cot_in,
    y_ref, dx_ref, fac_ref, gain1_ref, gain2_ref, wo_ref, gate_ref, up_ref, wd_ref, p_ref,
    nt_ref, q_ref, a_ref, b_ref, kv_ref, at_ref, af_ref, inv_ref, pbuf,
    fac, wo, gu, wd, nm, cot, mid_ref, dn_in, out_in, gu_part, wd_part,
    kv_land, gu_land, wd_land, gu_own, da_ref, dq_ref, dmid_ref, dp_land,
    fac_part, wo_part, fac_held, wo_held, fac_land, wo_land, fac_own, wo_own,
    own_sem, near_send, near_recv, ring_send, ring_recv, kv_send, kv_recv, sp_send, sp_recv,
    dkv_send, dkv_recv, end_send, end_recv, dp_send, dp_recv, pair_send, pair_recv, p_sem, own_dkv,
    gu_in, gu_ref, x_send, x_recv,
):
    d, c, core, cd, xd = places()
    t = x_ref.shape[0]
    n_dp = 4
    rows, ffq = gu_in.shape[1], gu_in.shape[2] // 2
    greet(n)
    keep_cot = pltpu.make_async_copy(cot_in, cot.at[d], own_sem.at[4])
    keep_cot.start()
    tail = FPAD - 128
    lane = lax.broadcasted_iota(jnp.int32, (rows, 128), 1)
    diag = lax.broadcasted_iota(jnp.int32, (rows, rows), 0) == lax.broadcasted_iota(
        jnp.int32, (rows, rows), 1
    )

    def column(ref):
        return jnp.sum(jnp.where(diag, ref[...], 0.0), axis=1, keepdims=True)

    gains = jnp.where(lane == FDIM - tail, column(g1_ref), 0.0)
    gains = jnp.where(lane == FDIM + 1 - tail, column(g2_ref), gains)
    fac[d, c, :, :tail] = fw_ref[:, :tail].astype(BF)
    fac[d, c, :, tail:] = gains.astype(BF)
    fac[d, c, :, tail:FDIM] = fw_ref[:, tail:].astype(BF)
    wo[d, c] = ow_ref[...].astype(BF)
    wd[c] = dw_ref[...].astype(BF)
    for dd in range(n_dp):
        for side, ref in enumerate((gw_ref, uw_ref)):
            gu_in[dd, :, side * ffq : (side + 1) * ffq] = ref[:, dd * ffq : (dd + 1) * ffq].astype(BF)
    keep_gu = pltpu.make_async_copy(gu_in.at[d], gu.at[d, c], own_sem.at[2])
    keep_gu.start()
    for k in range(1, nblk):
        @pl.when(c - k < 0)
        def _():
            kv_ref[:, (nblk - 1 - k) * t : (nblk - k) * t] = jnp.zeros((PACK, t), BF)
    met(n)

    fo = WideGather(n, fac, lane_half, ring_send.at[0], ring_recv.at[0], x_send.at[0], x_recv.at[0])
    oo = WideGather(n, wo, lane_half, ring_send.at[1], ring_recv.at[1], x_send.at[1], x_recv.at[1])
    cut = -(-dw_ref.shape[0] // 16) * 8
    gr = GatherRing(
        n, lambda o: gu.at[:, o], lambda o, w: gu.at[2 * w : 2 * w + 2, o],
        ring_send.at[4], ring_recv.at[4],
    )
    dr = GatherRing(
        n, lambda o: wd.at[o], lambda o, w: wd.at[o, :cut] if w == 0 else wd.at[o, cut:],
        ring_send.at[5], ring_recv.at[5],
    )
    small, large = (fo, oo), (gr, dr)
    fo.start(True)
    oo.start(False)
    a2a = []
    for k in range(1, n_dp):
        to = (d + k) % n_dp
        a2a.append(
            (
                remote(gu_in.at[to], gu.at[d, c], near_send.at[1 + k], near_recv.at[1 + k], (to, c)),
                remote(
                    gu_in.at[to], gu.at[(d + n_dp - k) % n_dp, c],
                    near_send.at[1 + k], near_recv.at[1 + k], (to, c),
                ),
            )
        )
        a2a[-1][0].start()
    cots = Spread(cot, sp_send.at[0], sp_recv.at[0])
    nms = Spread(nm, sp_send.at[1], sp_recv.at[1])
    steps(1, n // 2 - 1, lambda s: (fo.step(s, True), oo.step(s, False)))
    fo.step(n // 2 - 1, True)
    oo.step(n // 2 - 1, False)
    keep_gu.wait()
    for _, arrival in a2a:
        arrival.wait_recv()
    gr.start(0)

    def core_swap(ref, i, dd, da):
        return (
            remote(ref.at[dd], ref.at[dd], near_send.at[5 + i], near_recv.at[5 + i], (cd, c)),
            remote(ref.at[da], ref.at[da], near_send.at[5 + i], near_recv.at[5 + i], (cd, c)),
        )

    near = []

    def swap(i, ref, dd, da):
        near.append(core_swap(ref, i, dd, da))
        near[-1][0].start()

    fo.finish(True)
    swap(0, fac, d, cd)
    oo.finish(False)
    swap(2, wo, d, cd)
    fo.arrive()
    swap(1, fac, xd, (cd + 2) % 4)
    keep_cot.wait()
    cots.start()
    for _, arrival in (near[0], near[2]):
        arrival.wait_recv()

    width = x_ref.shape[1]
    x = x_ref[...].astype(F32)
    w = fac[...].reshape(width, FPAD)
    g1, g2 = gain_rows(w)
    own_kv = kv_ref.at[:, (nblk - 1) * t : nblk * t]
    pre_part(x, g1, w, cos_ref[...], sin_ref[...], nt_ref, q_ref, own_kv, a_ref, b_ref)

    def kv_copy(k):
        dst = kv_ref.at[:, lane_block(nblk - 1 - k, t)]
        return remote(own_kv, dst, kv_send.at[k - 1], kv_recv.at[k - 1], (d, (c + k) % n))

    for k in range(1, nblk):
        @pl.when(c + k < n)
        def _():
            kv_copy(k).start()
    dr.start(0)
    oo.arrive()
    swap(3, wo, xd, (cd + 2) % 4)
    full = n // 2 - 1
    middle_step = 1 + full // 2

    def arrive(i):
        @pl.when(c - i >= 0)
        def _():
            kv_copy(i).wait_recv()

        when(i == 2, lambda: steps(1, middle_step, gr.step))


    def p_out(j):
        return pltpu.make_async_copy(pbuf.at[j % 2], p_ref.at[j], p_sem.at[j % 2])

    pl.run_scoped(
        functools.partial(
            attend_part, nblk, arrive, len_ref, q_ref, kv_ref, at_ref, af_ref, inv_ref, p_out, pbuf
        ),
        pltpu.VMEM((2 * AK, 1, t), F32),
        pltpu.VMEM((t, t), F32),
        pltpu.VMEM((H // 2, 2 * DH, 2 * t), BF),
        pltpu.VMEM((H // 2, 2 * DH, 2 * t), F32),
        pltpu.VMEM((H // 2, 1, 2 * t), F32),
    )

    steps(1, middle_step, dr.step)
    for _, arrival in (near[1], near[3]):
        arrival.wait_recv()
    middle = x + nn(at_ref[...].T, wo[...].reshape(width, width))
    mid_ref[...] = middle
    r2 = lax.rsqrt(jnp.mean(middle * middle, axis=-1, keepdims=True) + EPS)
    nm[d] = (middle * r2 * g2).astype(BF)
    nms.start()
    cots.forward()
    steps(middle_step, full, lambda s: [one.step(s) for one in large])
    nms.forward()
    nms.finish()
    cots.finish()
    for one in large:
        one.last()
    for one in large:
        one.arrive(n // 2 - 1)

    x_at = d // 2
    parts = (dn_in, out_in)
    first = []
    for i, part in enumerate(parts):
        for j, xx in enumerate((1 - x_at, x_at)):
            first.append(
                remote(
                    part.at[2 * xx + 1 - core], dp_land.at[i, j],
                    dp_send.at[i, j], dp_recv.at[i, j], (cd, c),
                )
            )

    cut = -(-wd_part.shape[1] // 16) * 8

    def wd_half(ref, w):
        return ref.at[:cut] if w == 0 else ref.at[cut:]

    gs = ScatterRing(
        n, lambda o: gu_part.at[:, o], lambda o, w: gu_part.at[2 * w : 2 * w + 2, o], gu_land,
        None, lambda ref, w: ref.at[2 * w : 2 * w + 2], ring_send.at[6], ring_recv.at[6],
    )
    ds_ = ScatterRing(
        n, lambda o: wd_part.at[o], lambda o, w: wd_half(wd_part.at[o], w), wd_land,
        None, wd_half, ring_send.at[7], ring_recv.at[7],
    )
    scatter = (gs, ds_)
    fs = PairScatter(
        n, fac_part, fac_held, fac_land, fac_own, pair_send.at[0], pair_recv.at[0],
        ring_send.at[8], ring_recv.at[8],
    )
    ws = PairScatter(
        n, wo_part, wo_held, wo_land, wo_own, pair_send.at[1], pair_recv.at[1],
        ring_send.at[9], ring_recv.at[9], wo_own,
    )
    h = n // 2

    def advance(s):
        for one in scatter:
            one.step(s)

    points = 2

    def serve(k):
        steps(2 + -(-(k - 1) * (h - 2) // points), 2 + -(-k * (h - 2) // points), advance)

    def feed(both_ff, dh, hid, dgu):
        down = wd[...].reshape(ffq, width)

        def matrix():
            return gu[...].reshape(width, 2 * ffq)

        def pair_rows(i, carry):
            xx = i * x_at + (1 - i) * (1 - x_at)
            two = pl.ds(2 * xx, 2)
            both = 2 * t
            both_ff[...] = nn(nm[two].reshape(both, width), matrix())
            dh[...] = nt(cot[two].reshape(both, width), down)
            base = pl.multiple_of(xx * both, both)

            def rows_of(k, carry):
                some = pl.ds(pl.multiple_of(k * 32, 32), 32)
                to = pl.ds(pl.multiple_of(base + k * 32, 32), 32)
                v, u, g = both_ff[some, :ffq], both_ff[some, ffq:], dh[some, :]
                sig, act = silu_parts(v)
                hid[to, :] = (act * u).astype(BF)
                dgu[to, :ffq] = (g * u * sig * (1.0 + v * (1.0 - sig))).astype(BF)
                dgu[to, ffq:] = (g * act).astype(BF)
                return carry

            lax.fori_loop(0, both // 32, rows_of, 0)
            return carry

        def pair_back(i, carry):
            xx = i * x_at + (1 - i) * (1 - x_at)
            two = pl.ds(2 * xx, 2)
            both = 2 * t
            all_rows = pl.ds(pl.multiple_of(xx * both, both), both)
            dn_in[two] = nt(dgu[all_rows, :], matrix()).astype(BF).reshape(2, t, width)
            out_in[two] = nn(hid[all_rows, :], down).astype(BF).reshape(2, t, width)

            @pl.when(i == 0)
            def _():
                first[0].start()
                first[2].start()

            return carry

        lax.fori_loop(0, 2, pair_rows, 0)

        def tn(a, b):
            return lax.dot_general(a, b, (((0,), (0,)), ((), ())), preferred_element_type=F32)

        quarter = width // n_dp

        def columns(j, carry):
            lanes = pl.ds(pl.multiple_of(j * quarter, quarter), quarter)
            some = nm[:, :, lanes].reshape(n_dp * t, quarter)
            gu_part[j] = tn(some, dgu[...]).astype(BF).reshape(gu_part.shape[1:])
            c_some = cot[:, :, lanes].reshape(n_dp * t, quarter)
            wd_part[:, :, lanes] = tn(hid[...], c_some).astype(BF).reshape(wd_part.shape[:2] + (quarter,))
            return carry

        lax.fori_loop(0, n_dp, columns, 0)
        for one in scatter:
            one.start()
        lax.fori_loop(0, 2, pair_back, 0)
        first[1].start()
        first[3].start()
        for i, part in enumerate(parts):
            first[2 * i].wait_recv()
            dp_land[i, 0] = (dp_land[i, 0].astype(F32) + part[xd].astype(F32)).astype(BF)
            dp_next(i).start()
        advance(1)

    def dp_next(i):
        return remote(dp_land.at[i, 0], dp_land.at[i, 2], dp_send.at[i, 2], dp_recv.at[i, 2], (xd, c))

    pl.run_scoped(
        feed,
        pltpu.VMEM((2 * t, 2 * ffq), F32),
        pltpu.VMEM((2 * t, ffq), F32),
        pltpu.VMEM((n_dp * t, ffq), BF),
        pltpu.VMEM((n_dp * t, 2 * ffq), BF),
    )
    second = [dp_next(i) for i in range(2)]
    for i in range(2):
        first[2 * i + 1].wait_recv()
    second[0].wait_recv()
    middle = mid_ref[...]
    dn = dn_in[d].astype(F32) + dp_land[0, 1].astype(F32) + dp_land[0, 2].astype(F32)
    second_part = jnp.sum(dn * middle * r2, axis=0, keepdims=True)
    u2 = dn * g2
    d_middle = (
        cot_in[...].astype(F32)
        + r2 * u2
        - middle * (r2 * r2 * r2 * jnp.mean(u2 * middle, axis=-1, keepdims=True))
    )
    dmid_ref[...] = d_middle
    serve(1)
    d_branch = d_middle.astype(BF)
    wo_part[...] = nn(at_ref[...], d_branch).astype(BF).reshape(wo_part.shape)
    ws.start()
    da_ref[...] = nt(wo[...].reshape(width, width), d_branch)
    second[1].wait_recv()
    y_ref[...] = (
        mid_ref[...]
        + (out_in[d].astype(F32) + dp_land[1, 1].astype(F32) + dp_land[1, 2].astype(F32))
    ).astype(BF)
    ws.enter()
    def serve_block(j):
        when(j == nblk - 1, lambda: serve(2))

    def p_copy(j):
        return pltpu.make_async_copy(p_ref.at[j], pbuf.at[j % 2], p_sem.at[j % 2])

    p_copy(0).start()

    def attention_back(dkv16, dkv, *scratch):
        def dkv_copy(k):
            return remote(
                dkv16.at[k - 1], kv_land.at[k - 1], dkv_send.at[k - 1], dkv_recv.at[k - 1],
                (d, (c + n - k) % n),
            )

        def ship(j):
            k = nblk - 1 - j

            def away():
                dkv16[k - 1] = dkv[...].astype(BF)

                @pl.when(c - k >= 0)
                def _():
                    dkv_copy(k).start()

            def home():
                own_dkv[...] = dkv[...]

            when(k > 0, away)
            when(k == 0, home)

        ka, dka, dqa, db, qd, dn, dtot, dqs = scratch
        attend_back_part(
            nblk, serve_block, ship, da_ref, af_ref, inv_ref, p_copy, pbuf, q_ref, kv_ref, a_ref,
            b_ref, cos_ref, sin_ref, dq_ref, ka, dka, dqa, db, dkv, qd, dn, dtot, dqs,
        )
        for k in range(1, nblk):
            @pl.when(c + k < n)
            def _():
                dkv_copy(k).wait_recv()
                own_dkv[...] += kv_land[k - 1].astype(F32)
        for k in range(1, nblk):
            @pl.when(c - k >= 0)
            def _():
                dkv_copy(k).wait_send()

    pl.run_scoped(
        attention_back,
        pltpu.VMEM((nblk - 1, PACK, t), BF),
        pltpu.VMEM((PACK, t), F32),
        pltpu.VMEM((2 * AK, 1, t), F32),
        pltpu.VMEM((2 * AK, 1, t), F32),
        pltpu.VMEM((AQ, 1, t), F32),
        pltpu.VMEM((BQ, t), F32),
        pltpu.VMEM((H // 2, 2 * DH, 2 * t), BF),
        pltpu.VMEM((H // 2, 2 * DH, 2 * t), BF),
        pltpu.VMEM((H // 2, 1, 2 * t), F32),
        pltpu.VMEM((H * DH, t), F32),
    )
    ws.across()
    dp = own_dkv[...]
    d_bk = rope_back(dp[AK : AK + BK], cos_ref[...], sin_ref[...], RKV)
    d_fac_t = jnp.concatenate(
        [dq_ref[...], dp[:AK], d_bk, dp[KEY_ROWS:], jnp.zeros((FPAD - FDIM, t), F32)], axis=0
    ).astype(BF)
    x = x_ref[...].astype(F32)
    r1 = lax.rsqrt(jnp.mean(x * x, axis=-1, keepdims=True) + EPS)
    d_norm_in = nt(d_fac_t.T, w)
    first_part = jnp.sum(d_norm_in * x * r1, axis=0, keepdims=True)
    tail = FPAD - 128
    gains = jnp.concatenate(
        [jnp.zeros((FDIM - tail, width), F32), first_part, second_part,
         jnp.zeros((FPAD - FDIM - 2, width), F32)], axis=0).T
    product = nt(nt_ref[...], d_fac_t)
    shape = fac_part.shape[:3]
    fac_part[:, :, :, :tail] = product[:, :tail].astype(BF).reshape(shape + (tail,))
    fac_part[:, :, :, tail:] = (product[:, tail:] + gains).astype(BF).reshape(shape + (128,))
    fs.start()
    u1 = d_norm_in * g1
    dx_ref[...] = (
        dmid_ref[...] + r1 * u1 - x * (r1 * r1 * r1 * jnp.mean(u1 * x, axis=-1, keepdims=True))
    ).astype(BF)
    ws.ring.step(1)
    fs.enter()
    gu_own[...] = gs.result().astype(BF)
    keep = pltpu.make_async_copy(gu_own.at[d], gu_ref.at[d], own_sem.at[0])
    keep.start()
    last = []
    for k in range(1, n_dp):
        to = (d + k) % n_dp
        last.append(
            (
                remote(gu_own.at[to], gu_ref.at[d], end_send.at[k - 1], end_recv.at[k - 1], (to, c)),
                remote(
                    gu_own.at[to], gu_ref.at[(d + n_dp - k) % n_dp],
                    end_send.at[k - 1], end_recv.at[k - 1], (to, c),
                ),
            )
        )
        last[-1][0].start()
    steps(2, h, ws.ring.step)
    fs.ring.step(1)
    wd_ref[...] = ds_.result()
    steps(2, h, fs.ring.step)
    wo_ref[...] = ws.ring.result()
    fs.leave()
    for out, arrival in last:
        arrival.wait_recv()
        out.wait_send()
    keep.wait()
    for dd in range(n_dp):
        lanes = slice(dd * ffq, (dd + 1) * ffq)
        gate_ref[:, lanes] = gu_ref[dd, :, :ffq].astype(F32)
        up_ref[:, lanes] = gu_ref[dd, :, ffq:].astype(F32)
    total = fs.result()
    fac_ref[...] = total[:, :FDIM]
    for i, ref in enumerate((gain1_ref, gain2_ref)):
        one = total[:, FDIM + i : FDIM + i + 1]
        ref[...] = jnp.sum(jnp.where(diag, one, 0.0), axis=0, keepdims=True)
    for copy in first + second:
        copy.wait_send()
    for one in scatter + (ws, fs):
        one.drain()
    for k in range(1, nblk):
        @pl.when(c + k < n)
        def _():
            kv_copy(k).wait_send()
    for out, _ in a2a + near:
        out.wait_send()
    for one in small + large:
        one.drain()


def emit_kernel(*refs):
    k = (len(refs) - 2) // 3
    ins, outs, bufs, sems = refs[:k], refs[k : 2 * k], refs[2 * k : 3 * k], refs[3 * k :]
    into = [pltpu.make_async_copy(a, b, sems[0].at[i]) for i, (a, b) in enumerate(zip(ins, bufs))]
    out = [pltpu.make_async_copy(a, b, sems[1].at[i]) for i, (a, b) in enumerate(zip(bufs, outs))]
    for copy in into:
        copy.start()
    for one, two in zip(into, out):
        one.wait()
        two.start()
    for copy in out:
        copy.wait()


def vmem(n):
    return [pl.BlockSpec(memory_space=pltpu.VMEM)] * n


def hbm(n):
    return [pl.BlockSpec(memory_space=pl.ANY)] * n


SMEM = pl.BlockSpec(memory_space=pltpu.SMEM)
DMA = pltpu.SemaphoreType.DMA


def talks(i):
    return pltpu.CompilerParams(
        collective_id=i, has_side_effects=True, vmem_limit_bytes=63 * 1024 * 1024
    )


def silu_parts(gate):
    s = jax.nn.sigmoid(gate)
    return s, gate * s


def body(
    tokens,
    doc_lengths,
    first_gain,
    factor_weights,
    output_weights,
    second_gain,
    gate_weights,
    up_weights,
    down_weights,
    cotangent,
):
    _, t, width = tokens.shape
    n_ctx, n_dp = lax.axis_size("ctx"), lax.axis_size("dp")
    n_all = n_ctx * n_dp
    both = ("dp", "ctx")
    length = t * n_ctx
    nblk = min(n_ctx, -(-(length // 2 - 1) // t) + 1)
    ff = gate_weights.shape[1]
    ffq = ff // n_dp
    rows = width // n_all
    c = lax.axis_index("ctx")

    h = n_ctx // 2

    half = DH // 2
    freq = 10000.0 ** (-(np.arange(half) * 2.0 / DH))
    pos = (c * t + jnp.arange(t, dtype=jnp.int32)).astype(F32)
    angles = jnp.asarray(freq, F32)[:, None] * pos[None, :]
    cosine, sine = jnp.cos(angles), jnp.sin(angles)

    x16 = tokens.reshape(t, width)
    cot_own = cotangent.reshape(t, width)
    sds = jax.ShapeDtypeStruct
    down_rows = down_weights.shape[0]
    outs = pl.pallas_call(
        functools.partial(block_kernel, n_ctx, nblk),
        out_shape=(
            sds((t, width), BF),
            sds((t, width), BF),
            sds((rows, FDIM), F32),
            sds((1, rows), F32),
            sds((1, rows), F32),
            sds((rows, width), F32),
            sds((rows, ff), F32),
            sds((rows, ff), F32),
            sds((down_rows, width), F32),
            sds((nblk, H // 2, t, 2 * t), BF),
        ),
        in_specs=[SMEM] + vmem(11),
        out_specs=tuple(vmem(9) + hbm(1)),
        scratch_shapes=[
            pltpu.VMEM((width, t), BF),
            pltpu.VMEM((H * DH, t), BF),
            pltpu.VMEM((AQ, 1, t), F32),
            pltpu.VMEM((BQ, t), F32),
            pltpu.VMEM((PACK, nblk * t), BF),
            pltpu.VMEM((H * DH, t), BF),
            pltpu.VMEM((H * DH, t), F32),
            pltpu.VMEM((H // 2, 1, 2 * t), F32),
            pltpu.VMEM((2, H // 2, t, 2 * t), BF),
            pltpu.VMEM((n_dp, n_ctx, rows, FPAD), BF),
            pltpu.VMEM((n_dp, n_ctx, rows, width), BF),
            pltpu.VMEM((n_dp, n_ctx, rows, 2 * ffq), BF),
            pltpu.VMEM((n_ctx, down_rows, width), BF),
            pltpu.VMEM((n_dp, t, width), BF),
            pltpu.VMEM((n_dp, t, width), BF),
            pltpu.VMEM((t, width), F32),
            pltpu.VMEM((n_dp, t, width), BF),
            pltpu.VMEM((n_dp, t, width), BF),
            pltpu.VMEM((n_dp, n_ctx, rows, 2 * ffq), BF),
            pltpu.VMEM((n_ctx, down_rows, width), BF),
            pltpu.VMEM((nblk - 1, PACK, t), BF),
            pltpu.VMEM((2, h, n_dp, rows, 2 * ffq), BF),
            pltpu.VMEM((2, h, down_rows, width), BF),
            pltpu.VMEM((n_dp, rows, 2 * ffq), BF),
            pltpu.VMEM((H * DH, t), F32),
            pltpu.VMEM((AQ + BQ, t), F32),
            pltpu.VMEM((t, width), F32),
            pltpu.VMEM((2, 3, t, width), BF),
            pltpu.VMEM((n_dp, n_ctx, rows, FPAD), BF),
            pltpu.VMEM((n_dp, n_ctx, rows, width), BF),
            pltpu.VMEM((2, n_ctx, rows, FPAD), BF),
            pltpu.VMEM((2, n_ctx, rows, width), BF),
            pltpu.VMEM((2, h, 2, rows, FPAD), BF),
            pltpu.VMEM((2, h, rows, width), BF),
            pltpu.VMEM((3, rows, FPAD), BF),
            pltpu.VMEM((n_ctx, rows, width), BF),
            DMA((5,)),
            DMA((9,)),
            DMA((9,)),
            DMA((10, 2, h)),
            DMA((10, 2, h)),
            DMA((nblk - 1,)),
            DMA((nblk - 1,)),
            DMA((2, 3)),
            DMA((2, 3)),
            DMA((nblk - 1,)),
            DMA((nblk - 1,)),
            DMA((3,)),
            DMA((3,)),
            DMA((2, 3)),
            DMA((2, 3)),
            DMA((2, 3)),
            DMA((2, 3)),
            DMA((2,)),
            pltpu.VMEM((PACK, t), F32),
            pltpu.VMEM((n_dp, rows, 2 * ffq), BF),
            pltpu.VMEM((n_dp, rows, 2 * ffq), BF),
            DMA((2, n_ctx)),
            DMA((2, n_ctx)),
        ],
        compiler_params=talks(0),
        name="block",
    )(doc_lengths, x16, cosine, sine, factor_weights, first_gain.reshape(1, rows),
      second_gain.reshape(1, rows), output_weights, gate_weights, up_weights, down_weights, cot_own)
    outs = outs[:9]
    y, dx, fac_own, gain1, gain2, out_own, gate_own, up_own, down_own = pl.pallas_call(
        emit_kernel,
        out_shape=tuple(sds(o.shape, o.dtype) for o in outs),
        in_specs=hbm(9),
        out_specs=tuple(hbm(9)),
        scratch_shapes=[pltpu.VMEM(o.shape, o.dtype) for o in outs] + [DMA((9,)), DMA((9,))],
        name="emit",
    )(*outs)
    return (
        y.reshape(1, t, width),
        dx.reshape(1, t, width),
        gain1.reshape(rows),
        fac_own,
        out_own,
        gain2.reshape(rows),
        gate_own,
        up_own,
        down_own,
    )


def solution(mesh):
    return jax.shard_map(
        body,
        mesh=mesh,
        in_specs=(
            P("dp", "ctx", None),
            P("dp", None),
            P(("dp", "ctx")),
            P(("dp", "ctx"), None),
            P(("dp", "ctx"), None),
            P(("dp", "ctx")),
            P(("dp", "ctx"), None),
            P(("dp", "ctx"), None),
            P(("dp", "ctx"), None),
            P("dp", "ctx", None),
        ),
        out_specs=(
            P("dp", "ctx", None),
            P("dp", "ctx", None),
            P(("dp", "ctx")),
            P(("dp", "ctx"), None),
            P(("dp", "ctx"), None),
            P(("dp", "ctx")),
            P(("dp", "ctx"), None),
            P(("dp", "ctx"), None),
            P(("dp", "ctx"), None),
        ),
        check_vma=False,
    )
```

```python
import functools

import jax
import jax.numpy as jnp
import numpy as np
from jax import lax
from jax.experimental import pallas as pl
from jax.experimental.pallas import tpu as pltpu
from jax.sharding import PartitionSpec as P

H = 16
DH = 64
RQ = 6
RKV = 2
EPS = 1e-05
BF = jnp.bfloat16
F32 = jnp.float32
AQ = RQ * H
BQ = RQ * DH
AK = RKV * H
BK = RKV * DH
PACK = 2 * (AK + BK)
KEY_ROWS = AK + BK
FDIM = AQ + BQ + PACK
FPAD = 896
LOG2E = 1.4426950408889634
NEG = -1e30


def nt(a, b):
    return lax.dot_general(a, b, (((1,), (1,)), ((), ())), preferred_element_type=F32)


def nn(a, b):
    return jnp.dot(a, b, preferred_element_type=F32)

MESH = pl.DeviceIdType.MESH


def ring_place(c, n):
    z = c // 2
    return z + (c % 2) * (n - 1 - 2 * z)


def ring_index(p, n):
    p = (p + 2 * n) % n
    q = p // (n // 2)
    return (1 - q) * (2 * p) + q * (2 * (n - 1 - p) + 1)


def remote(src, dst, send, recv, dev):
    return pltpu.make_async_remote_copy(
        src_ref=src, dst_ref=dst, send_sem=send, recv_sem=recv, device_id=dev, device_id_type=MESH
    )


def places():
    d, c = lax.axis_index("dp"), lax.axis_index("ctx")
    core = d % 2
    return d, c, core, d + 1 - 2 * core, (d + 2) % 4


def greet(n):
    d, c, _, _, _ = places()
    barrier = pltpu.get_barrier_semaphore()
    n_dp = lax.axis_size("dp")
    for k in range(1, n_dp):
        pl.semaphore_signal(barrier, inc=1, device_id=((d + k) % n_dp, c), device_id_type=MESH)
    for k in range(1, n):
        pl.semaphore_signal(barrier, inc=1, device_id=(d, (c + k) % n), device_id_type=MESH)


def met(n):
    pl.semaphore_wait(pltpu.get_barrier_semaphore(), n + lax.axis_size("dp") - 2)


def steps(lo, hi, step):
    if isinstance(lo, int) and isinstance(hi, int) and hi - lo <= 4:
        for s in range(lo, hi):
            step(s)
    elif not (isinstance(lo, int) and isinstance(hi, int) and hi <= lo):
        lax.fori_loop(lo, hi, lambda s, _: (step(s), _)[1], 0)


class GatherRing:
    def __init__(self, n, slot, half, send, recv):
        self.n, self.h, self.slot, self.half, self.send, self.recv = n, n // 2, slot, half, send, recv
        self.d, c, _, _, _ = places()
        self.r = ring_place(c, n)

    def copy(self, s, i, arriving=False):
        way = 1 - 2 * i
        last = isinstance(s, int) and s == self.h - 1
        owner = ring_index(self.r - way * (s + (1 if arriving else 0)), self.n)
        ref = self.half(owner, i) if last else self.slot(owner)
        to = (self.d, ring_index(self.r + way, self.n))
        return remote(ref, ref, self.send.at[i, s], self.recv.at[i, s], to)

    def start(self, s):
        for i in range(2):
            self.copy(s, i).start()

    def arrive(self, s):
        for i in range(2):
            self.copy(s, i, True).wait_recv()

    def step(self, s):
        for i in range(2):
            self.copy(s - 1, i, True).wait_recv()
            self.copy(s, i).start()

    def last(self):
        self.step(self.h - 1)

    def drain(self):
        steps(0, self.h - 1, lambda s: [self.copy(s, i).wait_send() for i in range(2)])
        for i in range(2):
            self.copy(self.h - 1, i).wait_send()


class WideGather:
    def __init__(self, n, ref, half, send, recv, x_send, x_recv):
        self.d, self.c, _, _, self.xd = places()
        self.n, self.h, self.ref = n, n // 2, ref
        self.x_send, self.x_recv = x_send, x_recv
        self.ring = GatherRing(
            n, lambda o: ref.at[self.d, o], lambda o, w: half(ref.at[self.d, o], w), send, recv
        )

    def pass_on(self, i, owner, arriving=False):
        ref = self.ref.at[self.xd if arriving else self.d, owner]
        return remote(ref, ref, self.x_send.at[i], self.x_recv.at[i], (self.xd, self.c))

    def owner(self, s, i):
        return ring_index(self.ring.r - (1 - 2 * i) * (s + 1), self.n)

    def start(self, now):
        if now:
            self.pass_on(0, self.c).start()
        self.ring.start(0)

    def step(self, s, now):
        self.ring.step(s)
        if now:
            for i in range(2):
                self.pass_on(2 * s - 1 + i, self.owner(s - 1, i)).start()

    def finish(self, now):
        self.ring.arrive(self.h - 1)
        if now:
            self.pass_on(self.n - 1, self.owner(self.h - 1, 0)).start()
        else:
            self.passed(lambda i, o: self.pass_on(i, o).start())

    def passed(self, wait):
        wait(0, self.c)
        steps(0, self.h - 1, lambda s: [wait(1 + 2 * s + i, self.owner(s, i)) for i in range(2)])
        wait(self.n - 1, self.owner(self.h - 1, 0))

    def arrive(self):
        self.passed(lambda i, o: self.pass_on(i, o, True).wait_recv())

    def drain(self):
        self.ring.drain()
        self.passed(lambda i, o: self.pass_on(i, o).wait_send())


class ScatterRing:
    def __init__(self, n, part, half, land, whole_of, half_of, send, recv):
        self.n, self.h, self.part, self.half = n, n // 2, part, half
        self.land, self.whole_of, self.half_of = land, whole_of, half_of
        self.send, self.recv = send, recv
        self.d, c, _, _, _ = places()
        self.c, self.r = c, ring_place(c, n)

    def copy(self, s, i):
        way = 1 - 2 * i
        to = (self.d, ring_index(self.r + way, self.n))
        first = isinstance(s, int) and s == 0
        if first:
            owner = ring_index(self.r + way * self.h, self.n)
            src, dst = self.half(owner, i), self.half_of(self.land.at[i, 0], i)
        else:
            src, dst = self.land.at[i, s - 1], self.land.at[i, s]
        return remote(src, dst, self.send.at[i, s], self.recv.at[i, s], to)

    def start(self):
        for i in range(2):
            self.copy(0, i).start()

    def step(self, s):
        first = isinstance(s, int) and s == 1
        for i in range(2):
            way = 1 - 2 * i
            self.copy(s - 1, i).wait_recv()
            owner = ring_index(self.r + way * (self.h - s), self.n)
            held = self.land.at[i, s - 1]
            if first:
                mine = self.half_of(held, i)
                mine[...] = (mine[...].astype(F32) + self.half(owner, i)[...].astype(F32)).astype(BF)
                self.half_of(held, 1 - i)[...] = self.half(owner, 1 - i)[...]
            else:
                held[...] = (held[...].astype(F32) + self.part(owner)[...].astype(F32)).astype(BF)
            self.copy(s, i).start()

    def rest(self, lo, hi):
        if lo == 1 and hi > 1:
            self.step(1)
            lo = 2
        steps(lo, hi, self.step)

    def result(self):
        for i in range(2):
            self.copy(self.h - 1, i).wait_recv()
        out = self.part(self.c)[...].astype(F32)
        for i in range(2):
            out = out + self.land[i, self.h - 1].astype(F32)
        return out

    def drain(self):
        for i in range(2):
            self.copy(0, i).wait_send()
        steps(1, self.h, lambda s: [self.copy(s, i).wait_send() for i in range(2)])


class Spread:
    def __init__(self, ref, send, recv):
        d, c, _, cd, xd = places()
        self.copies = [
            remote(ref.at[d], ref.at[d], send.at[0], recv.at[0], (cd, c)),
            remote(ref.at[d], ref.at[d], send.at[1], recv.at[1], (xd, c)),
            remote(ref.at[xd], ref.at[xd], send.at[2], recv.at[2], (cd, c)),
        ]

    def start(self):
        self.copies[1].start()
        self.copies[0].start()

    def forward(self):
        self.copies[1].wait_recv()
        self.copies[2].start()

    def finish(self):
        self.copies[0].wait_recv()
        self.copies[2].wait_recv()
        for copy in self.copies:
            copy.wait_send()


def blocks(count, step, state):
    if count <= 8:
        for j in range(count):
            state = step(j, state)
        return state
    return lax.fori_loop(0, count, step, state)


def lane_block(j, size):
    if isinstance(j, int):
        return pl.ds(j * size, size)
    return pl.ds(pl.multiple_of(j * size, size), size)


def rope(b, cosine, sine, ranks):
    parts = []
    half = DH // 2
    for r in range(ranks):
        u1 = b[r * DH : r * DH + half]
        u2 = b[r * DH + half : (r + 1) * DH]
        parts += [u1 * cosine - u2 * sine, u2 * cosine + u1 * sine]
    return jnp.concatenate(parts, axis=0)


def rope_back(v, cosine, sine, ranks):
    return rope(v, cosine, -sine, ranks)


def pre_part(x, g1, w, cosine, sine, nt_ref, q_ref, p_ref, a_ref, b_ref):
    r1 = lax.rsqrt(jnp.mean(x * x, axis=-1, keepdims=True) + EPS)
    n = (x * r1 * g1).astype(BF)
    nt_ref[...] = n.T
    ft = nn(n, w).T
    a = ft[:AQ]
    b = rope(ft[AQ : AQ + BQ], cosine, sine, RQ)
    for i in range(AQ):
        a_ref[i] = a[i : i + 1]
    b_ref[...] = b
    k0 = AQ + BQ
    bk = rope(ft[k0 + AK : k0 + AK + BK], cosine, sine, RKV)
    p_ref[...] = jnp.concatenate(
        [ft[k0 : k0 + AK], bk, ft[k0 + KEY_ROWS : k0 + PACK]], axis=0
    ).astype(BF)
    for h in range(H):
        acc = a[h : h + 1] * b[:DH]
        for r in range(1, RQ):
            acc = acc + a[r * H + h : r * H + h + 1] * b[r * DH : (r + 1) * DH]
        q_ref[h * DH : (h + 1) * DH, :] = (acc * (1.0 / RQ)).astype(BF)


def vectors(kv_ref, side, r, lanes):
    first = side * KEY_ROWS + AK + r * DH
    return kv_ref[first : first + DH, lanes].astype(F32)


def expand_pair(ka, kv_ref, side, p, lanes):
    rows = []
    for hh in range(2):
        acc = 0.0
        for r in range(RKV):
            acc = acc + ka[side * AK + r * H + 2 * p + hh] * vectors(kv_ref, side, r, lanes)
        rows.append(acc * (1.0 / RKV))
    return jnp.concatenate(rows, axis=0)


def unpack(kv_ref, ka, lanes):
    for side in range(2):
        first = side * KEY_ROWS
        a = kv_ref[first : first + AK, lanes].astype(F32)
        for i in range(AK):
            ka[side * AK + i] = a[i : i + 1]


def unrolled(pair, some):
    def group(q, carry):
        for u in range(some):
            pair(q * some + u, carry)
        return carry

    lax.fori_loop(0, H // 2 // some, group, 0)


def when(condition, run):
    if isinstance(condition, bool):
        if condition:
            run()
    else:
        pl.when(condition)(run)


def diagonal(pair):
    zero = jnp.zeros((DH, pair.shape[1]), pair.dtype)
    left = jnp.concatenate([pair[:DH], zero], axis=0)
    right = jnp.concatenate([zero, pair[DH:]], axis=0)
    return jnp.concatenate([left, right], axis=1)


def undiagonal(wide):
    t = wide.shape[1] // 2
    return jnp.concatenate([wide[:DH, :t], wide[DH:, t:]], axis=0)


def attend_part(
    nblk, arrive, len_ref, q_ref, kv_ref, at_ref, af_ref, inv_ref, p_out, pbuf, ka, bias, qd_ref,
    num_ref, tot_ref,
):
    t = q_ref.shape[1]
    c = lax.axis_index("ctx")
    tpos = c * t + lax.broadcasted_iota(jnp.int32, (1, t), 1)
    start = jnp.zeros((1, t), jnp.int32)
    run = jnp.int32(0)
    for j in range(len_ref.shape[1]):
        start = jnp.where(tpos >= run, run, start)
        run = run + len_ref[0, j]

    def prepare(p, carry):
        rows = pl.ds(pl.multiple_of(p * 2 * DH, 2 * DH), 2 * DH)
        qd_ref[p] = diagonal(q_ref[rows, :])
        return carry

    lax.fori_loop(0, H // 2, prepare, 0)
    num_ref[...] = jnp.zeros_like(num_ref)
    tot_ref[...] = jnp.zeros_like(tot_ref)

    def block(i, carry):
        j = nblk - 1 - i
        when(i > 0, lambda: arrive(i))
        when(i > 1, lambda: p_out(j + 2).wait())
        lanes = lane_block(j, t)
        unpack(kv_ref, ka, lanes)
        spos = (c - i) * t + lax.broadcasted_iota(jnp.int32, (t, t), 0)
        ok = (spos >= start) & (spos <= tpos)
        bias[...] = jnp.where(ok, 0.0, NEG)

        def pair(p, carry):
            k = expand_pair(ka, kv_ref, 0, p, lanes).T.astype(BF)
            v = expand_pair(ka, kv_ref, 1, p, lanes).astype(BF)
            b = bias[...]
            s = nn(k, qd_ref[p]) * (LOG2E * DH**-0.5) + jnp.concatenate([b, b], axis=1)
            e = jnp.exp2(s)
            tot_ref[p] += jnp.sum(e, axis=0, keepdims=True)
            pb = e.astype(BF)
            pbuf[j % 2, p] = pb
            num_ref[p] += nn(v, pb)
            return carry

        unrolled(pair, 4)
        p_out(j).start()
        return carry

    blocks(nblk, block, 0)

    def finish(p, carry):
        rows = pl.ds(pl.multiple_of(p * 2 * DH, 2 * DH), 2 * DH)
        inv = 1.0 / tot_ref[p]
        af = undiagonal(num_ref[p] * inv)
        af_ref[rows, :] = af
        at_ref[rows, :] = af.astype(BF)
        inv_ref[p] = inv
        return carry

    lax.fori_loop(0, H // 2, finish, 0)
    for j in range(2):
        p_out(j).wait()


def attend_back_part(
    nblk, serve, ship, da_ref, af_ref, inv_ref, p_copy, pbuf, q_ref, kv_ref, a_ref, b_ref,
    cos_ref, sin_ref, dq_ref, ka, dka, dqa, db, dkv, qd_ref, dn_ref, dtot_ref, dqs,
):
    t = q_ref.shape[1]

    def factor_back(dwide, side, p, lanes):
        for hh in range(2):
            d = dwide[hh * DH : (hh + 1) * DH] * (1.0 / RKV)
            for r in range(RKV):
                row = side * AK + r * H + 2 * p + hh
                first = side * KEY_ROWS + AK + r * DH
                b = vectors(kv_ref, side, r, lanes)
                dka[row] = jnp.sum(d * b, axis=0, keepdims=True)
                dkv[first : first + DH, :] += d * ka[row]

    def prepare(p, carry):
        rows = pl.ds(pl.multiple_of(p * 2 * DH, 2 * DH), 2 * DH)
        inv = inv_ref[p]
        dd = diagonal(da_ref[rows, :])
        dn_ref[p] = (dd * inv).astype(BF)
        dtot_ref[p] = -jnp.sum(dd * diagonal(af_ref[rows, :]), axis=0, keepdims=True) * inv
        qd_ref[p] = diagonal(q_ref[rows, :])
        return carry

    lax.fori_loop(0, H // 2, prepare, 0)
    dqs[...] = jnp.zeros_like(dqs)

    def block(j, carry):
        when(j + 1 < nblk, lambda: p_copy(j + 1).start())
        p_copy(j).wait()
        lanes = lane_block(j, t)
        unpack(kv_ref, ka, lanes)
        for side in range(2):
            first = side * KEY_ROWS + AK
            dkv[first : first + BK, :] = jnp.zeros((BK, t), F32)

        def pair(p, carry):
            rows = pl.ds(pl.multiple_of(p * 2 * DH, 2 * DH), 2 * DH)
            k = expand_pair(ka, kv_ref, 0, p, lanes).astype(BF)
            v = expand_pair(ka, kv_ref, 1, p, lanes).T.astype(BF)
            pb = pbuf[j % 2, p]
            dn = dn_ref[p]
            ds = (pb.astype(F32) * (nn(v, dn) + dtot_ref[p])).astype(BF)
            dqs[rows, :] += undiagonal(nn(k, ds))
            factor_back(nt(qd_ref[p], ds) * (DH**-0.5), 0, p, lanes)
            factor_back(nt(dn, pb), 1, p, lanes)
            return carry

        unrolled(pair, 4)
        for side in range(2):
            for i in range(AK):
                dkv[side * KEY_ROWS + i : side * KEY_ROWS + i + 1, :] = dka[side * AK + i]
        ship(j)
        serve(j)
        return carry

    blocks(nblk, block, 0)
    db[...] = jnp.zeros_like(db)

    def pair_q(p, carry):
        rows = pl.ds(pl.multiple_of(p * 2 * DH, 2 * DH), 2 * DH)
        dq = dqs[rows, :] * (DH**-0.5 / RQ)
        for hh in range(2):
            d = dq[hh * DH : (hh + 1) * DH]
            for r in range(RQ):
                row = r * H + 2 * p + hh
                dqa[row] = jnp.sum(d * b_ref[r * DH : (r + 1) * DH, :], axis=0, keepdims=True)
                db[r * DH : (r + 1) * DH, :] += d * a_ref[row]
        return carry

    lax.fori_loop(0, H // 2, pair_q, 0)
    for i in range(AQ):
        dq_ref[i : i + 1, :] = dqa[i]
    dq_ref[AQ : AQ + BQ, :] = rope_back(db[...], cos_ref[...], sin_ref[...], RQ)


def gain_rows(w):
    first = FPAD - 128
    gains = w[:, first:].astype(F32).T
    return gains[FDIM - first : FDIM - first + 1], gains[FDIM - first + 1 : FDIM - first + 2]


def lane_half(ref, w):
    return ref.at[:, :512] if w == 0 else ref.at[:, 512:]


class PairScatter:
    def __init__(self, n, part, held, land, own, send, recv, ring_send, ring_recv, x_first=None):
        d, c, core, cd, xd = places()
        self.x_first = x_first
        self.core, self.x, self.part, self.held, self.own = core, d // 2, part, held, own
        self.swaps = [
            remote(part.at[2 * xx + 1 - core], held.at[xx], send.at[xx], recv.at[xx], (cd, c))
            for xx in range(2)
        ]
        if x_first is not None:
            self.end = remote(held.at[1 - self.x], x_first, send.at[2], recv.at[2], (xd, c))
            self.ring = ScatterRing(
                n, lambda o: x_first.at[o], lambda o, w: lane_half(x_first.at[o], w), land,
                None, lane_half, ring_send, ring_recv,
            )
            return
        self.end = remote(own.at[1 - self.x], own.at[2], send.at[2], recv.at[2], (xd, c))
        self.ring = ScatterRing(
            n, lambda o: held.at[:, o], lambda o, w: held.at[w, o], land,
            None, lambda ref, w: ref.at[w], ring_send, ring_recv,
        )

    def start(self):
        for swap in self.swaps:
            swap.start()

    def enter(self):
        for xx in range(2):
            self.swaps[xx].wait_recv()
            mine = self.part[2 * xx + self.core].astype(F32)
            self.held[xx] = (self.held[xx].astype(F32) + mine).astype(BF)
        if self.x_first is None:
            self.ring.start()
        else:
            self.end.start()

    def across(self):
        self.end.wait_recv()
        total = self.x_first[...].astype(F32) + self.held[self.x].astype(F32)
        self.x_first[...] = total.astype(BF)
        self.ring.start()

    def leave(self):
        total = self.ring.result()
        for xx in range(2):
            self.own[xx] = total[xx].astype(BF)
        self.end.start()

    def result(self):
        self.end.wait_recv()
        return self.own[self.x].astype(F32) + self.own[2].astype(F32)

    def drain(self):
        for copy in self.swaps + [self.end]:
            copy.wait_send()
        self.ring.drain()


def block_kernel(
    n, nblk,
    len_ref, x_ref, cos_ref, sin_ref, fw_ref, g1_ref, g2_ref, ow_ref, gw_ref, uw_ref, dw_ref, cot_in,
    y_ref, dx_ref, fac_ref, gain1_ref, gain2_ref, wo_ref, gate_ref, up_ref, wd_ref, p_ref,
    nt_ref, q_ref, a_ref, b_ref, kv_ref, at_ref, af_ref, inv_ref, pbuf,
    fac, wo, gu, wd, nm, cot, mid_ref, dn_in, out_in, gu_part, wd_part,
    kv_land, gu_land, wd_land, gu_own, da_ref, dq_ref, dmid_ref, dp_land,
    fac_part, wo_part, fac_held, wo_held, fac_land, wo_land, fac_own, wo_own,
    own_sem, near_send, near_recv, ring_send, ring_recv, kv_send, kv_recv, sp_send, sp_recv,
    dkv_send, dkv_recv, end_send, end_recv, dp_send, dp_recv, pair_send, pair_recv, p_sem, own_dkv,
    gu_in, gu_ref, x_send, x_recv,
):
    d, c, core, cd, xd = places()
    t = x_ref.shape[0]
    n_dp = 4
    rows, ffq = gu_in.shape[1], gu_in.shape[2] // 2
    greet(n)
    keep_cot = pltpu.make_async_copy(cot_in, cot.at[d], own_sem.at[4])
    keep_cot.start()
    tail = FPAD - 128
    lane = lax.broadcasted_iota(jnp.int32, (rows, 128), 1)
    diag = lax.broadcasted_iota(jnp.int32, (rows, rows), 0) == lax.broadcasted_iota(
        jnp.int32, (rows, rows), 1
    )

    def column(ref):
        return jnp.sum(jnp.where(diag, ref[...], 0.0), axis=1, keepdims=True)

    gains = jnp.where(lane == FDIM - tail, column(g1_ref), 0.0)
    gains = jnp.where(lane == FDIM + 1 - tail, column(g2_ref), gains)
    fac[d, c, :, :tail] = fw_ref[:, :tail].astype(BF)
    fac[d, c, :, tail:] = gains.astype(BF)
    fac[d, c, :, tail:FDIM] = fw_ref[:, tail:].astype(BF)
    wo[d, c] = ow_ref[...].astype(BF)
    wd[c] = dw_ref[...].astype(BF)
    for dd in range(n_dp):
        for side, ref in enumerate((gw_ref, uw_ref)):
            gu_in[dd, :, side * ffq : (side + 1) * ffq] = ref[:, dd * ffq : (dd + 1) * ffq].astype(BF)
    keep_gu = pltpu.make_async_copy(gu_in.at[d], gu.at[d, c], own_sem.at[2])
    keep_gu.start()
    for k in range(1, nblk):
        @pl.when(c - k < 0)
        def _():
            kv_ref[:, (nblk - 1 - k) * t : (nblk - k) * t] = jnp.zeros((PACK, t), BF)
    met(n)

    fo = WideGather(n, fac, lane_half, ring_send.at[0], ring_recv.at[0], x_send.at[0], x_recv.at[0])
    oo = WideGather(n, wo, lane_half, ring_send.at[1], ring_recv.at[1], x_send.at[1], x_recv.at[1])
    cut = -(-dw_ref.shape[0] // 16) * 8
    gr = GatherRing(
        n, lambda o: gu.at[:, o], lambda o, w: gu.at[2 * w : 2 * w + 2, o],
        ring_send.at[4], ring_recv.at[4],
    )
    dr = GatherRing(
        n, lambda o: wd.at[o], lambda o, w: wd.at[o, :cut] if w == 0 else wd.at[o, cut:],
        ring_send.at[5], ring_recv.at[5],
    )
    small, large = (fo, oo), (gr, dr)
    fo.start(True)
    oo.start(False)
    a2a = []
    for k in range(1, n_dp):
        to = (d + k) % n_dp
        a2a.append(
            (
                remote(gu_in.at[to], gu.at[d, c], near_send.at[1 + k], near_recv.at[1 + k], (to, c)),
                remote(
                    gu_in.at[to], gu.at[(d + n_dp - k) % n_dp, c],
                    near_send.at[1 + k], near_recv.at[1 + k], (to, c),
                ),
            )
        )
        a2a[-1][0].start()
    cots = Spread(cot, sp_send.at[0], sp_recv.at[0])
    nms = Spread(nm, sp_send.at[1], sp_recv.at[1])
    steps(1, n // 2 - 1, lambda s: (fo.step(s, True), oo.step(s, False)))
    fo.step(n // 2 - 1, True)
    oo.step(n // 2 - 1, False)
    keep_gu.wait()
    for _, arrival in a2a:
        arrival.wait_recv()
    gr.start(0)

    def core_swap(ref, i, dd, da):
        return (
            remote(ref.at[dd], ref.at[dd], near_send.at[5 + i], near_recv.at[5 + i], (cd, c)),
            remote(ref.at[da], ref.at[da], near_send.at[5 + i], near_recv.at[5 + i], (cd, c)),
        )

    near = []

    def swap(i, ref, dd, da):
        near.append(core_swap(ref, i, dd, da))
        near[-1][0].start()

    fo.finish(True)
    swap(0, fac, d, cd)
    oo.finish(False)
    swap(2, wo, d, cd)
    fo.arrive()
    swap(1, fac, xd, (cd + 2) % 4)
    keep_cot.wait()
    cots.start()
    for _, arrival in (near[0], near[2]):
        arrival.wait_recv()

    width = x_ref.shape[1]
    x = x_ref[...].astype(F32)
    w = fac[...].reshape(width, FPAD)
    g1, g2 = gain_rows(w)
    own_kv = kv_ref.at[:, (nblk - 1) * t : nblk * t]
    pre_part(x, g1, w, cos_ref[...], sin_ref[...], nt_ref, q_ref, own_kv, a_ref, b_ref)

    def kv_copy(k):
        dst = kv_ref.at[:, lane_block(nblk - 1 - k, t)]
        return remote(own_kv, dst, kv_send.at[k - 1], kv_recv.at[k - 1], (d, (c + k) % n))

    for k in range(1, nblk):
        @pl.when(c + k < n)
        def _():
            kv_copy(k).start()
    dr.start(0)
    oo.arrive()
    swap(3, wo, xd, (cd + 2) % 4)
    full = n // 2 - 1
    middle_step = 1 + full // 2

    def arrive(i):
        @pl.when(c - i >= 0)
        def _():
            kv_copy(i).wait_recv()

        when(i == 2, lambda: steps(1, middle_step, gr.step))


    def p_out(j):
        return pltpu.make_async_copy(pbuf.at[j % 2], p_ref.at[j], p_sem.at[j % 2])

    pl.run_scoped(
        functools.partial(
            attend_part, nblk, arrive, len_ref, q_ref, kv_ref, at_ref, af_ref, inv_ref, p_out, pbuf
        ),
        pltpu.VMEM((2 * AK, 1, t), F32),
        pltpu.VMEM((t, t), F32),
        pltpu.VMEM((H // 2, 2 * DH, 2 * t), BF),
        pltpu.VMEM((H // 2, 2 * DH, 2 * t), F32),
        pltpu.VMEM((H // 2, 1, 2 * t), F32),
    )

    steps(1, middle_step, dr.step)
    for _, arrival in (near[1], near[3]):
        arrival.wait_recv()
    middle = x + nn(at_ref[...].T, wo[...].reshape(width, width))
    mid_ref[...] = middle
    r2 = lax.rsqrt(jnp.mean(middle * middle, axis=-1, keepdims=True) + EPS)
    nm[d] = (middle * r2 * g2).astype(BF)
    nms.start()
    cots.forward()
    steps(middle_step, full, lambda s: [one.step(s) for one in large])
    nms.forward()
    nms.finish()
    cots.finish()
    for one in large:
        one.last()
    for one in large:
        one.arrive(n // 2 - 1)

    x_at = d // 2
    parts = (dn_in, out_in)
    first = []
    for i, part in enumerate(parts):
        for j, xx in enumerate((1 - x_at, x_at)):
            first.append(
                remote(
                    part.at[2 * xx + 1 - core], dp_land.at[i, j],
                    dp_send.at[i, j], dp_recv.at[i, j], (cd, c),
                )
            )

    cut = -(-wd_part.shape[1] // 16) * 8

    def wd_half(ref, w):
        return ref.at[:cut] if w == 0 else ref.at[cut:]

    gs = ScatterRing(
        n, lambda o: gu_part.at[:, o], lambda o, w: gu_part.at[2 * w : 2 * w + 2, o], gu_land,
        None, lambda ref, w: ref.at[2 * w : 2 * w + 2], ring_send.at[6], ring_recv.at[6],
    )
    ds_ = ScatterRing(
        n, lambda o: wd_part.at[o], lambda o, w: wd_half(wd_part.at[o], w), wd_land,
        None, wd_half, ring_send.at[7], ring_recv.at[7],
    )
    scatter = (gs, ds_)
    fs = PairScatter(
        n, fac_part, fac_held, fac_land, fac_own, pair_send.at[0], pair_recv.at[0],
        ring_send.at[8], ring_recv.at[8],
    )
    ws = PairScatter(
        n, wo_part, wo_held, wo_land, wo_own, pair_send.at[1], pair_recv.at[1],
        ring_send.at[9], ring_recv.at[9], wo_own,
    )
    h = n // 2

    def advance(s):
        for one in scatter:
            one.step(s)

    points = 2

    def serve(k):
        steps(2 + -(-(k - 1) * (h - 2) // points), 2 + -(-k * (h - 2) // points), advance)

    def feed(both_ff, dh, hid, dgu):
        def matrix():
            return gu[...].reshape(width, 2 * ffq)

        def pair_rows(i, carry):
            xx = i * x_at + (1 - i) * (1 - x_at)
            two = pl.ds(2 * xx, 2)
            both = 2 * t
            both_ff[...] = nn(nm[two].reshape(both, width), matrix())
            dh[...] = nt(cot[two].reshape(both, width), wd[...].reshape(ffq, width))
            base = pl.multiple_of(xx * both, both)

            def rows_of(k, carry):
                some = pl.ds(pl.multiple_of(k * 32, 32), 32)
                to = pl.ds(pl.multiple_of(base + k * 32, 32), 32)
                v, u, g = both_ff[some, :ffq], both_ff[some, ffq:], dh[some, :]
                sig, act = silu_parts(v)
                hid[to, :] = (act * u).astype(BF)
                dgu[to, :ffq] = (g * u * sig * (1.0 + v * (1.0 - sig))).astype(BF)
                dgu[to, ffq:] = (g * act).astype(BF)
                return carry

            lax.fori_loop(0, both // 32, rows_of, 0)
            return carry

        def ends(i):
            xx = i * x_at + (1 - i) * (1 - x_at)
            return pl.ds(2 * xx, 2), pl.ds(pl.multiple_of(xx * 2 * t, 2 * t), 2 * t)

        def norm_back(i, carry):
            two, these = ends(i)
            dn_in[two] = nt(dgu[these, :], matrix()).astype(BF).reshape(2, t, width)

            @pl.when(i == 0)
            def _():
                first[0].start()

            return carry

        def down(i, carry):
            two, these = ends(i)
            out_in[two] = nn(hid[these, :], wd[...].reshape(ffq, width)).astype(BF).reshape(2, t, width)

            @pl.when(i == 0)
            def _():
                first[2].start()

            return carry

        def onward(i, part):
            first[2 * i].wait_recv()
            dp_land[i, 0] = (dp_land[i, 0].astype(F32) + part[xd].astype(F32)).astype(BF)
            dp_next(i).start()

        lax.fori_loop(0, 2, pair_rows, 0)

        def tn(a, b):
            return lax.dot_general(a, b, (((0,), (0,)), ((), ())), preferred_element_type=F32)

        quarter = width // n_dp

        def down_columns(j, carry):
            lanes = pl.ds(pl.multiple_of(j * quarter, quarter), quarter)
            some = cot[:, :, lanes].reshape(n_dp * t, quarter)
            wd_part[:, :, lanes] = tn(hid[...], some).astype(BF).reshape(wd_part.shape[:2] + (quarter,))
            return carry

        def columns(j, carry):
            lanes = pl.ds(pl.multiple_of(j * quarter, quarter), quarter)
            some = nm[:, :, lanes].reshape(n_dp * t, quarter)
            gu_part[j] = tn(some, dgu[...]).astype(BF).reshape(gu_part.shape[1:])
            return carry

        lax.fori_loop(0, n_dp, down_columns, 0)
        ds_.start()
        lax.fori_loop(0, n_dp, columns, 0)
        gs.start()
        lax.fori_loop(0, 2, norm_back, 0)
        first[1].start()
        onward(0, dn_in)
        lax.fori_loop(0, 2, down, 0)
        first[3].start()
        onward(1, out_in)
        advance(1)

    def dp_next(i):
        return remote(dp_land.at[i, 0], dp_land.at[i, 2], dp_send.at[i, 2], dp_recv.at[i, 2], (xd, c))

    pl.run_scoped(
        feed,
        pltpu.VMEM((2 * t, 2 * ffq), F32),
        pltpu.VMEM((2 * t, ffq), F32),
        pltpu.VMEM((n_dp * t, ffq), BF),
        pltpu.VMEM((n_dp * t, 2 * ffq), BF),
    )
    second = [dp_next(i) for i in range(2)]
    for i in range(2):
        first[2 * i + 1].wait_recv()
    second[0].wait_recv()
    middle = mid_ref[...]
    dn = dn_in[d].astype(F32) + dp_land[0, 1].astype(F32) + dp_land[0, 2].astype(F32)
    second_part = jnp.sum(dn * middle * r2, axis=0, keepdims=True)
    u2 = dn * g2
    d_middle = (
        cot_in[...].astype(F32)
        + r2 * u2
        - middle * (r2 * r2 * r2 * jnp.mean(u2 * middle, axis=-1, keepdims=True))
    )
    dmid_ref[...] = d_middle
    serve(1)
    d_branch = d_middle.astype(BF)
    wo_part[...] = nn(at_ref[...], d_branch).astype(BF).reshape(wo_part.shape)
    ws.start()
    da_ref[...] = nt(wo[...].reshape(width, width), d_branch)
    second[1].wait_recv()
    y_ref[...] = (
        mid_ref[...]
        + (out_in[d].astype(F32) + dp_land[1, 1].astype(F32) + dp_land[1, 2].astype(F32))
    ).astype(BF)
    ws.enter()
    def serve_block(j):
        when(j == nblk - 1, lambda: serve(2))

    def p_copy(j):
        return pltpu.make_async_copy(p_ref.at[j], pbuf.at[j % 2], p_sem.at[j % 2])

    p_copy(0).start()

    def attention_back(dkv16, dkv, *scratch):
        def dkv_copy(k):
            return remote(
                dkv16.at[k - 1], kv_land.at[k - 1], dkv_send.at[k - 1], dkv_recv.at[k - 1],
                (d, (c + n - k) % n),
            )

        def ship(j):
            k = nblk - 1 - j

            def away():
                dkv16[k - 1] = dkv[...].astype(BF)

                @pl.when(c - k >= 0)
                def _():
                    dkv_copy(k).start()

            def home():
                own_dkv[...] = dkv[...]

            when(k > 0, away)
            when(k == 0, home)

        ka, dka, dqa, db, qd, dn, dtot, dqs = scratch
        attend_back_part(
            nblk, serve_block, ship, da_ref, af_ref, inv_ref, p_copy, pbuf, q_ref, kv_ref, a_ref,
            b_ref, cos_ref, sin_ref, dq_ref, ka, dka, dqa, db, dkv, qd, dn, dtot, dqs,
        )
        for k in range(1, nblk):
            @pl.when(c + k < n)
            def _():
                dkv_copy(k).wait_recv()
                own_dkv[...] += kv_land[k - 1].astype(F32)
        for k in range(1, nblk):
            @pl.when(c - k >= 0)
            def _():
                dkv_copy(k).wait_send()

    pl.run_scoped(
        attention_back,
        pltpu.VMEM((nblk - 1, PACK, t), BF),
        pltpu.VMEM((PACK, t), F32),
        pltpu.VMEM((2 * AK, 1, t), F32),
        pltpu.VMEM((2 * AK, 1, t), F32),
        pltpu.VMEM((AQ, 1, t), F32),
        pltpu.VMEM((BQ, t), F32),
        pltpu.VMEM((H // 2, 2 * DH, 2 * t), BF),
        pltpu.VMEM((H // 2, 2 * DH, 2 * t), BF),
        pltpu.VMEM((H // 2, 1, 2 * t), F32),
        pltpu.VMEM((H * DH, t), F32),
    )
    ws.across()
    dp = own_dkv[...]
    d_bk = rope_back(dp[AK : AK + BK], cos_ref[...], sin_ref[...], RKV)
    d_fac_t = jnp.concatenate(
        [dq_ref[...], dp[:AK], d_bk, dp[KEY_ROWS:], jnp.zeros((FPAD - FDIM, t), F32)], axis=0
    ).astype(BF)
    x = x_ref[...].astype(F32)
    r1 = lax.rsqrt(jnp.mean(x * x, axis=-1, keepdims=True) + EPS)
    d_norm_in = nt(d_fac_t.T, w)
    first_part = jnp.sum(d_norm_in * x * r1, axis=0, keepdims=True)
    tail = FPAD - 128
    gains = jnp.concatenate(
        [jnp.zeros((FDIM - tail, width), F32), first_part, second_part,
         jnp.zeros((FPAD - FDIM - 2, width), F32)], axis=0).T
    product = nt(nt_ref[...], d_fac_t)
    shape = fac_part.shape[:3]
    fac_part[:, :, :, :tail] = product[:, :tail].astype(BF).reshape(shape + (tail,))
    fac_part[:, :, :, tail:] = (product[:, tail:] + gains).astype(BF).reshape(shape + (128,))
    fs.start()
    u1 = d_norm_in * g1
    dx_ref[...] = (
        dmid_ref[...] + r1 * u1 - x * (r1 * r1 * r1 * jnp.mean(u1 * x, axis=-1, keepdims=True))
    ).astype(BF)
    ws.ring.step(1)
    fs.enter()
    gu_own[...] = gs.result().astype(BF)
    keep = pltpu.make_async_copy(gu_own.at[d], gu_ref.at[d], own_sem.at[0])
    keep.start()
    last = []
    for k in range(1, n_dp):
        to = (d + k) % n_dp
        last.append(
            (
                remote(gu_own.at[to], gu_ref.at[d], end_send.at[k - 1], end_recv.at[k - 1], (to, c)),
                remote(
                    gu_own.at[to], gu_ref.at[(d + n_dp - k) % n_dp],
                    end_send.at[k - 1], end_recv.at[k - 1], (to, c),
                ),
            )
        )
        last[-1][0].start()
    steps(2, h, ws.ring.step)
    fs.ring.step(1)
    wd_ref[...] = ds_.result()
    steps(2, h, fs.ring.step)
    wo_ref[...] = ws.ring.result()
    fs.leave()
    for out, arrival in last:
        arrival.wait_recv()
        out.wait_send()
    keep.wait()
    for dd in range(n_dp):
        lanes = slice(dd * ffq, (dd + 1) * ffq)
        gate_ref[:, lanes] = gu_ref[dd, :, :ffq].astype(F32)
        up_ref[:, lanes] = gu_ref[dd, :, ffq:].astype(F32)
    total = fs.result()
    fac_ref[...] = total[:, :FDIM]
    for i, ref in enumerate((gain1_ref, gain2_ref)):
        one = total[:, FDIM + i : FDIM + i + 1]
        ref[...] = jnp.sum(jnp.where(diag, one, 0.0), axis=0, keepdims=True)
    for copy in first + second:
        copy.wait_send()
    for one in scatter + (ws, fs):
        one.drain()
    for k in range(1, nblk):
        @pl.when(c + k < n)
        def _():
            kv_copy(k).wait_send()
    for out, _ in a2a + near:
        out.wait_send()
    for one in small + large:
        one.drain()


def emit_kernel(*refs):
    k = (len(refs) - 2) // 3
    ins, outs, bufs, sems = refs[:k], refs[k : 2 * k], refs[2 * k : 3 * k], refs[3 * k :]
    into = [pltpu.make_async_copy(a, b, sems[0].at[i]) for i, (a, b) in enumerate(zip(ins, bufs))]
    out = [pltpu.make_async_copy(a, b, sems[1].at[i]) for i, (a, b) in enumerate(zip(bufs, outs))]
    for copy in into:
        copy.start()
    for one, two in zip(into, out):
        one.wait()
        two.start()
    for copy in out:
        copy.wait()


def vmem(n):
    return [pl.BlockSpec(memory_space=pltpu.VMEM)] * n


def hbm(n):
    return [pl.BlockSpec(memory_space=pl.ANY)] * n


SMEM = pl.BlockSpec(memory_space=pltpu.SMEM)
DMA = pltpu.SemaphoreType.DMA


def talks(i):
    return pltpu.CompilerParams(
        collective_id=i, has_side_effects=True, vmem_limit_bytes=63 * 1024 * 1024
    )


def silu_parts(gate):
    s = jax.nn.sigmoid(gate)
    return s, gate * s


def body(
    tokens,
    doc_lengths,
    first_gain,
    factor_weights,
    output_weights,
    second_gain,
    gate_weights,
    up_weights,
    down_weights,
    cotangent,
):
    _, t, width = tokens.shape
    n_ctx, n_dp = lax.axis_size("ctx"), lax.axis_size("dp")
    n_all = n_ctx * n_dp
    both = ("dp", "ctx")
    length = t * n_ctx
    nblk = min(n_ctx, -(-(length // 2 - 1) // t) + 1)
    ff = gate_weights.shape[1]
    ffq = ff // n_dp
    rows = width // n_all
    c = lax.axis_index("ctx")

    h = n_ctx // 2

    half = DH // 2
    freq = 10000.0 ** (-(np.arange(half) * 2.0 / DH))
    pos = (c * t + jnp.arange(t, dtype=jnp.int32)).astype(F32)
    angles = jnp.asarray(freq, F32)[:, None] * pos[None, :]
    cosine, sine = jnp.cos(angles), jnp.sin(angles)

    x16 = tokens.reshape(t, width)
    cot_own = cotangent.reshape(t, width)
    sds = jax.ShapeDtypeStruct
    down_rows = down_weights.shape[0]
    outs = pl.pallas_call(
        functools.partial(block_kernel, n_ctx, nblk),
        out_shape=(
            sds((t, width), BF),
            sds((t, width), BF),
            sds((rows, FDIM), F32),
            sds((1, rows), F32),
            sds((1, rows), F32),
            sds((rows, width), F32),
            sds((rows, ff), F32),
            sds((rows, ff), F32),
            sds((down_rows, width), F32),
            sds((nblk, H // 2, t, 2 * t), BF),
        ),
        in_specs=[SMEM] + vmem(11),
        out_specs=tuple(vmem(9) + hbm(1)),
        scratch_shapes=[
            pltpu.VMEM((width, t), BF),
            pltpu.VMEM((H * DH, t), BF),
            pltpu.VMEM((AQ, 1, t), F32),
            pltpu.VMEM((BQ, t), F32),
            pltpu.VMEM((PACK, nblk * t), BF),
            pltpu.VMEM((H * DH, t), BF),
            pltpu.VMEM((H * DH, t), F32),
            pltpu.VMEM((H // 2, 1, 2 * t), F32),
            pltpu.VMEM((2, H // 2, t, 2 * t), BF),
            pltpu.VMEM((n_dp, n_ctx, rows, FPAD), BF),
            pltpu.VMEM((n_dp, n_ctx, rows, width), BF),
            pltpu.VMEM((n_dp, n_ctx, rows, 2 * ffq), BF),
            pltpu.VMEM((n_ctx, down_rows, width), BF),
            pltpu.VMEM((n_dp, t, width), BF),
            pltpu.VMEM((n_dp, t, width), BF),
            pltpu.VMEM((t, width), F32),
            pltpu.VMEM((n_dp, t, width), BF),
            pltpu.VMEM((n_dp, t, width), BF),
            pltpu.VMEM((n_dp, n_ctx, rows, 2 * ffq), BF),
            pltpu.VMEM((n_ctx, down_rows, width), BF),
            pltpu.VMEM((nblk - 1, PACK, t), BF),
            pltpu.VMEM((2, h, n_dp, rows, 2 * ffq), BF),
            pltpu.VMEM((2, h, down_rows, width), BF),
            pltpu.VMEM((n_dp, rows, 2 * ffq), BF),
            pltpu.VMEM((H * DH, t), F32),
            pltpu.VMEM((AQ + BQ, t), F32),
            pltpu.VMEM((t, width), F32),
            pltpu.VMEM((2, 3, t, width), BF),
            pltpu.VMEM((n_dp, n_ctx, rows, FPAD), BF),
            pltpu.VMEM((n_dp, n_ctx, rows, width), BF),
            pltpu.VMEM((2, n_ctx, rows, FPAD), BF),
            pltpu.VMEM((2, n_ctx, rows, width), BF),
            pltpu.VMEM((2, h, 2, rows, FPAD), BF),
            pltpu.VMEM((2, h, rows, width), BF),
            pltpu.VMEM((3, rows, FPAD), BF),
            pltpu.VMEM((n_ctx, rows, width), BF),
            DMA((5,)),
            DMA((9,)),
            DMA((9,)),
            DMA((10, 2, h)),
            DMA((10, 2, h)),
            DMA((nblk - 1,)),
            DMA((nblk - 1,)),
            DMA((2, 3)),
            DMA((2, 3)),
            DMA((nblk - 1,)),
            DMA((nblk - 1,)),
            DMA((3,)),
            DMA((3,)),
            DMA((2, 3)),
            DMA((2, 3)),
            DMA((2, 3)),
            DMA((2, 3)),
            DMA((2,)),
            pltpu.VMEM((PACK, t), F32),
            pltpu.VMEM((n_dp, rows, 2 * ffq), BF),
            pltpu.VMEM((n_dp, rows, 2 * ffq), BF),
            DMA((2, n_ctx)),
            DMA((2, n_ctx)),
        ],
        compiler_params=talks(0),
        name="block",
    )(doc_lengths, x16, cosine, sine, factor_weights, first_gain.reshape(1, rows),
      second_gain.reshape(1, rows), output_weights, gate_weights, up_weights, down_weights, cot_own)
    outs = outs[:9]
    y, dx, fac_own, gain1, gain2, out_own, gate_own, up_own, down_own = pl.pallas_call(
        emit_kernel,
        out_shape=tuple(sds(o.shape, o.dtype) for o in outs),
        in_specs=hbm(9),
        out_specs=tuple(hbm(9)),
        scratch_shapes=[pltpu.VMEM(o.shape, o.dtype) for o in outs] + [DMA((9,)), DMA((9,))],
        name="emit",
    )(*outs)
    return (
        y.reshape(1, t, width),
        dx.reshape(1, t, width),
        gain1.reshape(rows),
        fac_own,
        out_own,
        gain2.reshape(rows),
        gate_own,
        up_own,
        down_own,
    )


def solution(mesh):
    return jax.shard_map(
        body,
        mesh=mesh,
        in_specs=(
            P("dp", "ctx", None),
            P("dp", None),
            P(("dp", "ctx")),
            P(("dp", "ctx"), None),
            P(("dp", "ctx"), None),
            P(("dp", "ctx")),
            P(("dp", "ctx"), None),
            P(("dp", "ctx"), None),
            P(("dp", "ctx"), None),
            P("dp", "ctx", None),
        ),
        out_specs=(
            P("dp", "ctx", None),
            P("dp", "ctx", None),
            P(("dp", "ctx")),
            P(("dp", "ctx"), None),
            P(("dp", "ctx"), None),
            P(("dp", "ctx")),
            P(("dp", "ctx"), None),
            P(("dp", "ctx"), None),
            P(("dp", "ctx"), None),
        ),
        check_vma=False,
    )
```
